32 devices in a mesh: dp: 1 (over z), tx: 4 (over y), ty: 8 (over x, core).
Axes of the slice: x: 4, y: 4, z: 1, core: 2. Of those that a mesh axis runs over, the one named last changes fastest.
The devices are a block of a 4x4x8 slice.
Arguments:
- x_in: bfloat16 [24, 576, 1024], P('dp', None, 'tx')
- ln1_gain: float32 [2, 1024], P(None, 'tx')
- ln1_bias: float32 [2, 1024], P(None, 'tx')
- w_q: bfloat16 [2, 1024, 16, 64], P(None, 'tx', 'ty')
- b_q: float32 [2, 16, 64], P(None, 'ty')
- w_k: bfloat16 [2, 1024, 16, 64], P(None, 'tx', 'ty')
- w_v: bfloat16 [2, 1024, 16, 64], P(None, 'tx', 'ty')
- b_v: float32 [2, 16, 64], P(None, 'ty')
- w_o: bfloat16 [2, 16, 64, 1024], P(None, 'ty', None, 'tx')
- b_o: float32 [2, 1024], P(None, 'tx')
- ln2_gain: float32 [2, 1024], P(None, 'tx')
- ln2_bias: float32 [2, 1024], P(None, 'tx')
- w_up: bfloat16 [2, 1024, 4096], P(None, 'tx', 'ty')
- b_up: float32 [2, 4096], P(None, 'ty')
- w_down: bfloat16 [2, 4096, 1024], P(None, 'ty', 'tx')
- b_down: float32 [2, 1024], P(None, 'tx')
Outputs:
- output: bfloat16 [24, 576, 1024], P('dp', None, 'tx')
All inputs are finite; a program needn't handle non-finite values.
Results may differ from the reference program's by a relative error of at most 0.02.
Values are sent between devices in bfloat16 or wider.
A program may use at most 768 MiB of HBM per device.

```python
import jax
import jax.numpy as jnp
from jax import lax

IMGS = 24
N = 576
W = 1024
HEADS = 16
HEAD = 64
F = 4096
EPS = 1e-6


def setup_inputs(seed: int = 0, part: int = 0) -> dict:
    key = jax.random.key(seed)
    keys = jax.random.split(key, 16)
    act_keys = jax.random.split(jax.random.fold_in(key, part), 3)
    col_mean = 0.5 * jax.random.normal(act_keys[0], (W,), jnp.float32)
    col_scale = jnp.exp(0.5 * jax.random.normal(act_keys[1], (W,), jnp.float32))
    x_vals = jax.random.normal(act_keys[2], (IMGS, N, W), jnp.float32) * col_scale + col_mean
    w_scale = W ** -0.5
    f_scale = F ** -0.5

    def draw(index, shape, scale):
        return scale * jax.random.normal(keys[index], shape, jnp.float32)

    return {
        "x_in": x_vals.astype(jnp.bfloat16),
        "ln1_gain": 1.0 + draw(0, (2, W), 0.3),
        "ln1_bias": draw(1, (2, W), 0.3),
        "w_q": draw(2, (2, W, HEADS, HEAD), 1.7 * w_scale).astype(jnp.bfloat16),
        "b_q": draw(3, (2, HEADS, HEAD), 0.5),
        "w_k": draw(4, (2, W, HEADS, HEAD), 1.7 * w_scale).astype(jnp.bfloat16),
        "w_v": draw(5, (2, W, HEADS, HEAD), w_scale).astype(jnp.bfloat16),
        "b_v": draw(6, (2, HEADS, HEAD), 0.5),
        "w_o": draw(7, (2, HEADS, HEAD, W), w_scale).astype(jnp.bfloat16),
        "b_o": draw(8, (2, W), 0.3),
        "ln2_gain": 1.0 + draw(9, (2, W), 0.3),
        "ln2_bias": draw(10, (2, W), 0.3),
        "w_up": draw(11, (2, W, F), w_scale).astype(jnp.bfloat16),
        "b_up": draw(12, (2, F), 0.5),
        "w_down": draw(13, (2, F, W), f_scale).astype(jnp.bfloat16),
        "b_down": draw(14, (2, W), 0.3),
    }


def layer_norm(x_f, gain, shift):
    mean = jnp.mean(x_f, axis=-1, keepdims=True)
    centred = x_f - mean
    variance = jnp.mean(centred * centred, axis=-1, keepdims=True)
    return (centred * lax.rsqrt(variance + EPS) * gain + shift).astype(jnp.bfloat16)


def encoder_layer(x_img, params):
    (ln1_gain, ln1_bias, w_q, b_q, w_k, w_v, b_v, w_o, b_o,
     ln2_gain, ln2_bias, w_up, b_up, w_down, b_down) = params
    x_f = x_img.astype(jnp.float32)
    normed = layer_norm(x_f, ln1_gain, ln1_bias)
    q_proj = (jnp.dot(normed, w_q.reshape(W, W), preferred_element_type=jnp.float32) + b_q.reshape(W)).astype(jnp.bfloat16)
    k_proj = jnp.dot(normed, w_k.reshape(W, W), preferred_element_type=jnp.float32).astype(jnp.bfloat16)
    v_proj = (jnp.dot(normed, w_v.reshape(W, W), preferred_element_type=jnp.float32) + b_v.reshape(W)).astype(jnp.bfloat16)
    q_heads = q_proj.reshape(N, HEADS, HEAD).astype(jnp.float32)
    k_heads = k_proj.reshape(N, HEADS, HEAD).astype(jnp.float32)
    v_heads = v_proj.reshape(N, HEADS, HEAD).astype(jnp.float32)
    scores = jnp.einsum("qhd,khd->hqk", q_heads, k_heads) * (HEAD ** -0.5)
    attn_prob = jax.nn.softmax(scores, axis=-1).astype(jnp.bfloat16)
    attended = jnp.einsum("hqk,khd->qhd", attn_prob.astype(jnp.float32), v_heads).astype(jnp.bfloat16)
    x_mid = (x_f + jnp.dot(attended.reshape(N, W), w_o.reshape(W, W), preferred_element_type=jnp.float32) + b_o).astype(jnp.bfloat16)
    mid_f = x_mid.astype(jnp.float32)
    normed2 = layer_norm(mid_f, ln2_gain, ln2_bias)
    hidden = jax.nn.gelu(jnp.dot(normed2, w_up, preferred_element_type=jnp.float32) + b_up, approximate=True).astype(jnp.bfloat16)
    x_out = (mid_f + jnp.dot(hidden, w_down, preferred_element_type=jnp.float32) + b_down).astype(jnp.bfloat16)
    return x_out, None


def reference(x_in, ln1_gain, ln1_bias, w_q, b_q, w_k, w_v, b_v, w_o, b_o, ln2_gain, ln2_bias, w_up, b_up, w_down, b_down):
    params = (ln1_gain, ln1_bias, w_q, b_q, w_k, w_v, b_v, w_o, b_o,
              ln2_gain, ln2_bias, w_up, b_up, w_down, b_down)

    def run_image(x_img):
        x_last, _ = lax.scan(encoder_layer, x_img, params)
        return x_last

    return lax.map(run_image, x_in)
```

```python
import functools
import math

import jax
import jax.numpy as jnp
from jax import lax
from jax.experimental import pallas as pl
from jax.experimental.pallas import tpu as pltpu
from jax.sharding import PartitionSpec as P

EPS = 1e-6
F32, BF16 = jnp.float32, jnp.bfloat16


def dot(a, b):
    return jnp.dot(a, b, preferred_element_type=F32)


def norm(x_f, gain, shift):
    mean = jnp.mean(x_f, axis=-1, keepdims=True)
    centred = x_f - mean
    variance = jnp.mean(centred * centred, axis=-1, keepdims=True)
    return (centred * lax.rsqrt(variance + EPS) * gain + shift).astype(BF16)


def norm_rows(x_ref, gain_ref, shift_ref, h_ref, rows):
    def body(r, _):
        at = pl.ds(pl.multiple_of(r * rows, rows), rows)
        h_ref[at, :] = norm(x_ref[at, :].astype(F32), gain_ref[...], shift_ref[...])
        return 0

    lax.fori_loop(0, x_ref.shape[0] // rows, body, 0)


def finish_rows(x_ref, acc_ref, bias_ref, out_ref, rows):
    def body(r, _):
        at = pl.ds(pl.multiple_of(r * rows, rows), rows)
        out_ref[at, :] = (x_ref[at, :].astype(F32) + acc_ref[at, :] + bias_ref[...]).astype(BF16)
        return 0

    lax.fori_loop(0, x_ref.shape[0] // rows, body, 0)


def attention_kernel(head, x_ref, gain_ref, shift_ref, wqkv_ref, bqkv_ref, wo_ref, bo_ref, out_ref, h_ref, qkv_ref, o_ref, acc_ref):
    step = pl.program_id(0)
    txs, _, depth, cols = wqkv_ref.shape
    tokens = x_ref.shape[0]
    pair = cols // 3

    @pl.when(step == 0)
    def _():
        norm_rows(x_ref, gain_ref, shift_ref, h_ref, 96)
        acc_ref[...] = jnp.zeros_like(acc_ref)

    for n in range(3):
        at = pl.ds(n * pair, pair)
        total = jnp.zeros((tokens, pair), F32)
        for t in range(txs):
            total += dot(h_ref[:, pl.ds(t * depth, depth)], wqkv_ref[t, 0, :, at])
        qkv_ref[:, at] = (total + bqkv_ref[0, :, at]).astype(BF16)

    scale = head ** -0.5 * math.log2(math.e)
    chunk = 192
    for c in range(tokens // chunk):
        rows = pl.ds(c * chunk, chunk)
        outs = []
        for hd in range(pair // head):
            q = qkv_ref[rows, pl.ds(hd * head, head)]
            k = qkv_ref[:, pl.ds(pair + hd * head, head)]
            v = qkv_ref[:, pl.ds(2 * pair + hd * head, head)]
            s = lax.dot_general(q, k, (((1,), (1,)), ((), ())), preferred_element_type=F32)
            e = jnp.exp2((s - jnp.max(s, axis=-1, keepdims=True)) * scale)
            p = (e * (1.0 / jnp.sum(e, axis=-1, keepdims=True))).astype(BF16)
            outs.append(dot(p, v))
        o_ref[rows, :] = jnp.concatenate(outs, axis=-1).astype(BF16)

    width = wo_ref.shape[3]
    for t in range(txs):
        at = pl.ds(t * width, width)
        acc_ref[:, at] += dot(o_ref[...], wo_ref[t, 0])

    @pl.when(step == pl.num_programs(0) - 1)
    def _():
        finish_rows(x_ref, acc_ref, bo_ref, out_ref, 96)


def mlp_kernel(x_ref, gain_ref, shift_ref, wup_ref, bup_ref, wdown_ref, bdown_ref, out_ref, h_ref, u_ref, acc_ref):
    step = pl.program_id(0)
    txs, _, depth, hidden = wup_ref.shape
    tokens = x_ref.shape[0]

    @pl.when(step == 0)
    def _():
        norm_rows(x_ref, gain_ref, shift_ref, h_ref, 96)
        acc_ref[...] = jnp.zeros_like(acc_ref)

    tile = 256
    for n in range(hidden // tile):
        at = pl.ds(n * tile, tile)
        total = jnp.zeros((tokens, tile), F32)
        for t in range(txs):
            total += dot(h_ref[:, pl.ds(t * depth, depth)], wup_ref[t, 0, :, at])
        u_ref[:, at] = jax.nn.gelu(total + bup_ref[0, :, at], approximate=True).astype(BF16)

    width = wdown_ref.shape[3]
    for t in range(txs):
        at = pl.ds(t * width, width)
        acc_ref[:, at] += dot(u_ref[...], wdown_ref[t, 0])

    @pl.when(step == pl.num_programs(0) - 1)
    def _():
        finish_rows(x_ref, acc_ref, bdown_ref, out_ref, 96)


def whole(a):
    return pl.BlockSpec(a.shape, lambda i: (0,) * a.ndim)


def per_step(a):
    return pl.BlockSpec((1,) + a.shape[1:], lambda i: (i,) + (0,) * (a.ndim - 1))


def blocks(a):
    return pl.BlockSpec((a.shape[0], 1) + a.shape[2:], lambda i: (0, i, 0, 0))


def attention_block(head, x, gain, shift, wqkv, bqkv, wo, bo):
    tokens, width = x.shape
    steps, cols = wqkv.shape[1], wqkv.shape[3]
    return pl.pallas_call(
        functools.partial(attention_kernel, head),
        out_shape=jax.ShapeDtypeStruct(x.shape, BF16),
        grid=(steps,),
        in_specs=[whole(x), whole(gain), whole(shift), blocks(wqkv), per_step(bqkv), blocks(wo), whole(bo)],
        out_specs=whole(x),
        scratch_shapes=[pltpu.VMEM((tokens, width), BF16), pltpu.VMEM((tokens, cols), BF16),
                        pltpu.VMEM((tokens, cols // 3), BF16), pltpu.VMEM((tokens, width), F32)],
        compiler_params=pltpu.CompilerParams(dimension_semantics=("arbitrary",), vmem_limit_bytes=48 << 20),
        cost_estimate=pl.CostEstimate(flops=20_000_000_000, bytes_accessed=10_000_000, transcendentals=5_000_000),
        name="attention_block",
    )(x, gain, shift, wqkv, bqkv, wo, bo)


def mlp_block(x, gain, shift, wup, bup, wdown, bdown):
    tokens, width = x.shape
    steps, hidden = wup.shape[1], wup.shape[3]
    return pl.pallas_call(
        mlp_kernel,
        out_shape=jax.ShapeDtypeStruct(x.shape, BF16),
        grid=(steps,),
        in_specs=[whole(x), whole(gain), whole(shift), blocks(wup), per_step(bup), blocks(wdown), whole(bdown)],
        out_specs=whole(x),
        scratch_shapes=[pltpu.VMEM((tokens, width), BF16), pltpu.VMEM((tokens, hidden), BF16), pltpu.VMEM((tokens, width), F32)],
        compiler_params=pltpu.CompilerParams(dimension_semantics=("arbitrary",), vmem_limit_bytes=48 << 20),
        cost_estimate=pl.CostEstimate(flops=20_000_000_000, bytes_accessed=18_000_000, transcendentals=2_000_000),
        name="mlp_block",
    )(x, gain, shift, wup, bup, wdown, bdown)


def solution(mesh):
    txs, tys = mesh.shape["tx"], mesh.shape["ty"]
    act_spec = P("dp", None, "tx")
    vec_tx = P(None, "tx")
    proj_spec = P(None, "tx", "ty", None)
    head_vec = P(None, "ty", None)
    in_specs = (act_spec, vec_tx, vec_tx, proj_spec, head_vec, proj_spec, proj_spec, head_vec,
                P(None, "ty", None, "tx"), vec_tx, vec_tx, vec_tx,
                P(None, "tx", "ty"), P(None, "ty"), P(None, "ty", "tx"), vec_tx)

    def local_fn(x_in, ln1_gain, ln1_bias, w_q, b_q, w_k, w_v, b_v, w_o, b_o, ln2_gain, ln2_bias, w_up, b_up, w_down, b_down):
        layers, depth, heads, head = w_q.shape
        imgs, tokens, part = x_in.shape
        width = part * txs
        each = imgs // tys
        pad = txs - each
        ty = lax.axis_index("ty")

        def gather(w):
            full = lax.all_gather(w, ("tx", "ty"), axis=0, tiled=False)
            return full.reshape((txs, tys) + w.shape)

        vecs = lax.all_gather(jnp.stack([ln1_gain, ln1_bias, b_o, ln2_gain, ln2_bias, b_down]), "tx", axis=2, tiled=True)
        pair = heads * head
        zero = jnp.zeros((layers, pair), F32)
        bias = lax.all_gather(jnp.concatenate([b_q.reshape(layers, pair), zero, b_v.reshape(layers, pair), b_up], axis=1), "ty", axis=1, tiled=False)
        bias = bias[:, :, None, :]

        mine = lax.dynamic_slice_in_dim(x_in, ty * each, each, 0)
        mine = jnp.concatenate([mine, mine[:pad]], axis=0)
        x = lax.all_to_all(mine, "tx", 0, 2, tiled=True).reshape(tokens, width)

        weights = []
        for layer in range(layers):
            qkv = jnp.concatenate([w[layer].reshape(depth, pair) for w in (w_q, w_k, w_v)], axis=1)
            weights.append((gather(qkv), gather(w_o[layer].reshape(pair, part)), gather(w_up[layer]), gather(w_down[layer])))
        for layer in range(layers):
            gain1, shift1, bo, gain2, shift2, bdown = (vecs[i, layer][None] for i in range(6))
            wqkv, wo, wup, wdown = weights[layer]
            x = attention_block(head, x, gain1, shift1, wqkv, bias[layer, ..., :3 * pair], wo, bo)
            x = mlp_block(x, gain2, shift2, wup, bias[layer, ..., 3 * pair:], wdown, bdown)
        y = lax.all_to_all(x.reshape(1, tokens, width), "tx", 2, 0, tiled=True)[:each]
        return lax.all_gather(y, "ty", axis=0, tiled=True)

    return jax.shard_map(local_fn, mesh=mesh, in_specs=in_specs, out_specs=act_spec, check_vma=False)
```

```python
import functools
import math

import jax
import jax.numpy as jnp
from jax import lax
from jax.experimental import pallas as pl
from jax.experimental.pallas import tpu as pltpu
from jax.sharding import PartitionSpec as P

EPS = 1e-6
F32, BF16 = jnp.float32, jnp.bfloat16
MESH = pl.DeviceIdType.MESH
CORES = 2
STEPS = {"xp": (1, 0), "xm": (-1, 0), "yp": (0, 1), "ym": (0, -1)}
ALL, A, B = (0, 2), (0, 1), (1, 1)
PLUS, MINUS = (0, 1), (1, 1)
PHASES = (
    [("xp", (0, 0), ALL, ALL), ("yp", (0, 0), ALL, ALL), ("xm", (0, 0), ALL, ALL), ("ym", (0, 0), ALL, ALL),
     ("sib", (0, 0), ALL, ALL)],
    [("xp", (-1, 0), ALL, PLUS), ("yp", (0, -1), ALL, PLUS), ("xm", (1, 0), ALL, MINUS), ("ym", (0, 1), ALL, MINUS),
     ("xp", (0, -1), B, ALL), ("yp", (-1, 0), A, ALL), ("xm", (0, -1), B, ALL), ("ym", (-1, 0), A, ALL),
     ("xp", (0, 1), B, ALL), ("yp", (1, 0), A, ALL), ("xm", (0, 1), B, ALL), ("ym", (1, 0), A, ALL),
     ("sib", (-1, 0), ALL, ALL), ("sib", (1, 0), ALL, ALL), ("sib", (0, -1), ALL, ALL), ("sib", (0, 1), ALL, ALL)],
    [("xp", (0, 2), B, ALL), ("yp", (2, 0), A, ALL), ("xm", (0, 2), B, ALL), ("ym", (2, 0), A, ALL),
     ("xp", (-1, -1), B, PLUS), ("yp", (-1, -1), A, PLUS), ("xm", (1, -1), B, MINUS), ("ym", (-1, 1), A, MINUS),
     ("xp", (-1, 1), B, PLUS), ("yp", (1, -1), A, PLUS), ("xm", (1, 1), B, MINUS), ("ym", (1, 1), A, MINUS),
     ("sib", (2, 0), ALL, ALL), ("sib", (0, 2), ALL, ALL), ("sib", (-1, -1), ALL, ALL), ("sib", (1, -1), ALL, ALL),
     ("sib", (-1, 1), ALL, ALL), ("sib", (1, 1), ALL, ALL)],
    [("xp", (-1, 2), B, PLUS), ("yp", (2, -1), A, PLUS), ("xm", (1, 2), B, MINUS), ("ym", (2, 1), A, MINUS),
     ("sib", (-1, 2), ALL, ALL), ("sib", (1, 2), ALL, ALL), ("sib", (2, -1), ALL, ALL), ("sib", (2, 1), ALL, ALL)],
    [("sib", (2, 2), ALL, ALL)],
)
SENT = ((5, 1), (5, 2), (5, 2), (5, 1), (1, 1))
FIRST = [sum(len(p) for p in PHASES[:i]) for i in range(len(PHASES) + 1)]
BEFORE = [(0, 0), (1, 0), (0, 1), (2, 0), (1, 1), (3, 0), (0, 2), (4, 0), (5, 0)]
SLOTS = (
    {0: [(2, 1)], 1: [(1, 2)], 2: [(3, 1), (0, 3)], 3: [(4, 1), (2, 2)], 4: [(1, 3)], 5: [(3, 2), (0, 4)], 6: [(4, 2)], 7: [(2, 3)]},
    {0: [(5, 1), (5, 2)], 1: [(1, 4)], 3: [(3, 3), (0, 5)], 5: [(4, 3)], 7: [(2, 4)]},
    {0: [(5, 3), (1, 5)], 1: [(3, 4)], 2: [(4, 4), (2, 5)], 4: [(3, 5)], 5: [(4, 5)]},
    {0: [(5, 4), (5, 5)]},
)


def dot(a, b):
    return jnp.dot(a, b, preferred_element_type=F32)


def kernel(head, each, w_ref, vec_ref, bias_ref, x_hbm, out_ref, g_ref,
           x_ref, h_ref, acc_ref, qkv_ref, o_ref, u_ref, wbuf, vecs, biases,
           send_sem, recv_sem, own_sem, load_sem, vec_send, vec_recv, bias_send, bias_recv,
           xin_send, xin_recv, o1_send, o1_recv, ring_send, ring_recv):
    groups, tys, txs = g_ref.shape[:3]
    nx, ny = tys // CORES, txs
    tokens, part = x_ref.shape[1:]
    me_t, me_s = lax.axis_index("tx"), lax.axis_index("ty")
    my_x, my_c = me_s // CORES, lax.rem(me_s, CORES)
    sibling = my_x * CORES + (CORES - 1 - my_c)
    worker = me_t < each

    def ty_at(dx):
        return lax.rem(my_x + dx + nx, nx) * CORES + my_c

    def tx_at(dy):
        return lax.rem(me_t + dy + ny, ny)

    def target(to):
        if to == "sib":
            return {"ty": sibling}
        dx, dy = STEPS[to]
        return {"ty": ty_at(dx)} if dx else {"tx": tx_at(dy)}

    barrier = pltpu.get_barrier_semaphore()
    for k in range(1, txs):
        pl.semaphore_signal(barrier, inc=1, device_id={"tx": tx_at(k)}, device_id_type=MESH)
    for k in range(1, tys):
        pl.semaphore_signal(barrier, inc=1, device_id={"ty": lax.rem(me_s + k, tys)}, device_id_type=MESH)
    pl.semaphore_wait(barrier, txs - 1 + tys - 1)

    def piece(g, ty, tx, half, sign):
        return g_ref.at[g, ty, tx, pl.ds(*half), pl.ds(*sign)]

    def copy(phase, i, g):
        to, (dx, dy), half, sign = PHASES[phase][i]
        place = piece(g, ty_at(dx), tx_at(dy), half, sign)
        return pltpu.make_async_remote_copy(
            src_ref=w_ref.at[g] if phase == 0 else place, dst_ref=place, send_sem=send_sem.at[g, phase],
            recv_sem=recv_sem.at[g, FIRST[phase] + i], device_id=target(to), device_id_type=MESH)

    def arrival(phase, i, g):
        to, (dx, dy), half, sign = PHASES[phase][i]
        if to == "sib":
            ty = lax.rem(my_x + dx + nx, nx) * CORES + (CORES - 1 - my_c)
            place = piece(g, ty, tx_at(dy), half, sign)
        else:
            sx, sy = STEPS[to]
            place = piece(g, ty_at(dx - sx), tx_at(dy - sy), half, sign)
        return pltpu.make_async_remote_copy(
            src_ref=place, dst_ref=place, send_sem=send_sem.at[g, phase],
            recv_sem=recv_sem.at[g, FIRST[phase] + i], device_id=target(to), device_id_type=MESH)

    def event(phase, g):
        if phase == 5:
            for p in range(5):
                for i, c in enumerate(PHASES[p]):
                    if c[0] == "sib":
                        arrival(p, i, g).wait_recv()
            return
        if phase:
            for i, c in enumerate(PHASES[phase - 1]):
                if c[0] != "sib":
                    arrival(phase - 1, i, g).wait_recv()
        for i in range(len(PHASES[phase])):
            copy(phase, i, g).start()

    for e in BEFORE[:1]:
        event(*e)
    own = pltpu.make_async_copy(w_ref, g_ref.at[:, me_s, me_t], own_sem)
    own.start()

    def x_copy(j):
        return pltpu.make_async_remote_copy(
            src_ref=x_hbm.at[me_s * each + j], dst_ref=x_ref.at[me_t], send_sem=xin_send.at[j],
            recv_sem=xin_recv.at[me_t], device_id={"tx": j}, device_id_type=MESH)

    def x_local():
        return pltpu.make_async_copy(x_hbm.at[me_s * each + me_t], x_ref.at[me_t], xin_recv.at[me_t])

    for j in range(each):
        @pl.when(me_t != j)
        def _():
            x_copy(j).start()

        @pl.when(me_t == j)
        def _():
            x_local().start()

    def vec_copy(k):
        return pltpu.make_async_remote_copy(
            src_ref=vec_ref, dst_ref=vecs.at[me_t], send_sem=vec_send.at[k], recv_sem=vec_recv.at[k],
            device_id={"tx": tx_at(k)}, device_id_type=MESH)

    def bias_copy(k):
        return pltpu.make_async_remote_copy(
            src_ref=bias_ref, dst_ref=biases.at[me_s], send_sem=bias_send.at[k], recv_sem=bias_recv.at[k],
            device_id={"ty": lax.rem(me_s + k, tys)}, device_id_type=MESH)

    for k in range(1, txs):
        vec_copy(k).start()
    for k in range(1, tys):
        bias_copy(k).start()
    vecs[me_t] = vec_ref[...]
    biases[me_s] = bias_ref[...]

    for e in BEFORE[1:]:
        event(*e)

    for k in range(1, txs):
        vec_copy(k).wait()
    for k in range(1, tys):
        bias_copy(k).wait()
    own.wait()

    @pl.when(worker)
    def _():
        for m in range(txs):
            pltpu.make_async_copy(x_hbm.at[0], x_ref.at[m], xin_recv.at[m]).wait()

    def vec(row):
        return jnp.concatenate([vecs[t, pl.ds(row, 1), :] for t in range(txs)], axis=-1)

    def norm(gain_row, shift_row):
        rows = 96

        def body(r, _):
            at = pl.ds(pl.multiple_of(r * rows, rows), rows)
            x_f = jnp.concatenate([x_ref[t, at, :] for t in range(txs)], axis=-1).astype(F32)
            mean = jnp.mean(x_f, axis=-1, keepdims=True)
            centred = x_f - mean
            variance = jnp.mean(centred * centred, axis=-1, keepdims=True)
            h = (centred * lax.rsqrt(variance + EPS) * vec(gain_row) + vec(shift_row)).astype(BF16)
            for t in range(txs):
                h_ref[t, at, :] = h[:, t * part:(t + 1) * part]
                acc_ref[t, at, :] = jnp.zeros((rows, part), F32)
            return 0

        lax.fori_loop(0, tokens // rows, body, 0)

    def finish(bias_row):
        rows = 96

        def body(r, _):
            at = pl.ds(pl.multiple_of(r * rows, rows), rows)
            for t in range(txs):
                x_ref[t, at, :] = (x_ref[t, at, :].astype(F32) + acc_ref[t, at, :] + vecs[t, pl.ds(bias_row, 1), :]).astype(BF16)
            return 0

        lax.fori_loop(0, tokens // rows, body, 0)

    depth = 4 * g_ref.shape[5]
    pair = o_ref.shape[1]

    def block(slot, which, t, columns):
        part_of = wbuf[slot, which, t, :, :, :, columns]
        return part_of.reshape(depth, part_of.shape[-1])

    def loads(slot, g, step, count):
        return [pltpu.make_async_copy(g_ref.at[g + i, step], wbuf.at[slot, i], load_sem.at[slot, i]) for i in range(count)]

    def run(slots, g, count, body):
        @pl.when(worker)
        def _():
            for c in ():
                c.start()

        def step_body(step, _):
            slot = lax.rem(step, 2)
            for s, events in slots.items():
                @pl.when(step == s)
                def _(events=events):
                    for e in events:
                        event(*e)

            @pl.when(worker)
            def _():
                @pl.when(step == 0)
                def _():
                    for c in loads(slot, g, step, count):
                        c.start()

                @pl.when(step + 1 < tys)
                def _():
                    for c in loads(1 - slot, g, step + 1, count):
                        c.start()
                for c in loads(slot, g, step, count):
                    c.wait()
                body(step, slot)
            return 0

        lax.fori_loop(0, tys, step_body, 0)

    def attention(layer, step, slot):
        for n in range(3):
            at = pl.ds(n * pair, pair)
            total = jnp.zeros((tokens, pair), F32)
            for t in range(txs):
                total += dot(h_ref[t], block(slot, 0, t, at))
            qkv_ref[:, at] = (total + biases[step, pl.ds(layer, 1), at]).astype(BF16)

        scale = head ** -0.5 * math.log2(math.e)
        chunk = 192
        for c in range(tokens // chunk):
            rows = pl.ds(c * chunk, chunk)
            outs = []
            for hd in range(pair // head):
                q = qkv_ref[rows, pl.ds(hd * head, head)]
                k = qkv_ref[:, pl.ds(pair + hd * head, head)]
                v = qkv_ref[:, pl.ds(2 * pair + hd * head, head)]
                s = lax.dot_general(q, k, (((1,), (1,)), ((), ())), preferred_element_type=F32)
                e = jnp.exp2((s - jnp.max(s, axis=-1, keepdims=True)) * scale)
                p = (e * (1.0 / jnp.sum(e, axis=-1, keepdims=True))).astype(BF16)
                outs.append(dot(p, v))
            o_ref[rows, :] = jnp.concatenate(outs, axis=-1).astype(BF16)

        for t in range(txs):
            w = block(slot, 0, t, pl.ds(3 * pair, part - pair))
            wo = jnp.concatenate([w[i * pair:(i + 1) * pair] for i in range(part // pair)], axis=1)
            acc_ref[t] += dot(o_ref[...], wo)

    def mlp(layer, step, slot):
        hidden = u_ref.shape[1]
        for n in range(hidden // part):
            at = pl.ds(n * part, part)
            total = jnp.zeros((tokens, part), F32)
            for t in range(txs):
                total += dot(h_ref[t], block(slot, 0, t, at))
            bias = biases[step, pl.ds(layer, 1), pl.ds(3 * pair + n * part, part)]
            u_ref[:, at] = jax.nn.gelu(total + bias, approximate=True).astype(BF16)
        for t in range(txs):
            total = acc_ref[t]
            for n in range(hidden // depth):
                total += dot(u_ref[:, pl.ds(n * depth, depth)], block(slot, 1, t, pl.ds(n * part, part)))
            acc_ref[t] = total

    layers = groups // 3
    for layer in range(layers):
        row = 6 * layer

        @pl.when(worker)
        def _():
            norm(row, row + 1)
        run(SLOTS[2 * layer], 3 * layer, 1, functools.partial(attention, layer))

        @pl.when(worker)
        def _():
            finish(row + 2)
            norm(row + 3, row + 4)
        run(SLOTS[2 * layer + 1], 3 * layer + 1, 2, functools.partial(mlp, layer))

        @pl.when(worker)
        def _():
            finish(row + 5)

    def o1_copy(k):
        return pltpu.make_async_remote_copy(
            src_ref=x_ref.at[tx_at(k)], dst_ref=out_ref.at[me_s * each + me_t], send_sem=o1_send.at[k],
            recv_sem=o1_recv.at[me_t], device_id={"tx": tx_at(k)}, device_id_type=MESH)

    def o1_local():
        return pltpu.make_async_copy(x_ref.at[me_t], out_ref.at[me_s * each + me_t], o1_recv.at[me_t])

    @pl.when(worker)
    def _():
        for k in range(1, txs):
            o1_copy(k).start()
        o1_local().start()

    half = tokens // 2
    every, first, second = pl.ds(0, tokens), pl.ds(0, half), pl.ds(half, half)
    ring = (("xp", 0, every), ("xm", 0, every), ("sib", 0, every),
            ("xp", -1, first), ("xm", 1, second), ("sib", -1, every), ("sib", 1, every), ("sib", 2, every))

    def ring_copy(kind, m):
        to, dx, rows = ring[kind]
        place = out_ref.at[ty_at(dx) * each + m, rows]
        return pltpu.make_async_remote_copy(
            src_ref=place, dst_ref=place, send_sem=ring_send.at[kind, m], recv_sem=ring_recv.at[kind, m],
            device_id=target(to), device_id_type=MESH)

    def ring_arrival(kind, m):
        to, dx, rows = ring[kind]
        if to == "sib":
            ty = lax.rem(my_x + dx + nx, nx) * CORES + (CORES - 1 - my_c)
        else:
            ty = ty_at(dx - STEPS[to][0])
        place = out_ref.at[ty * each + m, rows]
        return pltpu.make_async_remote_copy(
            src_ref=place, dst_ref=place, send_sem=ring_send.at[kind, m], recv_sem=ring_recv.at[kind, m],
            device_id=target(to), device_id_type=MESH)

    for m in range(each):
        place = out_ref.at[me_s * each + m]
        pltpu.make_async_copy(x_ref.at[0], place, o1_recv.at[m]).wait()
        for kind in (0, 1, 2):
            ring_copy(kind, m).start()
    for m in range(each):
        ring_arrival(0, m).wait_recv()
        ring_copy(3, m).start()
        ring_copy(5, m).start()
        ring_arrival(1, m).wait_recv()
        ring_copy(4, m).start()
        ring_copy(6, m).start()
    for m in range(each):
        ring_arrival(3, m).wait_recv()
        ring_arrival(4, m).wait_recv()
        ring_copy(7, m).start()
    for m in range(each):
        for kind in (2, 5, 6, 7):
            ring_arrival(kind, m).wait_recv()

    for m in range(each):
        for kind in range(len(ring)):
            ring_copy(kind, m).wait_send()
    for j in range(each):
        @pl.when(me_t != j)
        def _():
            x_copy(j).wait_send()

    @pl.when(worker)
    def _():
        for k in range(1, txs):
            o1_copy(k).wait_send()
    for g in range(groups):
        for phase, (a, b) in enumerate(SENT):
            place = g_ref.at[g, pl.ds(0, a), pl.ds(0, b)]
            pltpu.make_async_remote_copy(
                src_ref=place, dst_ref=place, send_sem=send_sem.at[g, phase], recv_sem=recv_sem.at[g, 0],
                device_id={"ty": sibling}, device_id_type=MESH).wait_send()


def solution(mesh):
    txs, tys = mesh.shape["tx"], mesh.shape["ty"]
    act_spec = P("dp", None, "tx")
    vec_tx = P(None, "tx")
    proj_spec = P(None, "tx", "ty", None)
    head_vec = P(None, "ty", None)
    in_specs = (act_spec, vec_tx, vec_tx, proj_spec, head_vec, proj_spec, proj_spec, head_vec,
                P(None, "ty", None, "tx"), vec_tx, vec_tx, vec_tx,
                P(None, "tx", "ty"), P(None, "ty"), P(None, "ty", "tx"), vec_tx)

    def local_fn(x_in, ln1_gain, ln1_bias, w_q, b_q, w_k, w_v, b_v, w_o, b_o, ln2_gain, ln2_bias, w_up, b_up, w_down, b_down):
        layers, depth, heads, head = w_q.shape
        imgs, tokens, part = x_in.shape
        hidden = w_up.shape[2]
        each, pair = imgs // tys, heads * head

        qkv = [w.reshape(layers, depth, pair) for w in (w_q, w_k, w_v)]
        wo = w_o.reshape(layers, pair, part)
        wo = jnp.concatenate([wo[:, :, i * pair:(i + 1) * pair] for i in range(part // pair)], axis=1)
        down = jnp.concatenate([w_down[:, i * depth:(i + 1) * depth] for i in range(hidden // depth)], axis=2)
        packed = jnp.stack([jnp.concatenate(qkv + [wo], axis=2), w_up, down], axis=1)
        groups = 3 * layers
        packed = packed.reshape(groups, 2, 2, depth // 4, hidden)

        vec = jnp.stack([ln1_gain, ln1_bias, b_o, ln2_gain, ln2_bias, b_down], axis=1).reshape(6 * layers, part)
        vec = jnp.pad(vec, ((0, -vec.shape[0] % 8), (0, 0)))
        bias = jnp.concatenate([b_q.reshape(layers, pair), jnp.zeros((layers, pair), F32), b_v.reshape(layers, pair), b_up], axis=1)
        bias = jnp.pad(bias, ((0, -layers % 8), (0, 0)))

        vmem = pl.BlockSpec(memory_space=pltpu.VMEM)
        hbm = pl.BlockSpec(memory_space=pl.ANY)
        dma = pltpu.SemaphoreType.DMA
        out, _ = pl.pallas_call(
            functools.partial(kernel, head, each),
            out_shape=(jax.ShapeDtypeStruct(x_in.shape, BF16),
                       jax.ShapeDtypeStruct((groups, tys, txs) + packed.shape[1:], BF16)),
            in_specs=[vmem, vmem, vmem, hbm],
            out_specs=(hbm, hbm),
            scratch_shapes=[
                pltpu.VMEM((txs, tokens, part), BF16), pltpu.VMEM((txs, tokens, part), BF16), pltpu.VMEM((txs, tokens, part), F32),
                pltpu.VMEM((tokens, 3 * pair), BF16), pltpu.VMEM((tokens, pair), BF16), pltpu.VMEM((tokens, hidden), BF16),
                pltpu.VMEM((2, 2, txs) + packed.shape[1:], BF16),
                pltpu.VMEM((txs,) + vec.shape, F32), pltpu.VMEM((tys,) + bias.shape, F32),
                dma((groups, 5)), dma((groups, FIRST[-1])), dma, dma((2, 2)), dma((txs,)), dma((txs,)), dma((tys,)), dma((tys,)),
                dma((each,)), dma((txs,)), dma((txs,)), dma((txs,)), dma((8, each)), dma((8, each)),
            ],
            compiler_params=pltpu.CompilerParams(collective_id=0, has_side_effects=True, vmem_limit_bytes=60 << 20),
            cost_estimate=pl.CostEstimate(flops=80_000_000_000, bytes_accessed=150_000_000, transcendentals=20_000_000),
            name="encoder",
        )(packed, vec, bias, x_in)
        return out

    return jax.shard_map(local_fn, mesh=mesh, in_specs=in_specs, out_specs=act_spec, check_vma=False)
```

```python
import functools
import math

import jax
import jax.numpy as jnp
from jax import lax
from jax.experimental import pallas as pl
from jax.experimental.pallas import tpu as pltpu
from jax.sharding import PartitionSpec as P

EPS = 1e-6
F32, BF16 = jnp.float32, jnp.bfloat16
MESH = pl.DeviceIdType.MESH
CORES = 2
STEPS = {"xp": (1, 0), "xm": (-1, 0), "yp": (0, 1), "ym": (0, -1)}


def phases():
    out = [[] for _ in range(5)]
    for to, (sx, sy) in STEPS.items():
        s, turned = sx + sy, "B" if sx else "A"
        sign = "plus" if s > 0 else "minus"

        def along(d, e, sx=sx):
            return (d, e) if sx else (e, d)

        out[0] += [(to, (0, 0), "all", "all")]
        out[1] += [(to, along(-s, 0), "all", sign)] + [(to, along(0, e), turned, "all") for e in (-1, 1)]
        out[2] += [(to, along(0, 2), turned, "all")] + [(to, along(-s, e), turned, sign) for e in (-1, 1)]
        out[3] += [(to, along(-s, 2), turned, sign)]
    for part in out:
        n = len(part) // 4
        part[:] = [part[link * n + i] for i in range(n) for link in range(4)]
    for dx in range(-1, 3):
        for dy in range(-1, 3):
            out[abs(dx) + abs(dy)].append(("sib", (dx, dy), "all", "all"))
    return out


PHASES = phases()
SENT = ((5, 1), (5, 2), (5, 2), (5, 1), (1, 1))
FIRST = [sum(len(p) for p in PHASES[:i]) for i in range(len(PHASES) + 1)]
BEFORE = "s10 s01 s20"
SLOTS = (
    ("c00", "s11", "s30", "s02 c01", "s21", "s12", "s40 c02", "s31 s03", "026"),
    ("s22 c10 c20", "s41 s13", "s32", "c11 c21", "s04", "s23", "s42 c12 c22", "", "026"),
    ("s14 c30", "s33 s05", "c31", "s24", "s43 s15", "", "s34 c32", "s25", "0"),
    ("s44 c40 c50", "s35", "", "c41 c51", "", "", "s45 c42 c52", "", "026"),
)
PARTS = 2


def dot(a, b):
    return jnp.dot(a, b, preferred_element_type=F32)


def kernel(head, each, x_hbm, *refs):
    (wq_ref, wk_ref, wv_ref, wo_ref, wup_ref, wdown_ref, bq_ref, bv_ref, bup_ref,
     gain1_ref, shift1_ref, bo_ref, gain2_ref, shift2_ref, bdown_ref,
     out_ref, ga_ref, gu_ref, gd_ref,
     x_ref, h_ref, acc_ref, qkv_ref, o_ref, u_ref, own_a, own_u, own_d, wbuf_a, wbuf_u, wbuf_d, own_vec, own_bias, vecs, biases,
     send_sem, recv_sem, in_sem, own_sem, load_sem, vec_send, vec_recv, bias_send, bias_recv,
     xin_send, xin_recv, o1_send, o1_recv, ring_send, ring_recv) = refs
    layers, tys, txs = ga_ref.shape[:3]
    groups = 3 * layers
    owns, gathered = (own_a, own_u, own_d), (ga_ref, gu_ref, gd_ref)
    nx, ny = tys // CORES, txs
    tokens, part = x_ref.shape[1:]
    me_t, me_s = lax.axis_index("tx"), lax.axis_index("ty")
    my_x, my_c = me_s // CORES, lax.rem(me_s, CORES)
    sibling = my_x * CORES + (CORES - 1 - my_c)
    worker = me_t < each

    def ty_at(dx):
        return lax.rem(my_x + dx + nx, nx) * CORES + my_c

    def tx_at(dy):
        return lax.rem(me_t + dy + ny, ny)

    def target(to):
        if to == "sib":
            return {"ty": sibling}
        dx, dy = STEPS[to]
        return {"ty": ty_at(dx)} if dx else {"tx": tx_at(dy)}

    fills = [pltpu.make_async_copy(w, own_a.at[:, i], in_sem.at[i]) for i, w in enumerate((wq_ref, wk_ref, wv_ref, wo_ref))]
    fills += [pltpu.make_async_copy(wup_ref, own_u, in_sem.at[4]), pltpu.make_async_copy(wdown_ref, own_d, in_sem.at[5])]
    for c in fills:
        c.start()
    for i, ref in enumerate((gain1_ref, shift1_ref, bo_ref, gain2_ref, shift2_ref, bdown_ref)):
        own_vec[i] = ref[...]
    pair = o_ref.shape[1]
    own_bias[:, pl.ds(0, pair)] = jnp.concatenate([bq_ref[:, i, :] for i in range(pair // head)], axis=-1)
    own_bias[:, pl.ds(pair, pair)] = jnp.zeros((layers, pair), F32)
    own_bias[:, pl.ds(2 * pair, pair)] = jnp.concatenate([bv_ref[:, i, :] for i in range(pair // head)], axis=-1)
    own_bias[:, pl.ds(3 * pair, bup_ref.shape[1])] = bup_ref[...]

    barrier = pltpu.get_barrier_semaphore()
    for k in range(1, txs):
        pl.semaphore_signal(barrier, inc=1, device_id={"tx": tx_at(k)}, device_id_type=MESH)
    for k in range(1, tys):
        pl.semaphore_signal(barrier, inc=1, device_id={"ty": lax.rem(me_s + k, tys)}, device_id_type=MESH)
    pl.semaphore_wait(barrier, txs - 1 + tys - 1)

    def halves(g):
        cut = 1 if g == 0 else 2
        return {"all": pl.ds(0, 4), "A": pl.ds(0, cut), "B": pl.ds(cut, 4 - cut)}

    signs = {"all": pl.ds(0, 2), "plus": pl.ds(0, 1), "minus": pl.ds(1, 1)}

    def piece(g, ty, tx, half, sign):
        return gathered[g % 3].at[g // 3, ty, tx, halves(g)[half], signs[sign]]

    def copy(phase, i, g):
        to, (dx, dy), half, sign = PHASES[phase][i]
        place = piece(g, ty_at(dx), tx_at(dy), half, sign)
        return pltpu.make_async_remote_copy(
            src_ref=owns[g % 3].at[g // 3] if phase == 0 else place, dst_ref=place, send_sem=send_sem.at[g, phase],
            recv_sem=recv_sem.at[g, FIRST[phase] + i], device_id=target(to), device_id_type=MESH)

    def arrival(phase, i, g):
        to, (dx, dy), half, sign = PHASES[phase][i]
        if to == "sib":
            ty = lax.rem(my_x + dx + nx, nx) * CORES + (CORES - 1 - my_c)
            place = piece(g, ty, tx_at(dy), half, sign)
        else:
            sx, sy = STEPS[to]
            place = piece(g, ty_at(dx - sx), tx_at(dy - sy), half, sign)
        return pltpu.make_async_remote_copy(
            src_ref=place, dst_ref=place, send_sem=send_sem.at[g, phase],
            recv_sem=recv_sem.at[g, FIRST[phase] + i], device_id=target(to), device_id_type=MESH)

    def event(kind, first, second):
        with jax.named_scope(f"{kind}_{first}_{second}"):
            first, second = int(first), int(second)
            if kind == "c":
                for phase in range(5):
                    for i, (to, (dx, _), _, _) in enumerate(PHASES[phase]):
                        if to == "sib" and abs(dx) == second:
                            arrival(phase, i, first).wait_recv()
                return
            phase, g = first, second
            if phase:
                for i, c in enumerate(PHASES[phase - 1]):
                    if c[0] != "sib":
                        arrival(phase - 1, i, g).wait_recv()
            for i in range(len(PHASES[phase])):
                copy(phase, i, g).start()

    for c in fills:
        c.wait()
    event("s", 0, 0)
    keep = [pltpu.make_async_copy(owns[i], gathered[i].at[:, me_s, me_t], own_sem.at[i]) for i in range(3)]
    for c in keep:
        c.start()

    def x_copy(j):
        return pltpu.make_async_remote_copy(
            src_ref=x_hbm.at[me_s * each + j], dst_ref=x_ref.at[me_t], send_sem=xin_send.at[j],
            recv_sem=xin_recv.at[me_t], device_id={"tx": j}, device_id_type=MESH)

    def x_local():
        return pltpu.make_async_copy(x_hbm.at[me_s * each + me_t], x_ref.at[me_t], xin_recv.at[me_t])

    for j in range(each):
        @pl.when(me_t != j)
        def _():
            x_copy(j).start()

        @pl.when(me_t == j)
        def _():
            x_local().start()

    def vec_copy(k):
        return pltpu.make_async_remote_copy(
            src_ref=own_vec, dst_ref=vecs.at[me_t], send_sem=vec_send.at[k], recv_sem=vec_recv.at[k],
            device_id={"tx": tx_at(k)}, device_id_type=MESH)

    def bias_copy(k):
        return pltpu.make_async_remote_copy(
            src_ref=own_bias, dst_ref=biases.at[me_s], send_sem=bias_send.at[k], recv_sem=bias_recv.at[k],
            device_id={"ty": lax.rem(me_s + k, tys)}, device_id_type=MESH)

    for k in range(1, txs):
        vec_copy(k).start()
    for k in range(1, tys):
        bias_copy(k).start()
    vecs[me_t] = own_vec[...]
    biases[me_s] = own_bias[...]

    for e in BEFORE.split():
        event(*e)

    with jax.named_scope("wait_vectors"):
        for k in range(1, txs):
            vec_copy(k).wait()
        for k in range(1, tys):
            bias_copy(k).wait()
        for c in keep:
            c.wait()

    @pl.when(worker)
    def _():
        with jax.named_scope("wait_x"):
            for m in range(txs):
                pltpu.make_async_copy(x_hbm.at[0], x_ref.at[m], xin_recv.at[m]).wait()

    def vec(row, layer):
        return jnp.concatenate([vecs[t, row, pl.ds(layer, 1), :] for t in range(txs)], axis=-1)

    def norm(gain_row, shift_row, layer):
        rows = 96

        def body(r, _):
            at = pl.ds(pl.multiple_of(r * rows, rows), rows)
            x_f = jnp.concatenate([x_ref[t, at, :] for t in range(txs)], axis=-1).astype(F32)
            mean = jnp.mean(x_f, axis=-1, keepdims=True)
            centred = x_f - mean
            variance = jnp.mean(centred * centred, axis=-1, keepdims=True)
            h = (centred * lax.rsqrt(variance + EPS) * vec(gain_row, layer) + vec(shift_row, layer)).astype(BF16)
            for t in range(txs):
                h_ref[t, at, :] = h[:, t * part:(t + 1) * part]
                acc_ref[t, at, :] = jnp.zeros((rows, part), F32)
            return 0

        lax.fori_loop(0, tokens // rows, body, 0)

    def finish(bias_row, layer, start, count):
        rows = 96

        def body(r, _):
            at = pl.ds(pl.multiple_of(start + r * rows, rows), rows)
            for t in range(txs):
                bias = vecs[t, bias_row, pl.ds(layer, 1), :]
                x_ref[t, at, :] = (x_ref[t, at, :].astype(F32) + acc_ref[t, at, :] + bias).astype(BF16)
            return 0

        lax.fori_loop(0, count // rows, body, 0)

    def column(step):
        region = (step // 2 + 1) // 2
        near = lax.rem(region, 2)
        ring = near * (1 + lax.rem(step, 2)) + 3 * (region // 2)
        core = (1 - near) * lax.rem(step, 2) + near * (step // 2 - 1)
        return lax.rem(my_x + ring + ring // 2 - 2 * (ring // 3), nx) * CORES + lax.rem(my_c + core, CORES)

    def loads(kinds, layer, step):
        bufs = (wbuf_a, wbuf_u, wbuf_d)
        return [pltpu.make_async_copy(gathered[k].at[layer, column(step)], bufs[k].at[step], load_sem.at[k, step]) for k in kinds]

    def run(slots, kinds, layer, body):
        def step_body(step, _):
            for s in range(tys if slots else 0):
                @pl.when(step == s)
                def _(s=s, events=slots[s].split(), late=slots[tys]):
                    for e in events:
                        if e[0] == "s":
                            event(*e)
                    if str(s) in late:
                        @pl.when(worker)
                        def _():
                            for c in loads(kinds, layer, step):
                                c.start()
                    for e in events:
                        if e[0] == "c":
                            event(*e)
                    if s + 1 < tys and str(s + 1) not in late:
                        @pl.when(worker)
                        def _():
                            for c in loads(kinds, layer, step + 1):
                                c.start()

            @pl.when(worker)
            def _():
                if slots:
                    with jax.named_scope("wait_load"):
                        for c in loads(kinds, layer, step):
                            c.wait()
                with jax.named_scope(f"compute_{kinds[0]}_{layer}"):
                    body(column(step), step)
            return 0

        lax.fori_loop(0, tys, step_body, 0)

    def attention(layer, ty, slot):
        def project(first, columns):
            total = jnp.zeros((tokens, columns), F32)
            for t in range(txs):
                w = wbuf_a[slot, t, pl.ds(first, columns // pair)].reshape(columns, part)
                total += lax.dot_general(h_ref[t], w, (((1,), (1,)), ((), ())), preferred_element_type=F32)
            return total

        at = pl.ds(0, 2 * pair)
        qkv_ref[:, at] = (project(0, 2 * pair) + biases[ty, pl.ds(layer, 1), at]).astype(BF16)
        at = pl.ds(2 * pair, pair)
        qkv_ref[:, at] = (project(2, pair) + biases[ty, pl.ds(layer, 1), at]).astype(BF16)

        scale = head ** -0.5 * math.log2(math.e)
        chunk = 192
        for c in range(tokens // chunk):
            rows = pl.ds(c * chunk, chunk)
            outs = []
            for hd in range(pair // head):
                q = qkv_ref[rows, pl.ds(hd * head, head)]
                k = qkv_ref[:, pl.ds(pair + hd * head, head)]
                v = qkv_ref[:, pl.ds(2 * pair + hd * head, head)]
                s = lax.dot_general(q, k, (((1,), (1,)), ((), ())), preferred_element_type=F32)
                e = jnp.exp2((s - jnp.max(s, axis=-1, keepdims=True)) * scale)
                p = (e * (1.0 / jnp.sum(e, axis=-1, keepdims=True))).astype(BF16)
                outs.append(dot(p, v))
            o_ref[rows, :] = jnp.concatenate(outs, axis=-1).astype(BF16)

        for t in range(txs):
            acc_ref[t] += dot(o_ref[...], wbuf_a[slot, t, 3].reshape(pair, part))

    def mlp(layer, start, count, ty, slot):
        rows = pl.ds(start, count)
        hidden = u_ref.shape[1]
        for n in range(hidden // part):
            at = pl.ds(n * part, part)
            total = jnp.zeros((count, part), F32)
            for t in range(txs):
                total += dot(h_ref[t, rows, :], wbuf_u[slot, t, :, :, :, at].reshape(part, part))
            bias = biases[ty, pl.ds(layer, 1), pl.ds(3 * pair + n * part, part)]
            u_ref[rows, at] = jax.nn.gelu(total + bias, approximate=True).astype(BF16)
        for t in range(txs):
            acc_ref[t, rows, :] += dot(u_ref[rows, :], wbuf_d[slot, t].reshape(hidden, part))

    def at_work(scope, *calls):
        @pl.when(worker)
        def _():
            with jax.named_scope(scope):
                for f, *args in calls:
                    f(*args)

    each_part = tokens // PARTS
    for layer in range(layers):
        last = layer == layers - 1
        at_work("norm", (norm, 0, 1, layer))
        run(SLOTS[2 * layer], (0,), layer, functools.partial(attention, layer))
        at_work("finish_norm", (finish, 2, layer, 0, tokens), (norm, 3, 4, layer))
        if not last:
            run(SLOTS[2 * layer + 1], (1, 2), layer, functools.partial(mlp, layer, 0, tokens))
            at_work("finish", (finish, 5, layer, 0, tokens))

    def o1_copy(k, r):
        rows = pl.ds(r * each_part, each_part)
        return pltpu.make_async_remote_copy(
            src_ref=x_ref.at[tx_at(k), rows], dst_ref=out_ref.at[me_s * each + me_t, rows], send_sem=o1_send.at[r, k],
            recv_sem=o1_recv.at[r, me_t], device_id={"tx": tx_at(k)}, device_id_type=MESH)

    def keep_own(r):
        rows = pl.ds(r * each_part, each_part)
        pltpu.make_async_copy(x_ref.at[me_t, rows], out_ref.at[me_s * each + me_t, rows], o1_recv.at[r, me_t]).start()

    def wait_slice(m, r):
        rows = pl.ds(r * each_part, each_part)
        pltpu.make_async_copy(x_ref.at[0, rows], out_ref.at[me_s * each + m, rows], o1_recv.at[r, m]).wait()

    def mlp_part(r):
        run(SLOTS[2 * layers - 1] if r == 0 else (), (1, 2), layers - 1, functools.partial(mlp, layers - 1, r * each_part, each_part))
        at_work("finish", (finish, 5, layers - 1, r * each_part, each_part))

        @pl.when(worker)
        def _():
            for k in range(1, txs):
                o1_copy(k, r).start()
            keep_own(r)

    ring = (("xp", 0, 0, 2), ("xm", 0, 0, 2), ("sib", 0, 0, 2),
            ("xp", -1, 0, 1), ("xm", 1, 1, 1), ("sib", -1, 0, 2), ("sib", 1, 0, 2), ("sib", 2, 0, 2))

    def ring_place(kind, ty, m, r):
        first, count = ring[kind][2:]
        return out_ref.at[ty * each + m, pl.ds(r * each_part + first * each_part // 2, count * each_part // 2)]

    def ring_op(kind, place, m, r):
        return pltpu.make_async_remote_copy(
            src_ref=place, dst_ref=place, send_sem=ring_send.at[kind, r * each + m], recv_sem=ring_recv.at[kind, r * each + m],
            device_id=target(ring[kind][0]), device_id_type=MESH)

    def ring_copy(kind, m, r):
        return ring_op(kind, ring_place(kind, ty_at(ring[kind][1]), m, r), m, r)

    def ring_arrival(kind, m, r):
        to, dx = ring[kind][:2]
        if to == "sib":
            ty = lax.rem(my_x + dx + nx, nx) * CORES + (CORES - 1 - my_c)
        else:
            ty = ty_at(dx - STEPS[to][0])
        return ring_op(kind, ring_place(kind, ty, m, r), m, r)

    pieces = [(m, r) for r in range(PARTS) for m in range(each)]

    def spread(m, r):
        with jax.named_scope(f"wait_slice_{m}_{r}"):
            wait_slice(m, r)
        for kind in (0, 1, 2):
            ring_copy(kind, m, r).start()

    def pass_on(m, r):
        with jax.named_scope(f"wait_near_{m}_{r}"):
            ring_arrival(0, m, r).wait_recv()
            ring_copy(3, m, r).start()
            ring_copy(5, m, r).start()
            ring_arrival(1, m, r).wait_recv()
            ring_copy(4, m, r).start()
            ring_copy(6, m, r).start()

    def hand_over(m, r):
        with jax.named_scope(f"wait_far_{m}_{r}"):
            ring_arrival(3, m, r).wait_recv()
            ring_arrival(4, m, r).wait_recv()
        ring_copy(7, m, r).start()

    for r in range(PARTS + 3):
        if r < PARTS:
            mlp_part(r)
        for m in range(each):
            for stage, delay in ((spread, 1), (pass_on, 2), (hand_over, 3)):
                if 0 <= r - delay < PARTS:
                    stage(m, r - delay)
    with jax.named_scope("wait_core"):
        for m, r in pieces:
            for kind in (2, 5, 6, 7):
                ring_arrival(kind, m, r).wait_recv()

    for m, r in pieces:
        for kind in range(len(ring)):
            ring_copy(kind, m, r).wait_send()
    for j in range(each):
        @pl.when(me_t != j)
        def _():
            x_copy(j).wait_send()

    @pl.when(worker)
    def _():
        for r in range(PARTS):
            for k in range(1, txs):
                o1_copy(k, r).wait_send()
    for g in range(groups):
        for phase, (a, b) in enumerate(SENT):
            place = gathered[g % 3].at[g // 3, pl.ds(0, a), pl.ds(0, b)]
            pltpu.make_async_remote_copy(
                src_ref=place, dst_ref=place, send_sem=send_sem.at[g, phase], recv_sem=recv_sem.at[g, 0],
                device_id={"ty": sibling}, device_id_type=MESH).wait_send()


def solution(mesh):
    txs, tys = mesh.shape["tx"], mesh.shape["ty"]
    act_spec = P("dp", None, "tx")
    vec_tx = P(None, "tx")
    proj_spec = P(None, "tx", "ty", None)
    head_vec = P(None, "ty", None)
    in_specs = (act_spec, vec_tx, vec_tx, proj_spec, head_vec, proj_spec, proj_spec, head_vec,
                P(None, "ty", None, "tx"), vec_tx, vec_tx, vec_tx,
                P(None, "tx", "ty"), P(None, "ty"), P(None, "ty", "tx"), vec_tx)

    def local_fn(x_in, ln1_gain, ln1_bias, w_q, b_q, w_k, w_v, b_v, w_o, b_o, ln2_gain, ln2_bias, w_up, b_up, w_down, b_down):
        layers, depth, heads, head = w_q.shape
        imgs, tokens, part = x_in.shape
        hidden = w_up.shape[2]
        each, pair = imgs // tys, heads * head
        assert tys == 4 * CORES and txs == 4 and 4 * pair == hidden and depth == part and hidden % part == 0 and each < txs

        tall, wide = (4, 2, hidden // 8, part), (4, 2, depth // 8, hidden)
        wq, wk, wv = (w.transpose(0, 2, 3, 1).reshape((layers,) + tall[1:]) for w in (w_q, w_k, w_v))
        wo = w_o.reshape((layers,) + tall[1:])

        vmem = pl.BlockSpec(memory_space=pltpu.VMEM)
        hbm = pl.BlockSpec(memory_space=pl.ANY)
        dma = pltpu.SemaphoreType.DMA

        def buf(lead, shape):
            return pltpu.VMEM(lead + shape, BF16)

        out, *_ = pl.pallas_call(
            functools.partial(kernel, head, each),
            out_shape=(jax.ShapeDtypeStruct(x_in.shape, BF16),
                       jax.ShapeDtypeStruct((layers, tys, txs) + tall, BF16),
                       jax.ShapeDtypeStruct((layers, tys, txs) + wide, BF16),
                       jax.ShapeDtypeStruct((layers, tys, txs) + tall, BF16)),
            in_specs=[hbm] * 7 + [vmem] * 9,
            out_specs=(hbm,) * 4,
            scratch_shapes=[
                buf((txs,), (tokens, part)), buf((txs,), (tokens, part)), pltpu.VMEM((txs, tokens, part), F32),
                buf((), (tokens, 3 * pair)), buf((), (tokens, pair)), buf((), (tokens, hidden)),
                buf((layers,), tall), buf((layers,), wide), buf((layers,), tall),
                buf((tys, txs), tall), buf((tys, txs), wide), buf((tys, txs), tall),
                pltpu.VMEM((6, layers, part), F32), pltpu.VMEM((layers, 3 * pair + hidden), F32),
                pltpu.VMEM((txs, 6, layers, part), F32), pltpu.VMEM((tys, layers, 3 * pair + hidden), F32),
                dma((3 * layers, 5)), dma((3 * layers, FIRST[-1])), dma((6,)), dma((3,)), dma((3, tys)),
                dma((txs,)), dma((txs,)), dma((tys,)), dma((tys,)),
                dma((each,)), dma((txs,)), dma((PARTS, txs)), dma((PARTS, txs)), dma((8, PARTS * each)), dma((8, PARTS * each)),
            ],
            compiler_params=pltpu.CompilerParams(collective_id=0, has_side_effects=True, vmem_limit_bytes=60 << 20),
            cost_estimate=pl.CostEstimate(flops=80_000_000_000, bytes_accessed=150_000_000, transcendentals=20_000_000),
            name="encoder",
        )(x_in, wq, wk, wv, wo, w_up.reshape((layers,) + wide), w_down.reshape((layers,) + tall),
          b_q, b_v, b_up, ln1_gain, ln1_bias, b_o, ln2_gain, ln2_bias, b_down)
        return out

    return jax.shard_map(local_fn, mesh=mesh, in_specs=in_specs, out_specs=act_spec, check_vma=False)
```

```python
import functools
import math

import jax
import jax.numpy as jnp
from jax import lax
from jax.experimental import pallas as pl
from jax.experimental.pallas import tpu as pltpu
from jax.sharding import PartitionSpec as P

EPS = 1e-6
F32, BF16 = jnp.float32, jnp.bfloat16
MESH = pl.DeviceIdType.MESH
CORES = 2
STEPS = {"xp": (1, 0), "xm": (-1, 0), "yp": (0, 1), "ym": (0, -1)}


def phases():
    out = [[] for _ in range(5)]
    for to, (sx, sy) in STEPS.items():
        s, turned = sx + sy, "B" if sx else "A"
        sign = "plus" if s > 0 else "minus"

        def along(d, e, sx=sx):
            return (d, e) if sx else (e, d)

        out[0] += [(to, (0, 0), "all", "all")]
        out[1] += [(to, along(-s, 0), "all", sign)] + [(to, along(0, e), turned, "all") for e in (-1, 1)]
        out[2] += [(to, along(0, 2), turned, "all")] + [(to, along(-s, e), turned, sign) for e in (-1, 1)]
        out[3] += [(to, along(-s, 2), turned, sign)]
    for part in out:
        n = len(part) // 4
        part[:] = [part[link * n + i] for i in range(n) for link in range(4)]
    for dx in range(-1, 3):
        for dy in range(-1, 3):
            out[abs(dx) + abs(dy)].append(("sib", (dx, dy), "all", "all"))
    return out


PHASES = phases()
SENT = ((5, 1), (5, 2), (5, 2), (5, 1), (1, 1))
FIRST = [sum(len(p) for p in PHASES[:i]) for i in range(len(PHASES) + 1)]
BEFORE = "s10 s01 s20"
SLOTS = (
    ("c00", "s11", "s30", "s02 c01", "s21", "s12", "s40 c02", "s31 s03", "026"),
    ("s22 c10 c20", "s41 s13", "s32", "c11 c21", "s04", "s23", "s42 c12 c22", "", "026"),
    ("s14 c30", "s33 s05", "c31", "s24", "s43 s15", "", "s34 c32", "s25", "0"),
    ("s44 c40 c50", "s35", "", "c41 c51", "", "", "s45 c42 c52", "", "026"),
)
PARTS = 3


def dot(a, b):
    return jnp.dot(a, b, preferred_element_type=F32)


def kernel(head, each, x_hbm, *refs):
    (wq_ref, wk_ref, wv_ref, wo_ref, wup_ref, wdown_ref, bq_ref, bv_ref, bup_ref,
     gain1_ref, shift1_ref, bo_ref, gain2_ref, shift2_ref, bdown_ref,
     out_ref, ga_ref, gu_ref, gd_ref,
     x_ref, h_ref, acc_ref, qkv_ref, o_ref, u_ref, own_a, own_u, own_d, wbuf_a, wbuf_u, wbuf_d, own_vec, own_bias, vecs, biases,
     send_sem, recv_sem, in_sem, own_sem, load_sem, vec_send, vec_recv, bias_send, bias_recv,
     xin_send, xin_recv, o1_send, o1_recv, ring_send, ring_recv) = refs
    layers, tys, txs = ga_ref.shape[:3]
    groups = 3 * layers
    owns, gathered = (own_a, own_u, own_d), (ga_ref, gu_ref, gd_ref)
    nx, ny = tys // CORES, txs
    tokens, part = x_ref.shape[1:]
    me_t, me_s = lax.axis_index("tx"), lax.axis_index("ty")
    my_x, my_c = me_s // CORES, lax.rem(me_s, CORES)
    sibling = my_x * CORES + (CORES - 1 - my_c)
    worker = me_t < each

    def ty_at(dx):
        return lax.rem(my_x + dx + nx, nx) * CORES + my_c

    def tx_at(dy):
        return lax.rem(me_t + dy + ny, ny)

    def target(to):
        if to == "sib":
            return {"ty": sibling}
        dx, dy = STEPS[to]
        return {"ty": ty_at(dx)} if dx else {"tx": tx_at(dy)}

    fills = [pltpu.make_async_copy(w, own_a.at[:, i], in_sem.at[i]) for i, w in enumerate((wq_ref, wk_ref, wv_ref, wo_ref))]
    fills += [pltpu.make_async_copy(wup_ref, own_u, in_sem.at[4]), pltpu.make_async_copy(wdown_ref, own_d, in_sem.at[5])]
    for c in fills:
        c.start()
    for i, ref in enumerate((gain1_ref, shift1_ref, bo_ref, gain2_ref, shift2_ref, bdown_ref)):
        own_vec[i] = ref[...]
    pair = o_ref.shape[1]
    own_bias[:, pl.ds(0, pair)] = jnp.concatenate([bq_ref[:, i, :] for i in range(pair // head)], axis=-1)
    own_bias[:, pl.ds(pair, pair)] = jnp.zeros((layers, pair), F32)
    own_bias[:, pl.ds(2 * pair, pair)] = jnp.concatenate([bv_ref[:, i, :] for i in range(pair // head)], axis=-1)
    own_bias[:, pl.ds(3 * pair, bup_ref.shape[1])] = bup_ref[...]

    barrier = pltpu.get_barrier_semaphore()
    for k in range(1, txs):
        pl.semaphore_signal(barrier, inc=1, device_id={"tx": tx_at(k)}, device_id_type=MESH)
    for k in range(1, tys):
        pl.semaphore_signal(barrier, inc=1, device_id={"ty": lax.rem(me_s + k, tys)}, device_id_type=MESH)
    pl.semaphore_wait(barrier, txs - 1 + tys - 1)

    def halves(g):
        cut = 1 if g == 0 else 2
        return {"all": pl.ds(0, 4), "A": pl.ds(0, cut), "B": pl.ds(cut, 4 - cut)}

    signs = {"all": pl.ds(0, 2), "plus": pl.ds(0, 1), "minus": pl.ds(1, 1)}

    def piece(g, ty, tx, half, sign):
        return gathered[g % 3].at[g // 3, ty, tx, halves(g)[half], signs[sign]]

    def copy(phase, i, g):
        to, (dx, dy), half, sign = PHASES[phase][i]
        place = piece(g, ty_at(dx), tx_at(dy), half, sign)
        return pltpu.make_async_remote_copy(
            src_ref=owns[g % 3].at[g // 3] if phase == 0 else place, dst_ref=place, send_sem=send_sem.at[g, phase],
            recv_sem=recv_sem.at[g, FIRST[phase] + i], device_id=target(to), device_id_type=MESH)

    def arrival(phase, i, g):
        to, (dx, dy), half, sign = PHASES[phase][i]
        if to == "sib":
            ty = lax.rem(my_x + dx + nx, nx) * CORES + (CORES - 1 - my_c)
            place = piece(g, ty, tx_at(dy), half, sign)
        else:
            sx, sy = STEPS[to]
            place = piece(g, ty_at(dx - sx), tx_at(dy - sy), half, sign)
        return pltpu.make_async_remote_copy(
            src_ref=place, dst_ref=place, send_sem=send_sem.at[g, phase],
            recv_sem=recv_sem.at[g, FIRST[phase] + i], device_id=target(to), device_id_type=MESH)

    def event(kind, first, second):
        with jax.named_scope(f"{kind}_{first}_{second}"):
            first, second = int(first), int(second)
            if kind == "c":
                for phase in range(5):
                    for i, (to, (dx, _), _, _) in enumerate(PHASES[phase]):
                        if to == "sib" and abs(dx) == second:
                            arrival(phase, i, first).wait_recv()
                return
            phase, g = first, second
            if phase:
                for i, c in enumerate(PHASES[phase - 1]):
                    if c[0] != "sib":
                        arrival(phase - 1, i, g).wait_recv()
            for i in range(len(PHASES[phase])):
                copy(phase, i, g).start()

    for c in fills:
        c.wait()
    event("s", 0, 0)
    keep = [pltpu.make_async_copy(owns[i], gathered[i].at[:, me_s, me_t], own_sem.at[i]) for i in range(3)]
    for c in keep:
        c.start()

    def x_copy(j):
        return pltpu.make_async_remote_copy(
            src_ref=x_hbm.at[me_s * each + j], dst_ref=x_ref.at[me_t], send_sem=xin_send.at[j],
            recv_sem=xin_recv.at[me_t], device_id={"tx": j}, device_id_type=MESH)

    def x_local():
        return pltpu.make_async_copy(x_hbm.at[me_s * each + me_t], x_ref.at[me_t], xin_recv.at[me_t])

    for j in range(each):
        @pl.when(me_t != j)
        def _():
            x_copy(j).start()

        @pl.when(me_t == j)
        def _():
            x_local().start()

    def vec_copy(k):
        return pltpu.make_async_remote_copy(
            src_ref=own_vec, dst_ref=vecs.at[me_t], send_sem=vec_send.at[k], recv_sem=vec_recv.at[k],
            device_id={"tx": tx_at(k)}, device_id_type=MESH)

    def bias_copy(k):
        return pltpu.make_async_remote_copy(
            src_ref=own_bias, dst_ref=biases.at[me_s], send_sem=bias_send.at[k], recv_sem=bias_recv.at[k],
            device_id={"ty": lax.rem(me_s + k, tys)}, device_id_type=MESH)

    for k in range(1, txs):
        vec_copy(k).start()
    for k in range(1, tys):
        bias_copy(k).start()
    vecs[me_t] = own_vec[...]
    biases[me_s] = own_bias[...]

    for e in BEFORE.split():
        event(*e)

    with jax.named_scope("wait_vectors"):
        for k in range(1, txs):
            vec_copy(k).wait()
        for k in range(1, tys):
            bias_copy(k).wait()
        for c in keep:
            c.wait()

    @pl.when(worker)
    def _():
        with jax.named_scope("wait_x"):
            for m in range(txs):
                pltpu.make_async_copy(x_hbm.at[0], x_ref.at[m], xin_recv.at[m]).wait()

    def vec(row, layer):
        return jnp.concatenate([vecs[t, row, pl.ds(layer, 1), :] for t in range(txs)], axis=-1)

    def norm(gain_row, shift_row, layer):
        rows = 96

        def body(r, _):
            at = pl.ds(pl.multiple_of(r * rows, rows), rows)
            x_f = jnp.concatenate([x_ref[t, at, :] for t in range(txs)], axis=-1).astype(F32)
            mean = jnp.mean(x_f, axis=-1, keepdims=True)
            centred = x_f - mean
            variance = jnp.mean(centred * centred, axis=-1, keepdims=True)
            h = (centred * lax.rsqrt(variance + EPS) * vec(gain_row, layer) + vec(shift_row, layer)).astype(BF16)
            for t in range(txs):
                h_ref[t, at, :] = h[:, t * part:(t + 1) * part]
                acc_ref[t, at, :] = jnp.zeros((rows, part), F32)
            return 0

        lax.fori_loop(0, tokens // rows, body, 0)

    def finish(bias_row, layer, start, count):
        rows = 96

        def body(r, _):
            at = pl.ds(pl.multiple_of(start + r * rows, rows), rows)
            for t in range(txs):
                bias = vecs[t, bias_row, pl.ds(layer, 1), :]
                x_ref[t, at, :] = (x_ref[t, at, :].astype(F32) + acc_ref[t, at, :] + bias).astype(BF16)
            return 0

        lax.fori_loop(0, count // rows, body, 0)

    def column(step):
        region = (step // 2 + 1) // 2
        near = lax.rem(region, 2)
        ring = near * (1 + lax.rem(step, 2)) + 3 * (region // 2)
        core = (1 - near) * lax.rem(step, 2) + near * (step // 2 - 1)
        return lax.rem(my_x + ring + ring // 2 - 2 * (ring // 3), nx) * CORES + lax.rem(my_c + core, CORES)

    def loads(kinds, layer, step):
        bufs = (wbuf_a, wbuf_u, wbuf_d)
        return [pltpu.make_async_copy(gathered[k].at[layer, column(step)], bufs[k].at[step], load_sem.at[k, step]) for k in kinds]

    def run(slots, kinds, layer, body):
        def step_body(step, _):
            for s in range(tys if slots else 0):
                @pl.when(step == s)
                def _(s=s, events=slots[s].split(), late=slots[tys]):
                    for e in events:
                        if e[0] == "s":
                            event(*e)
                    if str(s) in late:
                        @pl.when(worker)
                        def _():
                            for c in loads(kinds, layer, step):
                                c.start()
                    for e in events:
                        if e[0] == "c":
                            event(*e)
                    if s + 1 < tys and str(s + 1) not in late:
                        @pl.when(worker)
                        def _():
                            for c in loads(kinds, layer, step + 1):
                                c.start()

            @pl.when(worker)
            def _():
                if slots:
                    with jax.named_scope("wait_load"):
                        for c in loads(kinds, layer, step):
                            c.wait()
                with jax.named_scope(f"compute_{kinds[0]}_{layer}"):
                    body(column(step), step)
            return 0

        lax.fori_loop(0, tys, step_body, 0)

    def attention(layer, ty, slot):
        def project(first, columns):
            total = jnp.zeros((tokens, columns), F32)
            for t in range(txs):
                w = wbuf_a[slot, t, pl.ds(first, columns // pair)].reshape(columns, part)
                total += lax.dot_general(h_ref[t], w, (((1,), (1,)), ((), ())), preferred_element_type=F32)
            return total

        at = pl.ds(0, 2 * pair)
        qkv_ref[:, at] = (project(0, 2 * pair) + biases[ty, pl.ds(layer, 1), at]).astype(BF16)
        at = pl.ds(2 * pair, pair)
        qkv_ref[:, at] = (project(2, pair) + biases[ty, pl.ds(layer, 1), at]).astype(BF16)

        scale = head ** -0.5 * math.log2(math.e)
        chunk = 192
        for c in range(tokens // chunk):
            rows = pl.ds(c * chunk, chunk)
            outs = []
            for hd in range(pair // head):
                q = qkv_ref[rows, pl.ds(hd * head, head)]
                k = qkv_ref[:, pl.ds(pair + hd * head, head)]
                v = qkv_ref[:, pl.ds(2 * pair + hd * head, head)]
                s = lax.dot_general(q, k, (((1,), (1,)), ((), ())), preferred_element_type=F32)
                e = jnp.exp2((s - jnp.max(s, axis=-1, keepdims=True)) * scale)
                p = (e * (1.0 / jnp.sum(e, axis=-1, keepdims=True))).astype(BF16)
                outs.append(dot(p, v))
            o_ref[rows, :] = jnp.concatenate(outs, axis=-1).astype(BF16)

        for t in range(txs):
            acc_ref[t] += dot(o_ref[...], wbuf_a[slot, t, 3].reshape(pair, part))

    def mlp(layer, start, count, ty, slot):
        rows = pl.ds(start, count)
        hidden = u_ref.shape[1]
        for n in range(hidden // part):
            at = pl.ds(n * part, part)
            total = jnp.zeros((count, part), F32)
            for t in range(txs):
                total += dot(h_ref[t, rows, :], wbuf_u[slot, t, :, :, :, at].reshape(part, part))
            bias = biases[ty, pl.ds(layer, 1), pl.ds(3 * pair + n * part, part)]
            u_ref[rows, at] = jax.nn.gelu(total + bias, approximate=True).astype(BF16)
        for t in range(txs):
            acc_ref[t, rows, :] += dot(u_ref[rows, :], wbuf_d[slot, t].reshape(hidden, part))

    def at_work(scope, *calls):
        @pl.when(worker)
        def _():
            with jax.named_scope(scope):
                for f, *args in calls:
                    f(*args)

    each_part = tokens // PARTS
    for layer in range(layers):
        last = layer == layers - 1
        at_work("norm", (norm, 0, 1, layer))
        run(SLOTS[2 * layer], (0,), layer, functools.partial(attention, layer))
        at_work("finish_norm", (finish, 2, layer, 0, tokens), (norm, 3, 4, layer))
        if not last:
            run(SLOTS[2 * layer + 1], (1, 2), layer, functools.partial(mlp, layer, 0, tokens))
            at_work("finish", (finish, 5, layer, 0, tokens))

    def o1_copy(k, r):
        rows = pl.ds(r * each_part, each_part)
        return pltpu.make_async_remote_copy(
            src_ref=x_ref.at[tx_at(k), rows], dst_ref=out_ref.at[me_s * each + me_t, rows], send_sem=o1_send.at[r, k],
            recv_sem=o1_recv.at[r, me_t], device_id={"tx": tx_at(k)}, device_id_type=MESH)

    def keep_own(r):
        rows = pl.ds(r * each_part, each_part)
        out_ref[me_s * each + me_t, rows, :] = x_ref[me_t, rows, :]

    def wait_slice(m, r):
        rows = pl.ds(r * each_part, each_part)

        @pl.when(me_t != m)
        def _():
            place = out_ref.at[me_s * each + m, rows]
            pltpu.make_async_remote_copy(
                src_ref=place, dst_ref=place, send_sem=o1_send.at[r, 0], recv_sem=o1_recv.at[r, m],
                device_id={"tx": m}, device_id_type=MESH).wait_recv()

    def mlp_part(r):
        run(SLOTS[2 * layers - 1] if r == 0 else (), (1, 2), layers - 1, functools.partial(mlp, layers - 1, r * each_part, each_part))
        at_work("finish", (finish, 5, layers - 1, r * each_part, each_part))

        @pl.when(worker)
        def _():
            for k in range(1, txs):
                o1_copy(k, r).start()
            keep_own(r)

    ring = (("xp", 0, 0, 2), ("xm", 0, 0, 2), ("sib", 0, 0, 2),
            ("xp", -1, 0, 1), ("xm", 1, 1, 1), ("sib", -1, 0, 2), ("sib", 1, 0, 2), ("sib", 2, 0, 2))

    def ring_place(kind, ty, m, r):
        first, count = ring[kind][2:]
        return out_ref.at[ty * each + m, pl.ds(r * each_part + first * each_part // 2, count * each_part // 2)]

    def ring_op(kind, place, m, r):
        return pltpu.make_async_remote_copy(
            src_ref=place, dst_ref=place, send_sem=ring_send.at[kind],
            recv_sem=ring_recv.at[kind, 0 if ring[kind][0] == "sib" else r * each + m],
            device_id=target(ring[kind][0]), device_id_type=MESH)

    def ring_copy(kind, m, r):
        return ring_op(kind, ring_place(kind, ty_at(ring[kind][1]), m, r), m, r)

    def ring_arrival(kind, m, r):
        to, dx = ring[kind][:2]
        if to == "sib":
            ty = lax.rem(my_x + dx + nx, nx) * CORES + (CORES - 1 - my_c)
        else:
            ty = ty_at(dx - STEPS[to][0])
        return ring_op(kind, ring_place(kind, ty, m, r), m, r)

    def spread(m, r):
        wait_slice(m, r)
        for kind in (0, 1, 2):
            ring_copy(kind, m, r).start()

    def pass_on(m, r):
        ring_arrival(0, m, r).wait_recv()
        ring_copy(3, m, r).start()
        ring_copy(5, m, r).start()
        ring_arrival(1, m, r).wait_recv()
        ring_copy(4, m, r).start()
        ring_copy(6, m, r).start()

    def hand_over(m, r):
        ring_arrival(3, m, r).wait_recv()
        ring_arrival(4, m, r).wait_recv()
        ring_copy(7, m, r).start()

    for r in range(PARTS + 3):
        if r < PARTS:
            mlp_part(r)

        def stages(m, _, r=r):
            for stage, delay in ((spread, 1), (pass_on, 2), (hand_over, 3)):
                if 0 <= r - delay < PARTS:
                    stage(m, r - delay)
            return 0

        if r:
            with jax.named_scope(f"output_{r}"):
                lax.fori_loop(0, each, stages, 0)

    def ring_total(kind):
        rows = tokens * ring[kind][3] // 2
        place = out_ref.at[pl.ds(0, each), pl.ds(0, rows)]
        return pltpu.make_async_remote_copy(
            src_ref=place, dst_ref=place, send_sem=ring_send.at[kind], recv_sem=ring_recv.at[kind, 0],
            device_id=target(ring[kind][0]), device_id_type=MESH)

    with jax.named_scope("wait_core"):
        for kind in (2, 5, 6, 7):
            ring_total(kind).wait_recv()

    for kind in range(len(ring)):
        ring_total(kind).wait_send()
    for j in range(each):
        @pl.when(me_t != j)
        def _():
            x_copy(j).wait_send()

    @pl.when(worker)
    def _():
        for r in range(PARTS):
            for k in range(1, txs):
                o1_copy(k, r).wait_send()
    for g in range(groups):
        for phase, (a, b) in enumerate(SENT):
            place = gathered[g % 3].at[g // 3, pl.ds(0, a), pl.ds(0, b)]
            pltpu.make_async_remote_copy(
                src_ref=place, dst_ref=place, send_sem=send_sem.at[g, phase], recv_sem=recv_sem.at[g, 0],
                device_id={"ty": sibling}, device_id_type=MESH).wait_send()


def solution(mesh):
    txs, tys = mesh.shape["tx"], mesh.shape["ty"]
    act_spec = P("dp", None, "tx")
    vec_tx = P(None, "tx")
    proj_spec = P(None, "tx", "ty", None)
    head_vec = P(None, "ty", None)
    in_specs = (act_spec, vec_tx, vec_tx, proj_spec, head_vec, proj_spec, proj_spec, head_vec,
                P(None, "ty", None, "tx"), vec_tx, vec_tx, vec_tx,
                P(None, "tx", "ty"), P(None, "ty"), P(None, "ty", "tx"), vec_tx)

    def local_fn(x_in, ln1_gain, ln1_bias, w_q, b_q, w_k, w_v, b_v, w_o, b_o, ln2_gain, ln2_bias, w_up, b_up, w_down, b_down):
        layers, depth, heads, head = w_q.shape
        imgs, tokens, part = x_in.shape
        hidden = w_up.shape[2]
        each, pair = imgs // tys, heads * head
        assert tys == 4 * CORES and txs == 4 and 4 * pair == hidden and depth == part and hidden % part == 0 and each < txs

        tall, wide = (4, 2, hidden // 8, part), (4, 2, depth // 8, hidden)
        wq, wk, wv = (w.transpose(0, 2, 3, 1).reshape((layers,) + tall[1:]) for w in (w_q, w_k, w_v))
        wo = w_o.reshape((layers,) + tall[1:])

        vmem = pl.BlockSpec(memory_space=pltpu.VMEM)
        hbm = pl.BlockSpec(memory_space=pl.ANY)
        dma = pltpu.SemaphoreType.DMA

        def buf(lead, shape):
            return pltpu.VMEM(lead + shape, BF16)

        out, *_ = pl.pallas_call(
            functools.partial(kernel, head, each),
            out_shape=(pltpu.VMEM(x_in.shape, BF16),
                       jax.ShapeDtypeStruct((layers, tys, txs) + tall, BF16),
                       jax.ShapeDtypeStruct((layers, tys, txs) + wide, BF16),
                       jax.ShapeDtypeStruct((layers, tys, txs) + tall, BF16)),
            in_specs=[hbm] * 7 + [vmem] * 9,
            out_specs=(vmem,) + (hbm,) * 3,
            scratch_shapes=[
                buf((txs,), (tokens, part)), buf((txs,), (tokens, part)), pltpu.VMEM((txs, tokens, part), F32),
                buf((), (tokens, 3 * pair)), buf((), (tokens, pair)), buf((), (tokens, hidden)),
                buf((layers,), tall), buf((layers,), wide), buf((layers,), tall),
                buf((tys, txs), tall), buf((tys, txs), wide), buf((tys, txs), tall),
                pltpu.VMEM((6, layers, part), F32), pltpu.VMEM((layers, 3 * pair + hidden), F32),
                pltpu.VMEM((txs, 6, layers, part), F32), pltpu.VMEM((tys, layers, 3 * pair + hidden), F32),
                dma((3 * layers, 5)), dma((3 * layers, FIRST[-1])), dma((6,)), dma((3,)), dma((3, tys)),
                dma((txs,)), dma((txs,)), dma((tys,)), dma((tys,)),
                dma((each,)), dma((txs,)), dma((PARTS, txs)), dma((PARTS, txs)), dma((8,)), dma((8, PARTS * each)),
            ],
            compiler_params=pltpu.CompilerParams(collective_id=0, has_side_effects=True, vmem_limit_bytes=52 << 20),
            cost_estimate=pl.CostEstimate(flops=80_000_000_000, bytes_accessed=150_000_000, transcendentals=20_000_000),
            name="encoder",
        )(x_in, wq, wk, wv, wo, w_up.reshape((layers,) + wide), w_down.reshape((layers,) + tall),
          b_q, b_v, b_up, ln1_gain, ln1_bias, b_o, ln2_gain, ln2_bias, b_down)
        return out

    return jax.shard_map(local_fn, mesh=mesh, in_specs=in_specs, out_specs=act_spec, check_vma=False)
```

```python
import functools
import math

import jax
import jax.numpy as jnp
from jax import lax
from jax.experimental import pallas as pl
from jax.experimental.pallas import tpu as pltpu
from jax.sharding import PartitionSpec as P

EPS = 1e-6
F32, BF16 = jnp.float32, jnp.bfloat16
MESH = pl.DeviceIdType.MESH
CORES = 2
STEPS = {"xp": (1, 0), "xm": (-1, 0), "yp": (0, 1), "ym": (0, -1)}


def phases():
    out = [[] for _ in range(5)]
    for to, (sx, sy) in STEPS.items():
        s, turned = sx + sy, "B" if sx else "A"
        sign = "plus" if s > 0 else "minus"

        def along(d, e, sx=sx):
            return (d, e) if sx else (e, d)

        out[0] += [(to, (0, 0), "all", "all")]
        out[1] += [(to, along(-s, 0), "all", sign)] + [(to, along(0, e), turned, "all") for e in (-1, 1)]
        out[2] += [(to, along(0, 2), turned, "all")] + [(to, along(-s, e), turned, sign) for e in (-1, 1)]
        out[3] += [(to, along(-s, 2), turned, sign)]
    for part in out:
        n = len(part) // 4
        part[:] = [part[link * n + i] for i in range(n) for link in range(4)]
    for dx in range(-1, 3):
        for dy in range(-1, 3):
            out[abs(dx) + abs(dy)].append(("sib", (dx, dy), "all", "all"))
    return out


PHASES = phases()
SENT = ((5, 1), (5, 2), (5, 2), (5, 1), (1, 1))
FIRST = [sum(len(p) for p in PHASES[:i]) for i in range(len(PHASES) + 1)]
BEFORE = "s10 s01 s20"
SLOTS = (
    ("l00 c00", "s11", "s30 l01", "s02 c01", "s21 l10", "s12", "s40 l02 c10 c02", "s31 s03 l11"),
    ("s22 l20 c20 c11", "s41 s13 l12", "s32 l21 c12", "c21", "s04", "s23 l30", "s42 l22 c30", "c22"),
    ("s05 s14", "s33 l31", "s15 c31", "", "s24 s43 l40 l32", "c32 c40", "s25 l50", "s34 l41 c50"),
    ("s35 l51 s44 l42", "c41 c51", "", "", "s45 l52", "", "c42 c52", ""),
)
RINGS = (((0,), (1,)), ((2, 3), (4, 5)), ((6,), (7,)))
PARTS = 3


def dot(a, b):
    return jnp.dot(a, b, preferred_element_type=F32)


def kernel(head, each, x_hbm, *refs):
    (wq_ref, wk_ref, wv_ref, wo_ref, wup_ref, wdown_ref, bq_ref, bv_ref, bup_ref,
     gain1_ref, shift1_ref, bo_ref, gain2_ref, shift2_ref, bdown_ref,
     out_ref, ga_ref, gu_ref, gd_ref,
     x_ref, h_ref, acc_ref, qkv_ref, o_ref, u_ref, own_a, own_u, own_d, wbuf_a, wbuf_u, wbuf_d, own_vec, own_bias, vecs, biases,
     send_sem, recv_sem, in_sem, own_sem, load_sem, vec_send, vec_recv, bias_send, bias_recv,
     xin_send, xin_recv, o1_send, o1_recv, ring_send, ring_recv) = refs
    layers, tys, txs = ga_ref.shape[:3]
    groups = 3 * layers
    owns, gathered = (own_a, own_u, own_d), (ga_ref, gu_ref, gd_ref)
    nx, ny = tys // CORES, txs
    tokens, part = x_ref.shape[1:]
    me_t, me_s = lax.axis_index("tx"), lax.axis_index("ty")
    my_x, my_c = me_s // CORES, lax.rem(me_s, CORES)
    sibling = my_x * CORES + (CORES - 1 - my_c)
    worker = me_t < each

    def ty_at(dx):
        return lax.rem(my_x + dx + nx, nx) * CORES + my_c

    def tx_at(dy):
        return lax.rem(me_t + dy + ny, ny)

    def target(to):
        if to == "sib":
            return {"ty": sibling}
        dx, dy = STEPS[to]
        return {"ty": ty_at(dx)} if dx else {"tx": tx_at(dy)}

    fills = [pltpu.make_async_copy(w, own_a.at[:, i], in_sem.at[i]) for i, w in enumerate((wq_ref, wk_ref, wv_ref, wo_ref))]
    fills += [pltpu.make_async_copy(wup_ref, own_u, in_sem.at[4]), pltpu.make_async_copy(wdown_ref, own_d, in_sem.at[5])]
    for c in fills:
        c.start()
    for i, ref in enumerate((gain1_ref, shift1_ref, bo_ref, gain2_ref, shift2_ref, bdown_ref)):
        own_vec[i] = ref[...]
    pair = o_ref.shape[1]
    own_bias[:, pl.ds(0, pair)] = jnp.concatenate([bq_ref[:, i, :] for i in range(pair // head)], axis=-1)
    own_bias[:, pl.ds(pair, pair)] = jnp.zeros((layers, pair), F32)
    own_bias[:, pl.ds(2 * pair, pair)] = jnp.concatenate([bv_ref[:, i, :] for i in range(pair // head)], axis=-1)
    own_bias[:, pl.ds(3 * pair, bup_ref.shape[1])] = bup_ref[...]

    barrier = pltpu.get_barrier_semaphore()
    for k in range(1, txs):
        pl.semaphore_signal(barrier, inc=1, device_id={"tx": tx_at(k)}, device_id_type=MESH)
    for k in range(1, tys):
        pl.semaphore_signal(barrier, inc=1, device_id={"ty": lax.rem(me_s + k, tys)}, device_id_type=MESH)
    pl.semaphore_wait(barrier, txs - 1 + tys - 1)

    def halves(g):
        cut = 1 if g == 0 else 2
        return {"all": pl.ds(0, 4), "A": pl.ds(0, cut), "B": pl.ds(cut, 4 - cut)}

    signs = {"all": pl.ds(0, 2), "plus": pl.ds(0, 1), "minus": pl.ds(1, 1)}

    def piece(g, ty, tx, half, sign):
        return gathered[g % 3].at[g // 3, ty, tx, halves(g)[half], signs[sign]]

    def copy(phase, i, g):
        to, (dx, dy), half, sign = PHASES[phase][i]
        place = piece(g, ty_at(dx), tx_at(dy), half, sign)
        return pltpu.make_async_remote_copy(
            src_ref=owns[g % 3].at[g // 3] if phase == 0 else place, dst_ref=place, send_sem=send_sem.at[g, phase],
            recv_sem=recv_sem.at[g, FIRST[phase] + i], device_id=target(to), device_id_type=MESH)

    def arrival(phase, i, g):
        to, (dx, dy), half, sign = PHASES[phase][i]
        if to == "sib":
            ty = lax.rem(my_x + dx + nx, nx) * CORES + (CORES - 1 - my_c)
            place = piece(g, ty, tx_at(dy), half, sign)
        else:
            sx, sy = STEPS[to]
            place = piece(g, ty_at(dx - sx), tx_at(dy - sy), half, sign)
        return pltpu.make_async_remote_copy(
            src_ref=place, dst_ref=place, send_sem=send_sem.at[g, phase],
            recv_sem=recv_sem.at[g, FIRST[phase] + i], device_id=target(to), device_id_type=MESH)

    def column(step):
        rem = lax.rem if isinstance(step, jax.Array) else lambda p, q: p % q
        region = (step // 2 + 1) // 2
        near = rem(region, 2)
        ring = near * (1 + rem(step, 2)) + 3 * (region // 2)
        core = (1 - near) * rem(step, 2) + near * (step // 2 - 1)
        return lax.rem(my_x + ring + ring // 2 - 2 * (ring // 3), nx) * CORES + lax.rem(my_c + core, CORES)

    def load(k, layer, step):
        return pltpu.make_async_copy(gathered[k].at[layer, column(step)], (wbuf_a, wbuf_u, wbuf_d)[k].at[step], load_sem.at[k, step])

    def event(kind, first, second):
        with jax.named_scope(f"{kind}_{first}_{second}"):
            first, second = int(first), int(second)
            if kind == "c":
                for phase in range(5):
                    for i, (to, (dx, _), _, _) in enumerate(PHASES[phase]):
                        if to == "sib" and abs(dx) == second:
                            arrival(phase, i, first).wait_recv()
            if kind in "cl":
                @pl.when(worker)
                def _():
                    for step in RINGS[second][kind == "c"]:
                        load(first % 3, first // 3, step).start()
                return
            phase, g = first, second
            if phase:
                for i, c in enumerate(PHASES[phase - 1]):
                    if c[0] != "sib":
                        arrival(phase - 1, i, g).wait_recv()
            for i in range(len(PHASES[phase])):
                copy(phase, i, g).start()

    for c in fills:
        c.wait()
    event("s", 0, 0)
    keep = [pltpu.make_async_copy(owns[i], gathered[i].at[:, me_s, me_t], own_sem.at[i]) for i in range(3)]
    for c in keep:
        c.start()

    def x_copy(j):
        return pltpu.make_async_remote_copy(
            src_ref=x_hbm.at[me_s * each + j], dst_ref=x_ref.at[me_t], send_sem=xin_send.at[j],
            recv_sem=xin_recv.at[me_t], device_id={"tx": j}, device_id_type=MESH)

    def x_local():
        return pltpu.make_async_copy(x_hbm.at[me_s * each + me_t], x_ref.at[me_t], xin_recv.at[me_t])

    for j in range(each):
        @pl.when(me_t != j)
        def _():
            x_copy(j).start()

        @pl.when(me_t == j)
        def _():
            x_local().start()

    def vec_copy(k):
        return pltpu.make_async_remote_copy(
            src_ref=own_vec, dst_ref=vecs.at[me_t], send_sem=vec_send.at[k], recv_sem=vec_recv.at[k],
            device_id={"tx": tx_at(k)}, device_id_type=MESH)

    def bias_copy(k):
        return pltpu.make_async_remote_copy(
            src_ref=own_bias, dst_ref=biases.at[me_s], send_sem=bias_send.at[k], recv_sem=bias_recv.at[k],
            device_id={"ty": lax.rem(me_s + k, tys)}, device_id_type=MESH)

    for k in range(1, txs):
        vec_copy(k).start()
    for k in range(1, tys):
        bias_copy(k).start()
    vecs[me_t] = own_vec[...]
    biases[me_s] = own_bias[...]

    for e in BEFORE.split():
        event(*e)

    with jax.named_scope("wait_vectors"):
        for k in range(1, txs):
            vec_copy(k).wait()
        for k in range(1, tys):
            bias_copy(k).wait()
        for c in keep:
            c.wait()

    @pl.when(worker)
    def _():
        with jax.named_scope("wait_x"):
            for m in range(txs):
                pltpu.make_async_copy(x_hbm.at[0], x_ref.at[m], xin_recv.at[m]).wait()

    def vec(row, layer):
        return jnp.concatenate([vecs[t, row, pl.ds(layer, 1), :] for t in range(txs)], axis=-1)

    def norm(gain_row, shift_row, layer):
        rows = 96

        def body(r, _):
            at = pl.ds(pl.multiple_of(r * rows, rows), rows)
            x_f = jnp.concatenate([x_ref[t, at, :] for t in range(txs)], axis=-1).astype(F32)
            mean = jnp.mean(x_f, axis=-1, keepdims=True)
            centred = x_f - mean
            variance = jnp.mean(centred * centred, axis=-1, keepdims=True)
            h = (centred * lax.rsqrt(variance + EPS) * vec(gain_row, layer) + vec(shift_row, layer)).astype(BF16)
            for t in range(txs):
                h_ref[t, at, :] = h[:, t * part:(t + 1) * part]
                acc_ref[t, at, :] = jnp.zeros((rows, part), F32)
            return 0

        lax.fori_loop(0, tokens // rows, body, 0)

    def finish(bias_row, layer, start, count):
        rows = 96

        def body(r, _):
            at = pl.ds(pl.multiple_of(start + r * rows, rows), rows)
            for t in range(txs):
                bias = vecs[t, bias_row, pl.ds(layer, 1), :]
                x_ref[t, at, :] = (x_ref[t, at, :].astype(F32) + acc_ref[t, at, :] + bias).astype(BF16)
            return 0

        lax.fori_loop(0, count // rows, body, 0)

    def run(parts, kinds, layer, body, middle=None):
        def step_body(step, _):
            for s, names in enumerate(parts):
                @pl.when(step == s)
                def _(names=names):
                    for e in names.split():
                        event(*e)

            if middle is not None:
                @pl.when(step == tys // 2)
                def _():
                    middle()

            @pl.when(worker)
            def _():
                if parts:
                    with jax.named_scope("wait_load"):
                        for k in kinds:
                            load(k, layer, step).wait()
                with jax.named_scope(f"compute_{kinds[0]}_{layer}"):
                    body(column(step), step)
            return 0

        lax.fori_loop(0, tys, step_body, 0)

    def attention(layer, ty, slot):
        def project(first, columns):
            total = jnp.zeros((tokens, columns), F32)
            for t in range(txs):
                w = wbuf_a[slot, t, pl.ds(first, columns // pair)].reshape(columns, part)
                total += lax.dot_general(h_ref[t], w, (((1,), (1,)), ((), ())), preferred_element_type=F32)
            return total

        at = pl.ds(0, 2 * pair)
        qkv_ref[:, at] = (project(0, 2 * pair) + biases[ty, pl.ds(layer, 1), at]).astype(BF16)
        at = pl.ds(2 * pair, pair)
        qkv_ref[:, at] = (project(2, pair) + biases[ty, pl.ds(layer, 1), at]).astype(BF16)

        scale = head ** -0.5 * math.log2(math.e)
        chunk = 192
        for c in range(tokens // chunk):
            rows = pl.ds(c * chunk, chunk)
            outs = []
            for hd in range(pair // head):
                q = qkv_ref[rows, pl.ds(hd * head, head)]
                k = qkv_ref[:, pl.ds(pair + hd * head, head)]
                v = qkv_ref[:, pl.ds(2 * pair + hd * head, head)]
                s = lax.dot_general(q, k, (((1,), (1,)), ((), ())), preferred_element_type=F32)
                e = jnp.exp2((s - jnp.max(s, axis=-1, keepdims=True)) * scale)
                p = (e * (1.0 / jnp.sum(e, axis=-1, keepdims=True))).astype(BF16)
                outs.append(dot(p, v))
            o_ref[rows, :] = jnp.concatenate(outs, axis=-1).astype(BF16)

        for t in range(txs):
            acc_ref[t] += dot(o_ref[...], wbuf_a[slot, t, 3].reshape(pair, part))

    def mlp(layer, start, count, ty, slot):
        rows = pl.ds(start, count)
        hidden = u_ref.shape[1]
        for n in range(hidden // part):
            at = pl.ds(n * part, part)
            total = jnp.zeros((count, part), F32)
            for t in range(txs):
                total += dot(h_ref[t, rows, :], wbuf_u[slot, t, :, :, :, at].reshape(part, part))
            bias = biases[ty, pl.ds(layer, 1), pl.ds(3 * pair + n * part, part)]
            u_ref[rows, at] = jax.nn.gelu(total + bias, approximate=True).astype(BF16)
        for t in range(txs):
            acc_ref[t, rows, :] += dot(u_ref[rows, :], wbuf_d[slot, t].reshape(hidden, part))

    def at_work(scope, *calls):
        @pl.when(worker)
        def _():
            with jax.named_scope(scope):
                for f, *args in calls:
                    f(*args)

    each_part = tokens // PARTS
    for layer in range(layers):
        last = layer == layers - 1
        at_work("norm", (norm, 0, 1, layer))
        run(SLOTS[2 * layer], (0,), layer, functools.partial(attention, layer))
        at_work("finish_norm", (finish, 2, layer, 0, tokens), (norm, 3, 4, layer))
        if not last:
            run(SLOTS[2 * layer + 1], (1, 2), layer, functools.partial(mlp, layer, 0, tokens))
            at_work("finish", (finish, 5, layer, 0, tokens))

    def o1_copy(j, r):
        rows = pl.ds(r * each_part, each_part)
        return pltpu.make_async_remote_copy(
            src_ref=x_ref.at[j, rows], dst_ref=out_ref.at[me_s * each + me_t, rows], send_sem=o1_send.at[r, j],
            recv_sem=o1_recv.at[r, me_t], device_id={"tx": j}, device_id_type=MESH)

    def slices(r, act):
        @pl.when(worker)
        def _():
            for j in reversed(range(txs)):
                @pl.when(me_t != j)
                def _(j=j):
                    act(o1_copy(j, r))

    def keep_own(r):
        rows = pl.ds(r * each_part, each_part)
        out_ref[me_s * each + me_t, rows, :] = x_ref[me_t, rows, :]

    def wait_slice(m, r):
        rows = pl.ds(r * each_part, each_part)

        @pl.when(me_t != m)
        def _():
            place = out_ref.at[me_s * each + m, rows]
            pltpu.make_async_remote_copy(
                src_ref=place, dst_ref=place, send_sem=o1_send.at[r, 0], recv_sem=o1_recv.at[r, m],
                device_id={"tx": m}, device_id_type=MESH).wait_recv()

    def mlp_part(r, middle):
        run(SLOTS[2 * layers - 1] if r == 0 else (), (1, 2), layers - 1,
            functools.partial(mlp, layers - 1, r * each_part, each_part), middle)
        at_work("finish", (finish, 5, layers - 1, r * each_part, each_part))
        slices(r, lambda c: c.start())

        @pl.when(worker)
        def _():
            keep_own(r)

    ring = (("xp", 0, 0, 2), ("xm", 0, 0, 2), ("sib", 0, 0, 2),
            ("xp", -1, 0, 1), ("xm", 1, 1, 1), ("sib", -1, 0, 2), ("sib", 1, 0, 2), ("sib", 2, 0, 2))

    def ring_place(kind, ty, m, r):
        first, count = ring[kind][2:]
        return out_ref.at[ty * each + m, pl.ds(r * each_part + first * each_part // 2, count * each_part // 2)]

    def ring_op(kind, place, m, r):
        return pltpu.make_async_remote_copy(
            src_ref=place, dst_ref=place, send_sem=ring_send.at[kind],
            recv_sem=ring_recv.at[kind, 0 if ring[kind][0] == "sib" else r * each + m],
            device_id=target(ring[kind][0]), device_id_type=MESH)

    def ring_copy(kind, m, r):
        return ring_op(kind, ring_place(kind, ty_at(ring[kind][1]), m, r), m, r)

    def ring_arrival(kind, m, r):
        to, dx = ring[kind][:2]
        if to == "sib":
            ty = lax.rem(my_x + dx + nx, nx) * CORES + (CORES - 1 - my_c)
        else:
            ty = ty_at(dx - STEPS[to][0])
        return ring_op(kind, ring_place(kind, ty, m, r), m, r)

    def spread(m, r):
        wait_slice(m, r)
        for kind in (0, 1, 2):
            ring_copy(kind, m, r).start()

    def pass_on(m, r):
        ring_arrival(0, m, r).wait_recv()
        ring_copy(3, m, r).start()
        ring_copy(5, m, r).start()
        ring_arrival(1, m, r).wait_recv()
        ring_copy(4, m, r).start()
        ring_copy(6, m, r).start()

    def hand_over(m, r):
        ring_arrival(3, m, r).wait_recv()
        ring_arrival(4, m, r).wait_recv()
        ring_copy(7, m, r).start()

    def stages(r):
        def body(i, _):
            m = lax.rem(me_t + i, each)
            for stage, delay in ((spread, 1), (pass_on, 2), (hand_over, 3)):
                if 0 <= r - delay < PARTS:
                    stage(m, r - delay)
            return 0

        with jax.named_scope(f"output_{r}"):
            lax.fori_loop(0, each, body, 0)

    for r in range(PARTS):
        mlp_part(r, functools.partial(stages, r) if r else None)
    for r in range(PARTS, PARTS + 3):
        stages(r)

    def ring_total(kind):
        rows = tokens * ring[kind][3] // 2
        place = out_ref.at[pl.ds(0, each), pl.ds(0, rows)]
        return pltpu.make_async_remote_copy(
            src_ref=place, dst_ref=place, send_sem=ring_send.at[kind], recv_sem=ring_recv.at[kind, 0],
            device_id=target(ring[kind][0]), device_id_type=MESH)

    with jax.named_scope("wait_core"):
        for kind in (2, 5, 6, 7):
            ring_total(kind).wait_recv()

    for kind in range(len(ring)):
        ring_total(kind).wait_send()
    for j in range(each):
        @pl.when(me_t != j)
        def _():
            x_copy(j).wait_send()

    for r in range(PARTS):
        slices(r, lambda c: c.wait_send())
    for g in range(groups):
        for phase, (a, b) in enumerate(SENT):
            place = gathered[g % 3].at[g // 3, pl.ds(0, a), pl.ds(0, b)]
            pltpu.make_async_remote_copy(
                src_ref=place, dst_ref=place, send_sem=send_sem.at[g, phase], recv_sem=recv_sem.at[g, 0],
                device_id={"ty": sibling}, device_id_type=MESH).wait_send()


def solution(mesh):
    txs, tys = mesh.shape["tx"], mesh.shape["ty"]
    act_spec = P("dp", None, "tx")
    vec_tx = P(None, "tx")
    proj_spec = P(None, "tx", "ty", None)
    head_vec = P(None, "ty", None)
    in_specs = (act_spec, vec_tx, vec_tx, proj_spec, head_vec, proj_spec, proj_spec, head_vec,
                P(None, "ty", None, "tx"), vec_tx, vec_tx, vec_tx,
                P(None, "tx", "ty"), P(None, "ty"), P(None, "ty", "tx"), vec_tx)

    def local_fn(x_in, ln1_gain, ln1_bias, w_q, b_q, w_k, w_v, b_v, w_o, b_o, ln2_gain, ln2_bias, w_up, b_up, w_down, b_down):
        layers, depth, heads, head = w_q.shape
        imgs, tokens, part = x_in.shape
        hidden = w_up.shape[2]
        each, pair = imgs // tys, heads * head
        assert tys == 4 * CORES and txs == 4 and 4 * pair == hidden and depth == part and hidden % part == 0 and each < txs

        tall, wide = (4, 2, hidden // 8, part), (4, 2, depth // 8, hidden)
        wq, wk, wv = (w.transpose(0, 2, 3, 1).reshape((layers,) + tall[1:]) for w in (w_q, w_k, w_v))
        wo = w_o.reshape((layers,) + tall[1:])

        vmem = pl.BlockSpec(memory_space=pltpu.VMEM)
        hbm = pl.BlockSpec(memory_space=pl.ANY)
        dma = pltpu.SemaphoreType.DMA

        def buf(lead, shape):
            return pltpu.VMEM(lead + shape, BF16)

        out, *_ = pl.pallas_call(
            functools.partial(kernel, head, each),
            out_shape=(pltpu.VMEM(x_in.shape, BF16),
                       jax.ShapeDtypeStruct((layers, tys, txs) + tall, BF16),
                       jax.ShapeDtypeStruct((layers, tys, txs) + wide, BF16),
                       jax.ShapeDtypeStruct((layers, tys, txs) + tall, BF16)),
            in_specs=[hbm] * 7 + [vmem] * 9,
            out_specs=(vmem,) + (hbm,) * 3,
            scratch_shapes=[
                buf((txs,), (tokens, part)), buf((txs,), (tokens, part)), pltpu.VMEM((txs, tokens, part), F32),
                buf((), (tokens, 3 * pair)), buf((), (tokens, pair)), buf((), (tokens, hidden)),
                buf((layers,), tall), buf((layers,), wide), buf((layers,), tall),
                buf((tys, txs), tall), buf((tys, txs), wide), buf((tys, txs), tall),
                pltpu.VMEM((6, layers, part), F32), pltpu.VMEM((layers, 3 * pair + hidden), F32),
                pltpu.VMEM((txs, 6, layers, part), F32), pltpu.VMEM((tys, layers, 3 * pair + hidden), F32),
                dma((3 * layers, 5)), dma((3 * layers, FIRST[-1])), dma((6,)), dma((3,)), dma((3, tys)),
                dma((txs,)), dma((txs,)), dma((tys,)), dma((tys,)),
                dma((each,)), dma((txs,)), dma((PARTS, txs)), dma((PARTS, txs)), dma((8,)), dma((8, PARTS * each)),
            ],
            compiler_params=pltpu.CompilerParams(collective_id=0, has_side_effects=True, vmem_limit_bytes=52 << 20),
            cost_estimate=pl.CostEstimate(flops=80_000_000_000, bytes_accessed=150_000_000, transcendentals=20_000_000),
            name="encoder",
        )(x_in, wq, wk, wv, wo, w_up.reshape((layers,) + wide), w_down.reshape((layers,) + tall),
          b_q, b_v, b_up, ln1_gain, ln1_bias, b_o, ln2_gain, ln2_bias, b_down)
        return out

    return jax.shard_map(local_fn, mesh=mesh, in_specs=in_specs, out_specs=act_spec, check_vma=False)
```

```python
import functools
import math

import jax
import jax.numpy as jnp
from jax import lax
from jax.experimental import pallas as pl
from jax.experimental.pallas import tpu as pltpu
from jax.sharding import PartitionSpec as P

EPS = 1e-6
F32, BF16 = jnp.float32, jnp.bfloat16
MESH = pl.DeviceIdType.MESH
CORES = 2
STEPS = {"xp": (1, 0), "xm": (-1, 0), "yp": (0, 1), "ym": (0, -1)}


def phases():
    out = [[] for _ in range(5)]
    for to, (sx, sy) in STEPS.items():
        s, turned = sx + sy, "B" if sx else "A"
        sign = "plus" if s > 0 else "minus"

        def along(d, e, sx=sx):
            return (d, e) if sx else (e, d)

        out[0] += [(to, (0, 0), "all", "all")]
        out[1] += [(to, along(-s, 0), "all", sign)] + [(to, along(0, e), turned, "all") for e in (-1, 1)]
        out[2] += [(to, along(0, 2), turned, "all")] + [(to, along(-s, e), turned, sign) for e in (-1, 1)]
        out[3] += [(to, along(-s, 2), turned, sign)]
    for part in out:
        n = len(part) // 4
        part[:] = [part[link * n + i] for i in range(n) for link in range(4)]
    for dx in range(-1, 3):
        for dy in range(-1, 3):
            out[abs(dx) + abs(dy)].append(("sib", (dx, dy), "all", "all"))
    return out


PHASES = phases()
SENT = ((5, 1), (5, 2), (5, 2), (5, 1), (1, 1))
FIRST = [sum(len(p) for p in PHASES[:i]) for i in range(len(PHASES) + 1)]
BEFORE = "s10 s01 s20"
SLOTS = (
    ("l00 c00", "s11", "s30 l01", "s02 c01", "s21 l10", "s12", "s40 l02 c10 c02", "s31 s03 l11"),
    ("s22 l20 c20 c11", "s41 s13 l12", "s32 l21 c12", "c21", "s04", "s23 l30", "s42 l22 c30", "c22"),
    ("s05 s14", "s33 l31", "s15 c31", "", "s24 s43 l40 l32", "c32 c40", "s25 l50", "s34 l41 c50"),
    ("s35 l51 s44 l42", "c41 c51", "s45 l52", "", "", "", "c42 c52", ""),
)
RINGS = (((0,), (1,)), ((2, 3), (4, 5)), ((6,), (7,)))
PARTS = 3


def dot(a, b):
    return jnp.dot(a, b, preferred_element_type=F32)


def kernel(head, each, x_hbm, *refs):
    (wq_ref, wk_ref, wv_ref, wo_ref, wup_ref, wdown_ref, bq_ref, bv_ref, bup_ref,
     gain1_ref, shift1_ref, bo_ref, gain2_ref, shift2_ref, bdown_ref,
     out_ref, ga_ref, gu_ref, gd_ref,
     x_ref, h_ref, acc_ref, qkv_ref, o_ref, u_ref, own_a, own_u, own_d, wbuf_a, wbuf_u, wbuf_d, own_vec, own_bias, vecs, biases,
     send_sem, recv_sem, in_sem, own_sem, load_sem, vec_send, vec_recv, bias_send, bias_recv,
     xin_send, xin_recv, o1_send, o1_recv, ring_send, ring_recv) = refs
    layers, tys, txs = ga_ref.shape[:3]
    groups = 3 * layers
    owns, gathered = (own_a, own_u, own_d), (ga_ref, gu_ref, gd_ref)
    nx, ny = tys // CORES, txs
    tokens, part = x_ref.shape[1:]
    me_t, me_s = lax.axis_index("tx"), lax.axis_index("ty")
    my_x, my_c = me_s // CORES, lax.rem(me_s, CORES)
    sibling = my_x * CORES + (CORES - 1 - my_c)
    worker = me_t < each

    def ty_at(dx):
        return lax.rem(my_x + dx + nx, nx) * CORES + my_c

    def tx_at(dy):
        return lax.rem(me_t + dy + ny, ny)

    def target(to):
        if to == "sib":
            return {"ty": sibling}
        dx, dy = STEPS[to]
        return {"ty": ty_at(dx)} if dx else {"tx": tx_at(dy)}

    fills = [pltpu.make_async_copy(w, own_a.at[:, i], in_sem.at[i]) for i, w in enumerate((wq_ref, wk_ref, wv_ref, wo_ref))]
    fills += [pltpu.make_async_copy(wup_ref, own_u, in_sem.at[4]), pltpu.make_async_copy(wdown_ref, own_d, in_sem.at[5])]
    for c in fills:
        c.start()
    for i, ref in enumerate((gain1_ref, shift1_ref, bo_ref, gain2_ref, shift2_ref, bdown_ref)):
        own_vec[i] = ref[...]
    pair = o_ref.shape[1]
    own_bias[:, pl.ds(0, pair)] = jnp.concatenate([bq_ref[:, i, :] for i in range(pair // head)], axis=-1)
    own_bias[:, pl.ds(pair, pair)] = jnp.zeros((layers, pair), F32)
    own_bias[:, pl.ds(2 * pair, pair)] = jnp.concatenate([bv_ref[:, i, :] for i in range(pair // head)], axis=-1)
    own_bias[:, pl.ds(3 * pair, bup_ref.shape[1])] = bup_ref[...]

    barrier = pltpu.get_barrier_semaphore()
    for k in range(1, txs):
        pl.semaphore_signal(barrier, inc=1, device_id={"tx": tx_at(k)}, device_id_type=MESH)
    for k in range(1, tys):
        pl.semaphore_signal(barrier, inc=1, device_id={"ty": lax.rem(me_s + k, tys)}, device_id_type=MESH)
    pl.semaphore_wait(barrier, txs - 1 + tys - 1)

    def halves(g):
        cut = 1 if g == 0 else 2
        return {"all": pl.ds(0, 4), "A": pl.ds(0, cut), "B": pl.ds(cut, 4 - cut)}

    signs = {"all": pl.ds(0, 2), "plus": pl.ds(0, 1), "minus": pl.ds(1, 1)}

    def piece(g, ty, tx, half, sign):
        return gathered[g % 3].at[g // 3, ty, tx, halves(g)[half], signs[sign]]

    def copy(phase, i, g):
        to, (dx, dy), half, sign = PHASES[phase][i]
        place = piece(g, ty_at(dx), tx_at(dy), half, sign)
        return pltpu.make_async_remote_copy(
            src_ref=owns[g % 3].at[g // 3] if phase == 0 else place, dst_ref=place, send_sem=send_sem.at[g, phase],
            recv_sem=recv_sem.at[g, FIRST[phase] + i], device_id=target(to), device_id_type=MESH)

    def arrival(phase, i, g):
        to, (dx, dy), half, sign = PHASES[phase][i]
        if to == "sib":
            ty = lax.rem(my_x + dx + nx, nx) * CORES + (CORES - 1 - my_c)
            place = piece(g, ty, tx_at(dy), half, sign)
        else:
            sx, sy = STEPS[to]
            place = piece(g, ty_at(dx - sx), tx_at(dy - sy), half, sign)
        return pltpu.make_async_remote_copy(
            src_ref=place, dst_ref=place, send_sem=send_sem.at[g, phase],
            recv_sem=recv_sem.at[g, FIRST[phase] + i], device_id=target(to), device_id_type=MESH)

    def column(step):
        rem = lax.rem if isinstance(step, jax.Array) else lambda p, q: p % q
        region = (step // 2 + 1) // 2
        near = rem(region, 2)
        ring = near * (1 + rem(step, 2)) + 3 * (region // 2)
        core = (1 - near) * rem(step, 2) + near * (step // 2 - 1)
        return lax.rem(my_x + ring + ring // 2 - 2 * (ring // 3), nx) * CORES + lax.rem(my_c + core, CORES)

    def load(k, layer, step):
        return pltpu.make_async_copy(gathered[k].at[layer, column(step)], (wbuf_a, wbuf_u, wbuf_d)[k].at[step], load_sem.at[k, step])

    def event(kind, first, second):
        with jax.named_scope(f"{kind}_{first}_{second}"):
            first, second = int(first), int(second)
            if kind == "c":
                for phase in range(5):
                    for i, (to, (dx, _), _, _) in enumerate(PHASES[phase]):
                        if to == "sib" and abs(dx) == second:
                            arrival(phase, i, first).wait_recv()
            if kind in "cl":
                @pl.when(worker)
                def _():
                    for step in RINGS[second][kind == "c"]:
                        load(first % 3, first // 3, step).start()
                return
            phase, g = first, second
            if phase:
                for i, c in enumerate(PHASES[phase - 1]):
                    if c[0] != "sib":
                        arrival(phase - 1, i, g).wait_recv()
            for i in range(len(PHASES[phase])):
                copy(phase, i, g).start()

    for c in fills:
        c.wait()
    event("s", 0, 0)
    keep = [pltpu.make_async_copy(owns[i], gathered[i].at[:, me_s, me_t], own_sem.at[i]) for i in range(3)]
    for c in keep:
        c.start()

    def x_copy(j):
        return pltpu.make_async_remote_copy(
            src_ref=x_hbm.at[me_s * each + j], dst_ref=x_ref.at[me_t], send_sem=xin_send.at[j],
            recv_sem=xin_recv.at[me_t], device_id={"tx": j}, device_id_type=MESH)

    def x_local():
        return pltpu.make_async_copy(x_hbm.at[me_s * each + me_t], x_ref.at[me_t], xin_recv.at[me_t])

    for j in range(each):
        @pl.when(me_t != j)
        def _():
            x_copy(j).start()

        @pl.when(me_t == j)
        def _():
            x_local().start()

    def vec_copy(k):
        return pltpu.make_async_remote_copy(
            src_ref=own_vec, dst_ref=vecs.at[me_t], send_sem=vec_send.at[k], recv_sem=vec_recv.at[k],
            device_id={"tx": tx_at(k)}, device_id_type=MESH)

    def bias_copy(k):
        return pltpu.make_async_remote_copy(
            src_ref=own_bias, dst_ref=biases.at[me_s], send_sem=bias_send.at[k], recv_sem=bias_recv.at[k],
            device_id={"ty": lax.rem(me_s + k, tys)}, device_id_type=MESH)

    for k in range(1, txs):
        vec_copy(k).start()
    for k in range(1, tys):
        bias_copy(k).start()
    vecs[me_t] = own_vec[...]
    biases[me_s] = own_bias[...]

    for e in BEFORE.split():
        event(*e)

    with jax.named_scope("wait_vectors"):
        for k in range(1, txs):
            vec_copy(k).wait()
        for k in range(1, tys):
            bias_copy(k).wait()
        for c in keep:
            c.wait()

    @pl.when(worker)
    def _():
        with jax.named_scope("wait_x"):
            for m in range(txs):
                pltpu.make_async_copy(x_hbm.at[0], x_ref.at[m], xin_recv.at[m]).wait()

    def vec(row, layer):
        return jnp.concatenate([vecs[t, row, pl.ds(layer, 1), :] for t in range(txs)], axis=-1)

    def norm(gain_row, shift_row, layer):
        rows = 96

        def body(r, _):
            at = pl.ds(pl.multiple_of(r * rows, rows), rows)
            x_f = jnp.concatenate([x_ref[t, at, :] for t in range(txs)], axis=-1).astype(F32)
            mean = jnp.mean(x_f, axis=-1, keepdims=True)
            centred = x_f - mean
            variance = jnp.mean(centred * centred, axis=-1, keepdims=True)
            h = (centred * lax.rsqrt(variance + EPS) * vec(gain_row, layer) + vec(shift_row, layer)).astype(BF16)
            for t in range(txs):
                h_ref[t, at, :] = h[:, t * part:(t + 1) * part]
                acc_ref[t, at, :] = jnp.zeros((rows, part), F32)
            return 0

        lax.fori_loop(0, tokens // rows, body, 0)

    def finish(bias_row, layer, start, count):
        rows = 96

        def body(r, _):
            at = pl.ds(pl.multiple_of(start + r * rows, rows), rows)
            for t in range(txs):
                bias = vecs[t, bias_row, pl.ds(layer, 1), :]
                x_ref[t, at, :] = (x_ref[t, at, :].astype(F32) + acc_ref[t, at, :] + bias).astype(BF16)
            return 0

        lax.fori_loop(0, count // rows, body, 0)

    def run(parts, kinds, layer, body, middle=None):
        def step_body(step, _):
            for s, names in enumerate(parts):
                @pl.when(step == s)
                def _(names=names):
                    for e in names.split():
                        event(*e)

            if middle is not None:
                @pl.when(step == tys // 2)
                def _():
                    middle()

            @pl.when(worker)
            def _():
                if parts:
                    with jax.named_scope("wait_load"):
                        for k in kinds:
                            load(k, layer, step).wait()
                with jax.named_scope(f"compute_{kinds[0]}_{layer}"):
                    body(column(step), step)
            return 0

        lax.fori_loop(0, tys, step_body, 0)

    def attention(layer, ty, slot):
        def project(first, columns):
            total = jnp.zeros((tokens, columns), F32)
            for t in range(txs):
                w = wbuf_a[slot, t, pl.ds(first, columns // pair)].reshape(columns, part)
                total += lax.dot_general(h_ref[t], w, (((1,), (1,)), ((), ())), preferred_element_type=F32)
            return total

        at = pl.ds(0, 2 * pair)
        qkv_ref[:, at] = (project(0, 2 * pair) + biases[ty, pl.ds(layer, 1), at]).astype(BF16)
        at = pl.ds(2 * pair, pair)
        qkv_ref[:, at] = (project(2, pair) + biases[ty, pl.ds(layer, 1), at]).astype(BF16)

        scale = head ** -0.5 * math.log2(math.e)
        chunk = 192
        for c in range(tokens // chunk):
            rows = pl.ds(c * chunk, chunk)
            outs = []
            for hd in range(pair // head):
                q = qkv_ref[rows, pl.ds(hd * head, head)]
                k = qkv_ref[:, pl.ds(pair + hd * head, head)]
                v = qkv_ref[:, pl.ds(2 * pair + hd * head, head)]
                s = lax.dot_general(q, k, (((1,), (1,)), ((), ())), preferred_element_type=F32)
                e = jnp.exp2((s - jnp.max(s, axis=-1, keepdims=True)) * scale)
                p = (e * (1.0 / jnp.sum(e, axis=-1, keepdims=True))).astype(BF16)
                outs.append(dot(p, v))
            o_ref[rows, :] = jnp.concatenate(outs, axis=-1).astype(BF16)

        for t in range(txs):
            acc_ref[t] += dot(o_ref[...], wbuf_a[slot, t, 3].reshape(pair, part))

    def mlp(layer, start, count, ty, slot):
        rows = pl.ds(start, count)
        hidden = u_ref.shape[1]
        for n in range(hidden // part):
            at = pl.ds(n * part, part)
            total = jnp.zeros((count, part), F32)
            for t in range(txs):
                total += dot(h_ref[t, rows, :], wbuf_u[slot, t, :, :, :, at].reshape(part, part))
            bias = biases[ty, pl.ds(layer, 1), pl.ds(3 * pair + n * part, part)]
            u_ref[rows, at] = jax.nn.gelu(total + bias, approximate=True).astype(BF16)
        for t in range(txs):
            acc_ref[t, rows, :] += dot(u_ref[rows, :], wbuf_d[slot, t].reshape(hidden, part))

    def at_work(scope, *calls):
        @pl.when(worker)
        def _():
            with jax.named_scope(scope):
                for f, *args in calls:
                    f(*args)

    each_part = tokens // PARTS
    for layer in range(layers):
        last = layer == layers - 1
        at_work("norm", (norm, 0, 1, layer))
        run(SLOTS[2 * layer], (0,), layer, functools.partial(attention, layer))
        at_work("finish_norm", (finish, 2, layer, 0, tokens), (norm, 3, 4, layer))
        if not last:
            run(SLOTS[2 * layer + 1], (1, 2), layer, functools.partial(mlp, layer, 0, tokens))
            at_work("finish", (finish, 5, layer, 0, tokens))

    def o1_copy(j, r):
        rows = pl.ds(r * each_part, each_part)
        return pltpu.make_async_remote_copy(
            src_ref=x_ref.at[j, rows], dst_ref=out_ref.at[me_s * each + me_t, rows], send_sem=o1_send.at[r, j],
            recv_sem=o1_recv.at[r, me_t], device_id={"tx": j}, device_id_type=MESH)

    def slices(r, act):
        @pl.when(worker)
        def _():
            for j in reversed(range(txs)):
                @pl.when(me_t != j)
                def _(j=j):
                    act(o1_copy(j, r))

    def keep_own(r):
        rows = pl.ds(r * each_part, each_part)
        out_ref[me_s * each + me_t, rows, :] = x_ref[me_t, rows, :]

    def wait_slice(m, r):
        rows = pl.ds(r * each_part, each_part)
        place = out_ref.at[me_s * each + m, rows]
        pltpu.make_async_remote_copy(
            src_ref=place, dst_ref=place, send_sem=o1_send.at[r, 0], recv_sem=o1_recv.at[r, m],
            device_id={"tx": m}, device_id_type=MESH).wait_recv()

    ring = (("xp", 0, 0, 2), ("xm", 0, 0, 2), ("sib", 0, 0, 2),
            ("xp", -1, 0, 1), ("xm", 1, 1, 1), ("sib", -1, 0, 2), ("sib", 1, 0, 2), ("sib", 2, 0, 2))

    def ring_place(kind, ty, m, r):
        first, count = ring[kind][2:]
        return out_ref.at[ty * each + m, pl.ds(r * each_part + first * each_part // 2, count * each_part // 2)]

    def ring_op(kind, place, m, r):
        return pltpu.make_async_remote_copy(
            src_ref=place, dst_ref=place, send_sem=ring_send.at[kind],
            recv_sem=ring_recv.at[kind, 0 if ring[kind][0] == "sib" else r * each + m],
            device_id=target(ring[kind][0]), device_id_type=MESH)

    def ring_copy(kind, m, r):
        return ring_op(kind, ring_place(kind, ty_at(ring[kind][1]), m, r), m, r)

    def ring_arrival(kind, m, r):
        to, dx = ring[kind][:2]
        if to == "sib":
            ty = lax.rem(my_x + dx + nx, nx) * CORES + (CORES - 1 - my_c)
        else:
            ty = ty_at(dx - STEPS[to][0])
        return ring_op(kind, ring_place(kind, ty, m, r), m, r)

    def start_ring(m, r):
        for kind in (0, 1, 2):
            ring_copy(kind, m, r).start()

    def mlp_part(r, middle):
        run(SLOTS[2 * layers - 1] if r == 0 else (), (1, 2), layers - 1,
            functools.partial(mlp, layers - 1, r * each_part, each_part), middle)
        at_work("finish", (finish, 5, layers - 1, r * each_part, each_part))

        @pl.when(worker)
        def _():
            keep_own(r)
        slices(r, lambda c: c.start())

        @pl.when(worker)
        def _():
            start_ring(me_t, r)

    def spread(m, r):
        @pl.when(me_t != m)
        def _():
            wait_slice(m, r)
            start_ring(m, r)

    def pass_on(m, r):
        ring_arrival(0, m, r).wait_recv()
        ring_copy(3, m, r).start()
        ring_copy(5, m, r).start()
        ring_arrival(1, m, r).wait_recv()
        ring_copy(4, m, r).start()
        ring_copy(6, m, r).start()

    def hand_over(m, r):
        ring_arrival(3, m, r).wait_recv()
        ring_arrival(4, m, r).wait_recv()
        ring_copy(7, m, r).start()

    def stages(r):
        def each_image(*todo):
            todo = [(stage, r - delay) for stage, delay in todo if 0 <= r - delay < PARTS]

            def body(i, _):
                for stage, of in todo:
                    stage(lax.rem(me_t + i, each), of)
                return 0

            if todo:
                lax.fori_loop(0, each, body, 0)

        with jax.named_scope(f"output_{r}"):
            each_image((pass_on, 2), (hand_over, 3))
            each_image((spread, 1))

    for r in range(PARTS):
        mlp_part(r, functools.partial(stages, r) if r else None)
    for r in range(PARTS, PARTS + 3):
        stages(r)

    def ring_total(kind):
        rows = tokens * ring[kind][3] // 2
        place = out_ref.at[pl.ds(0, each), pl.ds(0, rows)]
        return pltpu.make_async_remote_copy(
            src_ref=place, dst_ref=place, send_sem=ring_send.at[kind], recv_sem=ring_recv.at[kind, 0],
            device_id=target(ring[kind][0]), device_id_type=MESH)

    with jax.named_scope("wait_core"):
        for kind in (2, 5, 6, 7):
            ring_total(kind).wait_recv()

    for kind in range(len(ring)):
        ring_total(kind).wait_send()
    for j in range(each):
        @pl.when(me_t != j)
        def _():
            x_copy(j).wait_send()

    for r in range(PARTS):
        slices(r, lambda c: c.wait_send())
    for g in range(groups):
        for phase, (a, b) in enumerate(SENT):
            place = gathered[g % 3].at[g // 3, pl.ds(0, a), pl.ds(0, b)]
            pltpu.make_async_remote_copy(
                src_ref=place, dst_ref=place, send_sem=send_sem.at[g, phase], recv_sem=recv_sem.at[g, 0],
                device_id={"ty": sibling}, device_id_type=MESH).wait_send()


def solution(mesh):
    txs, tys = mesh.shape["tx"], mesh.shape["ty"]
    act_spec = P("dp", None, "tx")
    vec_tx = P(None, "tx")
    proj_spec = P(None, "tx", "ty", None)
    head_vec = P(None, "ty", None)
    in_specs = (act_spec, vec_tx, vec_tx, proj_spec, head_vec, proj_spec, proj_spec, head_vec,
                P(None, "ty", None, "tx"), vec_tx, vec_tx, vec_tx,
                P(None, "tx", "ty"), P(None, "ty"), P(None, "ty", "tx"), vec_tx)

    def local_fn(x_in, ln1_gain, ln1_bias, w_q, b_q, w_k, w_v, b_v, w_o, b_o, ln2_gain, ln2_bias, w_up, b_up, w_down, b_down):
        layers, depth, heads, head = w_q.shape
        imgs, tokens, part = x_in.shape
        hidden = w_up.shape[2]
        each, pair = imgs // tys, heads * head
        assert tys == 4 * CORES and txs == 4 and 4 * pair == hidden and depth == part and hidden % part == 0 and each < txs

        tall, wide = (4, 2, hidden // 8, part), (4, 2, depth // 8, hidden)
        wq, wk, wv = (w.transpose(0, 2, 3, 1).reshape((layers,) + tall[1:]) for w in (w_q, w_k, w_v))
        wo = w_o.reshape((layers,) + tall[1:])

        vmem = pl.BlockSpec(memory_space=pltpu.VMEM)
        hbm = pl.BlockSpec(memory_space=pl.ANY)
        dma = pltpu.SemaphoreType.DMA

        def buf(lead, shape):
            return pltpu.VMEM(lead + shape, BF16)

        out, *_ = pl.pallas_call(
            functools.partial(kernel, head, each),
            out_shape=(pltpu.VMEM(x_in.shape, BF16),
                       jax.ShapeDtypeStruct((layers, tys, txs) + tall, BF16),
                       jax.ShapeDtypeStruct((layers, tys, txs) + wide, BF16),
                       jax.ShapeDtypeStruct((layers, tys, txs) + tall, BF16)),
            in_specs=[hbm] * 7 + [vmem] * 9,
            out_specs=(vmem,) + (hbm,) * 3,
            scratch_shapes=[
                buf((txs,), (tokens, part)), buf((txs,), (tokens, part)), pltpu.VMEM((txs, tokens, part), F32),
                buf((), (tokens, 3 * pair)), buf((), (tokens, pair)), buf((), (tokens, hidden)),
                buf((layers,), tall), buf((layers,), wide), buf((layers,), tall),
                buf((tys, txs), tall), buf((tys, txs), wide), buf((tys, txs), tall),
                pltpu.VMEM((6, layers, part), F32), pltpu.VMEM((layers, 3 * pair + hidden), F32),
                pltpu.VMEM((txs, 6, layers, part), F32), pltpu.VMEM((tys, layers, 3 * pair + hidden), F32),
                dma((3 * layers, 5)), dma((3 * layers, FIRST[-1])), dma((6,)), dma((3,)), dma((3, tys)),
                dma((txs,)), dma((txs,)), dma((tys,)), dma((tys,)),
                dma((each,)), dma((txs,)), dma((PARTS, txs)), dma((PARTS, txs)), dma((8,)), dma((8, PARTS * each)),
            ],
            compiler_params=pltpu.CompilerParams(collective_id=0, has_side_effects=True, vmem_limit_bytes=52 << 20),
            cost_estimate=pl.CostEstimate(flops=80_000_000_000, bytes_accessed=150_000_000, transcendentals=20_000_000),
            name="encoder",
        )(x_in, wq, wk, wv, wo, w_up.reshape((layers,) + wide), w_down.reshape((layers,) + tall),
          b_q, b_v, b_up, ln1_gain, ln1_bias, b_o, ln2_gain, ln2_bias, b_down)
        return out

    return jax.shard_map(local_fn, mesh=mesh, in_specs=in_specs, out_specs=act_spec, check_vma=False)
```

```python
import functools
import math

import jax
import jax.numpy as jnp
from jax import lax
from jax.experimental import pallas as pl
from jax.experimental.pallas import tpu as pltpu
from jax.sharding import PartitionSpec as P

EPS = 1e-6
F32, BF16 = jnp.float32, jnp.bfloat16
MESH = pl.DeviceIdType.MESH
CORES = 2
STEPS = {"xp": (1, 0), "xm": (-1, 0), "yp": (0, 1), "ym": (0, -1)}


def phases():
    out = [[] for _ in range(5)]
    for to, (sx, sy) in STEPS.items():
        s, turned = sx + sy, "B" if sx else "A"
        sign = "plus" if s > 0 else "minus"

        def along(d, e, sx=sx):
            return (d, e) if sx else (e, d)

        out[0] += [(to, (0, 0), "all", "all")]
        out[1] += [(to, along(-s, 0), "all", sign)] + [(to, along(0, e), turned, "all") for e in (-1, 1)]
        out[2] += [(to, along(0, 2), turned, "all")] + [(to, along(-s, e), turned, sign) for e in (-1, 1)]
        out[3] += [(to, along(-s, 2), turned, sign)]
    for part in out:
        n = len(part) // 4
        part[:] = [part[link * n + i] for i in range(n) for link in range(4)]
    for dx in range(-1, 3):
        for dy in range(-1, 3):
            out[abs(dx) + abs(dy)].append(("sib", (dx, dy), "all", "all"))
    return out


PHASES = phases()
SENT = ((5, 1), (5, 2), (5, 2), (5, 1), (1, 1))
BROUGHT = ((4, 1), (6, 1), (4, 1), (1, 1))
PASSED = ((4, 1), (8, 1), (4, 1))
BEFORE = "s10 s01 s20"
SLOTS = (
    ("l00 c00", "s11", "s30 l01", "s02 c01", "s21 l10", "s12", "s40 l02 c10 c02", "s31 s03 l11"),
    ("s22 l20 c20 c11", "s41 s13 l12", "s32 l21 c12", "c21", "s04", "s23 l30", "s42 l22 c30", "c22"),
    ("s05 s14", "s33 l31", "s15 c31", "", "s24 s43 l40 l32", "c32 c40", "s25 l50", "s34 l41 c50"),
    ("s35 l51 s44 l42", "c41 c51", "s45 l52", "", "", "", "c42 c52", ""),
)
RINGS = (((0,), (1,)), ((2, 3), (4, 5)), ((6,), (7,)))
PARTS = 3


def dot(a, b):
    return jnp.dot(a, b, preferred_element_type=F32)


def kernel(head, each, x_hbm, *refs):
    (wq_ref, wk_ref, wv_ref, wo_ref, wup_ref, wdown_ref, bq_ref, bv_ref, bup_ref,
     gain1_ref, shift1_ref, bo_ref, gain2_ref, shift2_ref, bdown_ref,
     out_ref, ga_ref, gu_ref, gd_ref,
     x_ref, h_ref, acc_ref, qkv_ref, o_ref, u_ref, own_a, own_u, own_d, wbuf_a, wbuf_u, wbuf_d, own_vec, own_bias, vecs, biases,
     send_sem, recv_sem, core_sem, in_sem, own_sem, load_sem, vec_send, vec_recv, bias_send, bias_recv,
     xin_send, xin_recv, o1_send, o1_recv, ring_send, ring_recv, ring_core) = refs
    layers, tys, txs = ga_ref.shape[:3]
    groups = 3 * layers
    owns, gathered = (own_a, own_u, own_d), (ga_ref, gu_ref, gd_ref)
    nx, ny = tys // CORES, txs
    tokens, part = x_ref.shape[1:]
    me_t, me_s = lax.axis_index("tx"), lax.axis_index("ty")
    my_x, my_c = me_s // CORES, lax.rem(me_s, CORES)
    sibling = my_x * CORES + (CORES - 1 - my_c)
    worker = me_t < each

    def ty_at(dx):
        return lax.rem(my_x + dx + nx, nx) * CORES + my_c

    def tx_at(dy):
        return lax.rem(me_t + dy + ny, ny)

    def target(to):
        if to == "sib":
            return {"ty": sibling}
        dx, dy = STEPS[to]
        return {"ty": ty_at(dx)} if dx else {"tx": tx_at(dy)}

    fills = [pltpu.make_async_copy(w, own_a.at[:, i], in_sem.at[i]) for i, w in enumerate((wq_ref, wk_ref, wv_ref, wo_ref))]
    fills += [pltpu.make_async_copy(wup_ref, own_u, in_sem.at[4]), pltpu.make_async_copy(wdown_ref, own_d, in_sem.at[5])]
    for c in fills:
        c.start()
    for i, ref in enumerate((gain1_ref, shift1_ref, bo_ref, gain2_ref, shift2_ref, bdown_ref)):
        own_vec[i] = ref[...]
    pair = o_ref.shape[1]
    own_bias[:, pl.ds(0, pair)] = jnp.concatenate([bq_ref[:, i, :] for i in range(pair // head)], axis=-1)
    own_bias[:, pl.ds(pair, pair)] = jnp.zeros((layers, pair), F32)
    own_bias[:, pl.ds(2 * pair, pair)] = jnp.concatenate([bv_ref[:, i, :] for i in range(pair // head)], axis=-1)
    own_bias[:, pl.ds(3 * pair, bup_ref.shape[1])] = bup_ref[...]

    barrier = pltpu.get_barrier_semaphore()
    for k in range(1, txs):
        pl.semaphore_signal(barrier, inc=1, device_id={"tx": tx_at(k)}, device_id_type=MESH)
    for k in range(1, tys):
        pl.semaphore_signal(barrier, inc=1, device_id={"ty": lax.rem(me_s + k, tys)}, device_id_type=MESH)
    pl.semaphore_wait(barrier, txs - 1 + tys - 1)

    def halves(g):
        cut = 1 if g == 0 else 2
        return {"all": pl.ds(0, 4), "A": pl.ds(0, cut), "B": pl.ds(cut, 4 - cut)}

    signs = {"all": pl.ds(0, 2), "plus": pl.ds(0, 1), "minus": pl.ds(1, 1)}

    def piece(g, ty, tx, half, sign):
        return gathered[g % 3].at[g // 3, ty, tx, halves(g)[half], signs[sign]]

    def copy(phase, i, g):
        to, (dx, dy), half, sign = PHASES[phase][i]
        place = piece(g, ty_at(dx), tx_at(dy), half, sign)
        return pltpu.make_async_remote_copy(
            src_ref=owns[g % 3].at[g // 3] if phase == 0 else place, dst_ref=place, send_sem=send_sem.at[g % 3, phase],
            recv_sem=core_sem.at[g, abs(dx)] if to == "sib" else recv_sem.at[g, phase],
            device_id=target(to), device_id_type=MESH)

    def wait_all(place, sem):
        pltpu.make_async_copy(place, place, sem).wait()

    def blocks(g, shape):
        return gathered[g % 3].at[g // 3, pl.ds(0, shape[0]), pl.ds(0, shape[1])]

    def column(step):
        rem = lax.rem if isinstance(step, jax.Array) else lambda p, q: p % q
        region = (step // 2 + 1) // 2
        near = rem(region, 2)
        ring = near * (1 + rem(step, 2)) + 3 * (region // 2)
        core = (1 - near) * rem(step, 2) + near * (step // 2 - 1)
        return lax.rem(my_x + ring + ring // 2 - 2 * (ring // 3), nx) * CORES + lax.rem(my_c + core, CORES)

    def load(k, layer, step):
        return pltpu.make_async_copy(gathered[k].at[layer, column(step)], (wbuf_a, wbuf_u, wbuf_d)[k].at[step], load_sem.at[k, step])

    def event(kind, first, second):
        with jax.named_scope(f"{kind}_{first}_{second}"):
            first, second = int(first), int(second)
            if kind == "c":
                wait_all(blocks(first, PASSED[second]), core_sem.at[first, second])
            if kind in "cl":
                @pl.when(worker)
                def _():
                    for step in RINGS[second][kind == "c"]:
                        load(first % 3, first // 3, step).start()
                return
            phase, g = first, second
            if phase:
                wait_all(blocks(g, BROUGHT[phase - 1]), recv_sem.at[g, phase - 1])
            for i in range(len(PHASES[phase])):
                copy(phase, i, g).start()

    for c in fills:
        c.wait()
    event("s", 0, 0)
    keep = [pltpu.make_async_copy(owns[i], gathered[i].at[:, me_s, me_t], own_sem.at[i]) for i in range(3)]
    for c in keep:
        c.start()

    def x_copy(j):
        return pltpu.make_async_remote_copy(
            src_ref=x_hbm.at[me_s * each + j], dst_ref=x_ref.at[me_t], send_sem=xin_send,
            recv_sem=xin_recv.at[me_t], device_id={"tx": j}, device_id_type=MESH)

    def x_local():
        return pltpu.make_async_copy(x_hbm.at[me_s * each + me_t], x_ref.at[me_t], xin_recv.at[me_t])

    for j in range(each):
        @pl.when(me_t != j)
        def _():
            x_copy(j).start()

        @pl.when(me_t == j)
        def _():
            x_local().start()

    def vec_copy(k):
        return pltpu.make_async_remote_copy(
            src_ref=own_vec, dst_ref=vecs.at[me_t], send_sem=vec_send, recv_sem=vec_recv,
            device_id={"tx": tx_at(k)}, device_id_type=MESH)

    def bias_copy(k):
        return pltpu.make_async_remote_copy(
            src_ref=own_bias, dst_ref=biases.at[me_s], send_sem=bias_send, recv_sem=bias_recv,
            device_id={"ty": lax.rem(me_s + k, tys)}, device_id_type=MESH)

    for k in range(1, txs):
        vec_copy(k).start()
    for k in range(1, tys):
        bias_copy(k).start()
    vecs[me_t] = own_vec[...]
    biases[me_s] = own_bias[...]

    for e in BEFORE.split():
        event(*e)

    with jax.named_scope("wait_vectors"):
        for sem in (vec_send, vec_recv):
            wait_all(vecs.at[pl.ds(0, txs - 1)], sem)
        for sem in (bias_send, bias_recv):
            wait_all(biases.at[pl.ds(0, tys - 1)], sem)
        for c in keep:
            c.wait()

    @pl.when(worker)
    def _():
        with jax.named_scope("wait_x"):
            for m in range(txs):
                pltpu.make_async_copy(x_hbm.at[0], x_ref.at[m], xin_recv.at[m]).wait()

    def vec(row, layer):
        return jnp.concatenate([vecs[t, row, pl.ds(layer, 1), :] for t in range(txs)], axis=-1)

    def norm(gain_row, shift_row, layer):
        rows = 96

        def body(r, _):
            at = pl.ds(pl.multiple_of(r * rows, rows), rows)
            x_f = jnp.concatenate([x_ref[t, at, :] for t in range(txs)], axis=-1).astype(F32)
            mean = jnp.mean(x_f, axis=-1, keepdims=True)
            centred = x_f - mean
            variance = jnp.mean(centred * centred, axis=-1, keepdims=True)
            h = (centred * lax.rsqrt(variance + EPS) * vec(gain_row, layer) + vec(shift_row, layer)).astype(BF16)
            for t in range(txs):
                h_ref[t, at, :] = h[:, t * part:(t + 1) * part]
                acc_ref[t, at, :] = jnp.zeros((rows, part), F32)
            return 0

        lax.fori_loop(0, tokens // rows, body, 0)

    def finish(bias_row, layer, start, count):
        rows = 96

        def body(r, _):
            at = pl.ds(pl.multiple_of(start + r * rows, rows), rows)
            for t in range(txs):
                bias = vecs[t, bias_row, pl.ds(layer, 1), :]
                x_ref[t, at, :] = (x_ref[t, at, :].astype(F32) + acc_ref[t, at, :] + bias).astype(BF16)
            return 0

        lax.fori_loop(0, count // rows, body, 0)

    def run(parts, kinds, layer, body, middle=None):
        def step_body(step, _):
            for s, names in enumerate(parts):
                @pl.when(step == s)
                def _(names=names):
                    for e in names.split():
                        event(*e)

            if middle is not None:
                @pl.when(step == tys // 2)
                def _():
                    middle()

            @pl.when(worker)
            def _():
                if parts:
                    with jax.named_scope("wait_load"):
                        for k in kinds:
                            load(k, layer, step).wait()
                with jax.named_scope(f"compute_{kinds[0]}_{layer}"):
                    body(column(step), step)
            return 0

        lax.fori_loop(0, tys, step_body, 0)

    def attention(layer, ty, slot):
        def project(first, columns):
            total = jnp.zeros((tokens, columns), F32)
            for t in range(txs):
                w = wbuf_a[slot, t, pl.ds(first, columns // pair)].reshape(columns, part)
                total += lax.dot_general(h_ref[t], w, (((1,), (1,)), ((), ())), preferred_element_type=F32)
            return total

        at = pl.ds(0, 2 * pair)
        qkv_ref[:, at] = (project(0, 2 * pair) + biases[ty, pl.ds(layer, 1), at]).astype(BF16)
        at = pl.ds(2 * pair, pair)
        qkv_ref[:, at] = (project(2, pair) + biases[ty, pl.ds(layer, 1), at]).astype(BF16)

        scale = head ** -0.5 * math.log2(math.e)
        chunk = 192
        for c in range(tokens // chunk):
            rows = pl.ds(c * chunk, chunk)
            outs = []
            for hd in range(pair // head):
                q = qkv_ref[rows, pl.ds(hd * head, head)]
                k = qkv_ref[:, pl.ds(pair + hd * head, head)]
                v = qkv_ref[:, pl.ds(2 * pair + hd * head, head)]
                s = lax.dot_general(q, k, (((1,), (1,)), ((), ())), preferred_element_type=F32)
                e = jnp.exp2((s - jnp.max(s, axis=-1, keepdims=True)) * scale)
                p = (e * (1.0 / jnp.sum(e, axis=-1, keepdims=True))).astype(BF16)
                outs.append(dot(p, v))
            o_ref[rows, :] = jnp.concatenate(outs, axis=-1).astype(BF16)

        for t in range(txs):
            acc_ref[t] += dot(o_ref[...], wbuf_a[slot, t, 3].reshape(pair, part))

    def mlp(layer, start, count, ty, slot):
        rows = pl.ds(start, count)
        hidden = u_ref.shape[1]
        for n in range(hidden // part):
            at = pl.ds(n * part, part)
            total = jnp.zeros((count, part), F32)
            for t in range(txs):
                total += dot(h_ref[t, rows, :], wbuf_u[slot, t, :, :, :, at].reshape(part, part))
            bias = biases[ty, pl.ds(layer, 1), pl.ds(3 * pair + n * part, part)]
            u_ref[rows, at] = jax.nn.gelu(total + bias, approximate=True).astype(BF16)
        for t in range(txs):
            acc_ref[t, rows, :] += dot(u_ref[rows, :], wbuf_d[slot, t].reshape(hidden, part))

    def at_work(scope, *calls):
        @pl.when(worker)
        def _():
            with jax.named_scope(scope):
                for f, *args in calls:
                    f(*args)

    each_part = tokens // PARTS
    for layer in range(layers):
        last = layer == layers - 1
        at_work("norm", (norm, 0, 1, layer))
        run(SLOTS[2 * layer], (0,), layer, functools.partial(attention, layer))
        at_work("finish_norm", (finish, 2, layer, 0, tokens), (norm, 3, 4, layer))
        if not last:
            run(SLOTS[2 * layer + 1], (1, 2), layer, functools.partial(mlp, layer, 0, tokens))
            at_work("finish", (finish, 5, layer, 0, tokens))

    def o1_copy(j, r):
        rows = pl.ds(r * each_part, each_part)
        return pltpu.make_async_remote_copy(
            src_ref=x_ref.at[j, rows], dst_ref=out_ref.at[me_s * each + me_t, rows], send_sem=o1_send,
            recv_sem=o1_recv.at[r, me_t], device_id={"tx": j}, device_id_type=MESH)

    def slices(r):
        @pl.when(worker)
        def _():
            for j in reversed(range(txs)):
                @pl.when(me_t != j)
                def _(j=j):
                    o1_copy(j, r).start()

    def keep_own(r):
        rows = pl.ds(r * each_part, each_part)
        out_ref[me_s * each + me_t, rows, :] = x_ref[me_t, rows, :]

    def part_of(image, r):
        return out_ref.at[image, pl.ds(r * each_part, each_part)]

    def wait_slice(m, r):
        wait_all(part_of(0, r), o1_recv.at[r, m])

    ring = (("xp", 0, 0, 2), ("xm", 0, 0, 2), ("sib", 0, 0, 2),
            ("xp", -1, 0, 1), ("xm", 1, 1, 1), ("sib", -1, 0, 2), ("sib", 1, 0, 2), ("sib", 2, 0, 2))

    def ring_place(kind, ty, m, r):
        first, count = ring[kind][2:]
        return out_ref.at[ty * each + m, pl.ds(r * each_part + first * each_part // 2, count * each_part // 2)]

    def ring_copy(kind, m, r):
        to, dx, _, count = ring[kind]
        place = ring_place(kind, ty_at(dx), m, r)
        if to == "sib":
            sem = ring_core
        else:
            sem = ring_recv.at[2 if count == 1 else kind, r * each + m]
        return pltpu.make_async_remote_copy(
            src_ref=place, dst_ref=place, send_sem=ring_send.at[kind], recv_sem=sem, device_id=target(to), device_id_type=MESH)

    def ring_wait(stage, m, r):
        wait_all(part_of(0, r), ring_recv.at[stage, r * each + m])

    def start_ring(m, r):
        for kind in (0, 1, 2):
            ring_copy(kind, m, r).start()

    def mlp_part(r, middle):
        run(SLOTS[2 * layers - 1] if r == 0 else (), (1, 2), layers - 1,
            functools.partial(mlp, layers - 1, r * each_part, each_part), middle)
        at_work("finish", (finish, 5, layers - 1, r * each_part, each_part))

        @pl.when(worker)
        def _():
            keep_own(r)
        slices(r)

        @pl.when(worker)
        def _():
            start_ring(me_t, r)

    def spread(m, r):
        @pl.when(me_t != m)
        def _():
            wait_slice(m, r)
            start_ring(m, r)

    def pass_on(m, r):
        ring_wait(0, m, r)
        ring_copy(3, m, r).start()
        ring_copy(5, m, r).start()
        ring_wait(1, m, r)
        ring_copy(4, m, r).start()
        ring_copy(6, m, r).start()

    def hand_over(m, r):
        ring_wait(2, m, r)
        ring_copy(7, m, r).start()

    def stages(r):
        def each_image(*todo):
            todo = [(stage, r - delay) for stage, delay in todo if 0 <= r - delay < PARTS]

            def body(i, _):
                for stage, of in todo:
                    stage(lax.rem(me_t + i, each), of)
                return 0

            if todo:
                lax.fori_loop(0, each, body, 0)

        with jax.named_scope(f"output_{r}"):
            each_image((pass_on, 2), (spread, 1))
            each_image((hand_over, 3))

    for r in range(PARTS):
        mlp_part(r, functools.partial(stages, r) if r else None)
    for r in range(PARTS, PARTS + 3):
        stages(r)

    with jax.named_scope("wait_core"):
        wait_all(out_ref.at[pl.ds(0, 4 * each)], ring_core)

    with jax.named_scope("wait_sent"):
        for kind in range(len(ring)):
            wait_all(out_ref.at[pl.ds(0, each), pl.ds(0, tokens * ring[kind][3] // 2)], ring_send.at[kind])

        @pl.when(worker)
        def _():
            wait_all(x_hbm.at[pl.ds(0, each - 1)], xin_send)
            wait_all(x_ref.at[pl.ds(0, txs - 1)], o1_send)

        @pl.when(jnp.logical_not(worker))
        def _():
            wait_all(x_hbm.at[pl.ds(0, each)], xin_send)
        for k in range(3):
            for phase, (a, b) in enumerate(SENT):
                wait_all(gathered[k].at[:, pl.ds(0, a), pl.ds(0, b)], send_sem.at[k, phase])


def solution(mesh):
    txs, tys = mesh.shape["tx"], mesh.shape["ty"]
    act_spec = P("dp", None, "tx")
    vec_tx = P(None, "tx")
    proj_spec = P(None, "tx", "ty", None)
    head_vec = P(None, "ty", None)
    in_specs = (act_spec, vec_tx, vec_tx, proj_spec, head_vec, proj_spec, proj_spec, head_vec,
                P(None, "ty", None, "tx"), vec_tx, vec_tx, vec_tx,
                P(None, "tx", "ty"), P(None, "ty"), P(None, "ty", "tx"), vec_tx)

    def local_fn(x_in, ln1_gain, ln1_bias, w_q, b_q, w_k, w_v, b_v, w_o, b_o, ln2_gain, ln2_bias, w_up, b_up, w_down, b_down):
        layers, depth, heads, head = w_q.shape
        imgs, tokens, part = x_in.shape
        hidden = w_up.shape[2]
        each, pair = imgs // tys, heads * head
        assert tys == 4 * CORES and txs == 4 and 4 * pair == hidden and depth == part and hidden % part == 0 and each < txs

        tall, wide = (4, 2, hidden // 8, part), (4, 2, depth // 8, hidden)
        wq, wk, wv = (w.transpose(0, 2, 3, 1).reshape((layers,) + tall[1:]) for w in (w_q, w_k, w_v))
        wo = w_o.reshape((layers,) + tall[1:])

        vmem = pl.BlockSpec(memory_space=pltpu.VMEM)
        hbm = pl.BlockSpec(memory_space=pl.ANY)
        dma = pltpu.SemaphoreType.DMA

        def buf(lead, shape):
            return pltpu.VMEM(lead + shape, BF16)

        out, *_ = pl.pallas_call(
            functools.partial(kernel, head, each),
            out_shape=(pltpu.VMEM(x_in.shape, BF16),
                       jax.ShapeDtypeStruct((layers, tys, txs) + tall, BF16),
                       jax.ShapeDtypeStruct((layers, tys, txs) + wide, BF16),
                       jax.ShapeDtypeStruct((layers, tys, txs) + tall, BF16)),
            in_specs=[hbm] * 7 + [vmem] * 9,
            out_specs=(vmem,) + (hbm,) * 3,
            scratch_shapes=[
                buf((txs,), (tokens, part)), buf((txs,), (tokens, part)), pltpu.VMEM((txs, tokens, part), F32),
                buf((), (tokens, 3 * pair)), buf((), (tokens, pair)), buf((), (tokens, hidden)),
                buf((layers,), tall), buf((layers,), wide), buf((layers,), tall),
                buf((tys, txs), tall), buf((tys, txs), wide), buf((tys, txs), tall),
                pltpu.VMEM((6, layers, part), F32), pltpu.VMEM((layers, 3 * pair + hidden), F32),
                pltpu.VMEM((txs, 6, layers, part), F32), pltpu.VMEM((tys, layers, 3 * pair + hidden), F32),
                dma((3, 5)), dma((3 * layers, 4)), dma((3 * layers, 3)), dma((6,)), dma((3,)), dma((3, tys)), dma, dma, dma, dma,
                dma, dma((txs,)), dma, dma((PARTS, txs)), dma((8,)), dma((3, PARTS * each)), dma,
            ],
            compiler_params=pltpu.CompilerParams(collective_id=0, has_side_effects=True, vmem_limit_bytes=52 << 20),
            cost_estimate=pl.CostEstimate(flops=80_000_000_000, bytes_accessed=150_000_000, transcendentals=20_000_000),
            name="encoder",
        )(x_in, wq, wk, wv, wo, w_up.reshape((layers,) + wide), w_down.reshape((layers,) + tall),
          b_q, b_v, b_up, ln1_gain, ln1_bias, b_o, ln2_gain, ln2_bias, b_down)
        return out

    return jax.shard_map(local_fn, mesh=mesh, in_specs=in_specs, out_specs=act_spec, check_vma=False)
```

```python
import functools
import math

import jax
import jax.numpy as jnp
from jax import lax
from jax.experimental import pallas as pl
from jax.experimental.pallas import tpu as pltpu
from jax.sharding import PartitionSpec as P

EPS = 1e-6
F32, BF16 = jnp.float32, jnp.bfloat16
MESH = pl.DeviceIdType.MESH
CORES = 2
STEPS = {"xp": (1, 0), "xm": (-1, 0), "yp": (0, 1), "ym": (0, -1)}


def phases():
    out = [[] for _ in range(5)]
    for to, (sx, sy) in STEPS.items():
        s, turned = sx + sy, "B" if sx else "A"
        sign = "plus" if s > 0 else "minus"

        def along(d, e, sx=sx):
            return (d, e) if sx else (e, d)

        out[0] += [(to, (0, 0), "all", "all")]
        out[1] += [(to, along(-s, 0), "all", sign)] + [(to, along(0, e), turned, "all") for e in (-1, 1)]
        out[2] += [(to, along(0, 2), turned, "all")] + [(to, along(-s, e), turned, sign) for e in (-1, 1)]
        out[3] += [(to, along(-s, 2), turned, sign)]
    for part in out:
        n = len(part) // 4
        part[:] = [part[link * n + i] for i in range(n) for link in range(4)]
    for dx in range(-1, 3):
        for dy in range(-1, 3):
            out[abs(dx) + abs(dy)].append(("sib", (dx, dy), "all", "all"))
    return out


PHASES = phases()
SENT = ((5, 1), (5, 2), (5, 2), (5, 1), (1, 1))
BROUGHT = ((4, 1), (6, 1), (4, 1), (1, 1))
PASSED = ((4, 1), (8, 1), (4, 1))
BEFORE = "s10 s01 s20"
SLOTS = (
    ("l00 c00", "s11", "s30 l01", "s02 c01", "s21 l10", "s12", "s40 l02 c10 c02", "s31 s03 l11"),
    ("s22 l20 c20 c11", "s41 s13 l12", "s32 l21 c12", "c21", "s04", "s23 l30", "s42 l22 c30", "c22"),
    ("s05 s14", "s33 l31", "s15 c31", "", "s24 s43 l40 l32", "c32 c40", "s25 l50", "s34 l41 c50"),
    ("s35 l51 s44 l42", "c41 c51", "s45 l52", "", "", "", "c42 c52", ""),
)
RINGS = (((0,), (1,)), ((2, 3), (4, 5)), ((6,), (7,)))
PARTS = 4


def dot(a, b):
    return jnp.dot(a, b, preferred_element_type=F32)


def kernel(head, each, x_hbm, *refs):
    (wq_ref, wk_ref, wv_ref, wo_ref, wup_ref, wdown_ref, bq_ref, bv_ref, bup_ref,
     gain1_ref, shift1_ref, bo_ref, gain2_ref, shift2_ref, bdown_ref,
     out_ref, ga_ref, gu_ref, gd_ref,
     x_ref, h_ref, acc_ref, qkv_ref, o_ref, u_ref, own_a, own_u, own_d, wbuf_a, wbuf_u, wbuf_d, own_vec, own_bias, vecs, biases,
     send_sem, recv_sem, core_sem, in_sem, own_sem, load_sem, vec_send, vec_recv, bias_send, bias_recv,
     xin_send, xin_recv, o1_send, o1_recv, ring_send, ring_recv, ring_core) = refs
    layers, tys, txs = ga_ref.shape[:3]
    groups = 3 * layers
    owns, gathered = (own_a, own_u, own_d), (ga_ref, gu_ref, gd_ref)
    nx, ny = tys // CORES, txs
    tokens, part = x_ref.shape[1:]
    me_t, me_s = lax.axis_index("tx"), lax.axis_index("ty")
    my_x, my_c = me_s // CORES, lax.rem(me_s, CORES)
    sibling = my_x * CORES + (CORES - 1 - my_c)
    worker = me_t < each

    def ty_at(dx):
        return lax.rem(my_x + dx + nx, nx) * CORES + my_c

    def tx_at(dy):
        return lax.rem(me_t + dy + ny, ny)

    def target(to):
        if to == "sib":
            return {"ty": sibling}
        dx, dy = STEPS[to]
        return {"ty": ty_at(dx)} if dx else {"tx": tx_at(dy)}

    fills = [pltpu.make_async_copy(w, own_a.at[:, i], in_sem.at[i]) for i, w in enumerate((wq_ref, wk_ref, wv_ref, wo_ref))]
    fills += [pltpu.make_async_copy(wup_ref, own_u, in_sem.at[4]), pltpu.make_async_copy(wdown_ref, own_d, in_sem.at[5])]
    for c in fills:
        c.start()
    for i, ref in enumerate((gain1_ref, shift1_ref, bo_ref, gain2_ref, shift2_ref, bdown_ref)):
        own_vec[i] = ref[...]
    pair = o_ref.shape[1]
    own_bias[:, pl.ds(0, pair)] = jnp.concatenate([bq_ref[:, i, :] for i in range(pair // head)], axis=-1)
    own_bias[:, pl.ds(pair, pair)] = jnp.zeros((layers, pair), F32)
    own_bias[:, pl.ds(2 * pair, pair)] = jnp.concatenate([bv_ref[:, i, :] for i in range(pair // head)], axis=-1)
    own_bias[:, pl.ds(3 * pair, bup_ref.shape[1])] = bup_ref[...]

    barrier = pltpu.get_barrier_semaphore()
    for k in range(1, txs):
        pl.semaphore_signal(barrier, inc=1, device_id={"tx": tx_at(k)}, device_id_type=MESH)
    for k in range(1, tys):
        pl.semaphore_signal(barrier, inc=1, device_id={"ty": lax.rem(me_s + k, tys)}, device_id_type=MESH)
    pl.semaphore_wait(barrier, txs - 1 + tys - 1)

    def halves(g):
        cut = 1 if g == 0 else 2
        return {"all": pl.ds(0, 4), "A": pl.ds(0, cut), "B": pl.ds(cut, 4 - cut)}

    signs = {"all": pl.ds(0, 2), "plus": pl.ds(0, 1), "minus": pl.ds(1, 1)}

    def piece(g, ty, tx, half, sign):
        return gathered[g % 3].at[g // 3, ty, tx, halves(g)[half], signs[sign]]

    def copy(phase, i, g):
        to, (dx, dy), half, sign = PHASES[phase][i]
        place = piece(g, ty_at(dx), tx_at(dy), half, sign)
        return pltpu.make_async_remote_copy(
            src_ref=owns[g % 3].at[g // 3] if phase == 0 else place, dst_ref=place, send_sem=send_sem.at[g % 3, phase],
            recv_sem=core_sem.at[g, abs(dx)] if to == "sib" else recv_sem.at[g, phase],
            device_id=target(to), device_id_type=MESH)

    def wait_all(place, sem):
        pltpu.make_async_copy(place, place, sem).wait()

    def blocks(g, shape):
        return gathered[g % 3].at[g // 3, pl.ds(0, shape[0]), pl.ds(0, shape[1])]

    def column(step):
        rem = lax.rem if isinstance(step, jax.Array) else lambda p, q: p % q
        region = (step // 2 + 1) // 2
        near = rem(region, 2)
        ring = near * (1 + rem(step, 2)) + 3 * (region // 2)
        core = (1 - near) * rem(step, 2) + near * (step // 2 - 1)
        return lax.rem(my_x + ring + ring // 2 - 2 * (ring // 3), nx) * CORES + lax.rem(my_c + core, CORES)

    def load(k, layer, step):
        return pltpu.make_async_copy(gathered[k].at[layer, column(step)], (wbuf_a, wbuf_u, wbuf_d)[k].at[step], load_sem.at[k, step])

    def event(kind, first, second):
        with jax.named_scope(f"{kind}_{first}_{second}"):
            first, second = int(first), int(second)
            if kind == "c":
                wait_all(blocks(first, PASSED[second]), core_sem.at[first, second])
            if kind in "cl":
                @pl.when(worker)
                def _():
                    for step in RINGS[second][kind == "c"]:
                        load(first % 3, first // 3, step).start()
                return
            phase, g = first, second
            if phase:
                wait_all(blocks(g, BROUGHT[phase - 1]), recv_sem.at[g, phase - 1])
            for i in range(len(PHASES[phase])):
                copy(phase, i, g).start()

    for c in fills[:4]:
        c.wait()
    event("s", 0, 0)
    for c in fills[4:]:
        c.wait()
    keep = [pltpu.make_async_copy(owns[i], gathered[i].at[:, me_s, me_t], own_sem.at[i]) for i in range(3)]
    for c in keep:
        c.start()

    def x_copy(j):
        return pltpu.make_async_remote_copy(
            src_ref=x_hbm.at[me_s * each + j], dst_ref=x_ref.at[me_t], send_sem=xin_send,
            recv_sem=xin_recv.at[me_t], device_id={"tx": j}, device_id_type=MESH)

    def x_local():
        return pltpu.make_async_copy(x_hbm.at[me_s * each + me_t], x_ref.at[me_t], xin_recv.at[me_t])

    for j in range(each):
        @pl.when(me_t != j)
        def _():
            x_copy(j).start()

        @pl.when(me_t == j)
        def _():
            x_local().start()

    def vec_copy(k):
        return pltpu.make_async_remote_copy(
            src_ref=own_vec, dst_ref=vecs.at[me_t], send_sem=vec_send, recv_sem=vec_recv,
            device_id={"tx": tx_at(k)}, device_id_type=MESH)

    def bias_copy(k):
        return pltpu.make_async_remote_copy(
            src_ref=own_bias, dst_ref=biases.at[me_s], send_sem=bias_send, recv_sem=bias_recv,
            device_id={"ty": lax.rem(me_s + k, tys)}, device_id_type=MESH)

    for k in range(1, txs):
        vec_copy(k).start()
    for k in range(1, tys):
        bias_copy(k).start()
    vecs[me_t] = own_vec[...]
    biases[me_s] = own_bias[...]

    for e in BEFORE.split():
        event(*e)

    with jax.named_scope("wait_vectors"):
        for sem in (vec_send, vec_recv):
            wait_all(vecs.at[pl.ds(0, txs - 1)], sem)
        for sem in (bias_send, bias_recv):
            wait_all(biases.at[pl.ds(0, tys - 1)], sem)
        for c in keep:
            c.wait()

    @pl.when(worker)
    def _():
        with jax.named_scope("wait_x"):
            for m in range(txs):
                pltpu.make_async_copy(x_hbm.at[0], x_ref.at[m], xin_recv.at[m]).wait()

    def vec(row, layer):
        return jnp.concatenate([vecs[t, row, pl.ds(layer, 1), :] for t in range(txs)], axis=-1)

    def norm(gain_row, shift_row, layer):
        rows = 96

        def body(r, _):
            at = pl.ds(pl.multiple_of(r * rows, rows), rows)
            x_f = jnp.concatenate([x_ref[t, at, :] for t in range(txs)], axis=-1).astype(F32)
            mean = jnp.mean(x_f, axis=-1, keepdims=True)
            centred = x_f - mean
            variance = jnp.mean(centred * centred, axis=-1, keepdims=True)
            h = (centred * lax.rsqrt(variance + EPS) * vec(gain_row, layer) + vec(shift_row, layer)).astype(BF16)
            for t in range(txs):
                h_ref[t, at, :] = h[:, t * part:(t + 1) * part]
                acc_ref[t, at, :] = jnp.zeros((rows, part), F32)
            return 0

        lax.fori_loop(0, tokens // rows, body, 0)

    def finish(bias_row, layer, start, count):
        rows = 48

        def body(r, _):
            at = pl.ds(pl.multiple_of(start + r * rows, rows), rows)
            for t in range(txs):
                bias = vecs[t, bias_row, pl.ds(layer, 1), :]
                x_ref[t, at, :] = (x_ref[t, at, :].astype(F32) + acc_ref[t, at, :] + bias).astype(BF16)
            return 0

        lax.fori_loop(0, count // rows, body, 0)

    def run(parts, kinds, layer, body, middle=None):
        def step_body(step, _):
            for s, names in enumerate(parts):
                @pl.when(step == s)
                def _(names=names):
                    for e in names.split():
                        event(*e)

            if middle is not None:
                @pl.when(step == tys // 2)
                def _():
                    middle()

            @pl.when(worker)
            def _():
                if parts:
                    with jax.named_scope("wait_load"):
                        for k in kinds:
                            load(k, layer, step).wait()
                with jax.named_scope(f"compute_{kinds[0]}_{layer}"):
                    body(column(step), step)
            return 0

        lax.fori_loop(0, tys, step_body, 0)

    def attention(layer, ty, slot):
        def project(first, columns):
            total = jnp.zeros((tokens, columns), F32)
            for t in range(txs):
                w = wbuf_a[slot, t, pl.ds(first, columns // pair)].reshape(columns, part)
                total += lax.dot_general(h_ref[t], w, (((1,), (1,)), ((), ())), preferred_element_type=F32)
            return total

        at = pl.ds(0, 2 * pair)
        qkv_ref[:, at] = (project(0, 2 * pair) + biases[ty, pl.ds(layer, 1), at]).astype(BF16)
        at = pl.ds(2 * pair, pair)
        qkv_ref[:, at] = (project(2, pair) + biases[ty, pl.ds(layer, 1), at]).astype(BF16)

        scale = head ** -0.5 * math.log2(math.e)
        chunk = 192
        for c in range(tokens // chunk):
            rows = pl.ds(c * chunk, chunk)
            outs = []
            for hd in range(pair // head):
                q = qkv_ref[rows, pl.ds(hd * head, head)]
                k = qkv_ref[:, pl.ds(pair + hd * head, head)]
                v = qkv_ref[:, pl.ds(2 * pair + hd * head, head)]
                s = lax.dot_general(q, k, (((1,), (1,)), ((), ())), preferred_element_type=F32)
                e = jnp.exp2((s - jnp.max(s, axis=-1, keepdims=True)) * scale)
                p = (e * (1.0 / jnp.sum(e, axis=-1, keepdims=True))).astype(BF16)
                outs.append(dot(p, v))
            o_ref[rows, :] = jnp.concatenate(outs, axis=-1).astype(BF16)

        for t in range(txs):
            acc_ref[t] += dot(o_ref[...], wbuf_a[slot, t, 3].reshape(pair, part))

    def mlp(layer, start, count, ty, slot):
        rows = pl.ds(start, count)
        hidden = u_ref.shape[1]
        for n in range(hidden // part):
            at = pl.ds(n * part, part)
            total = jnp.zeros((count, part), F32)
            for t in range(txs):
                total += dot(h_ref[t, rows, :], wbuf_u[slot, t, :, :, :, at].reshape(part, part))
            bias = biases[ty, pl.ds(layer, 1), pl.ds(3 * pair + n * part, part)]
            u_ref[rows, at] = jax.nn.gelu(total + bias, approximate=True).astype(BF16)
        for t in range(txs):
            acc_ref[t, rows, :] += dot(u_ref[rows, :], wbuf_d[slot, t].reshape(hidden, part))

    def at_work(scope, *calls):
        @pl.when(worker)
        def _():
            with jax.named_scope(scope):
                for f, *args in calls:
                    f(*args)

    each_part = tokens // PARTS
    for layer in range(layers):
        last = layer == layers - 1
        at_work("norm", (norm, 0, 1, layer))
        run(SLOTS[2 * layer], (0,), layer, functools.partial(attention, layer))
        at_work("finish_norm", (finish, 2, layer, 0, tokens), (norm, 3, 4, layer))
        if not last:
            run(SLOTS[2 * layer + 1], (1, 2), layer, functools.partial(mlp, layer, 0, tokens))
            at_work("finish", (finish, 5, layer, 0, tokens))

    def o1_copy(j, r):
        rows = pl.ds(r * each_part, each_part)
        return pltpu.make_async_remote_copy(
            src_ref=x_ref.at[j, rows], dst_ref=out_ref.at[me_s * each + me_t, rows], send_sem=o1_send,
            recv_sem=o1_recv.at[r, me_t], device_id={"tx": j}, device_id_type=MESH)

    def slices(r):
        @pl.when(worker)
        def _():
            for j in reversed(range(txs)):
                @pl.when(me_t != j)
                def _(j=j):
                    o1_copy(j, r).start()

    def keep_own(r):
        rows = pl.ds(r * each_part, each_part)
        out_ref[me_s * each + me_t, rows, :] = x_ref[me_t, rows, :]

    def part_of(image, r):
        return out_ref.at[image, pl.ds(r * each_part, each_part)]

    def wait_slice(m, r):
        wait_all(part_of(0, r), o1_recv.at[r, m])

    ring = (("xp", 0, 0, 2), ("xm", 0, 0, 2), ("sib", 0, 0, 2),
            ("xp", -1, 0, 1), ("xm", 1, 1, 1), ("sib", -1, 0, 2), ("sib", 1, 0, 2), ("sib", 2, 0, 2))

    def ring_place(kind, ty, m, r):
        first, count = ring[kind][2:]
        return out_ref.at[ty * each + m, pl.ds(r * each_part + first * each_part // 2, count * each_part // 2)]

    def ring_copy(kind, m, r):
        to, dx, _, count = ring[kind]
        place = ring_place(kind, ty_at(dx), m, r)
        if to == "sib":
            sem = ring_core
        else:
            sem = ring_recv.at[2 if count == 1 else kind, r * each + m]
        return pltpu.make_async_remote_copy(
            src_ref=place, dst_ref=place, send_sem=ring_send.at[kind], recv_sem=sem, device_id=target(to), device_id_type=MESH)

    def ring_wait(stage, m, r):
        wait_all(part_of(0, r), ring_recv.at[stage, r * each + m])

    def start_ring(m, r):
        for kind in (0, 1, 2):
            ring_copy(kind, m, r).start()

    def mlp_part(r, middle):
        run(SLOTS[2 * layers - 1] if r == 0 else (), (1, 2), layers - 1,
            functools.partial(mlp, layers - 1, r * each_part, each_part), middle)
        at_work("finish", (finish, 5, layers - 1, r * each_part, each_part))

        @pl.when(worker)
        def _():
            keep_own(r)
        slices(r)

        @pl.when(worker)
        def _():
            start_ring(me_t, r)

    def spread(m, r):
        @pl.when(me_t != m)
        def _():
            wait_slice(m, r)
            start_ring(m, r)

    def pass_on(m, r):
        ring_wait(0, m, r)
        ring_copy(3, m, r).start()
        ring_copy(5, m, r).start()
        ring_wait(1, m, r)
        ring_copy(4, m, r).start()
        ring_copy(6, m, r).start()

    def hand_over(m, r):
        ring_wait(2, m, r)
        ring_copy(7, m, r).start()

    def stages(r):
        def each_image(*todo):
            todo = [(stage, r - delay) for stage, delay in todo if 0 <= r - delay < PARTS]

            def body(i, _):
                for stage, of in todo:
                    stage(lax.rem(me_t + i, each), of)
                return 0

            if todo:
                lax.fori_loop(0, each, body, 0)

        with jax.named_scope(f"output_{r}"):
            each_image((pass_on, 2), (spread, 1))
            each_image((hand_over, 3))

    for r in range(PARTS):
        mlp_part(r, functools.partial(stages, r) if r else None)
    for r in range(PARTS, PARTS + 3):
        stages(r)

    with jax.named_scope("wait_core"):
        wait_all(out_ref.at[pl.ds(0, 4 * each)], ring_core)

    with jax.named_scope("wait_sent"):
        for kind in range(len(ring)):
            wait_all(out_ref.at[pl.ds(0, each), pl.ds(0, tokens * ring[kind][3] // 2)], ring_send.at[kind])

        @pl.when(worker)
        def _():
            wait_all(x_hbm.at[pl.ds(0, each - 1)], xin_send)
            wait_all(x_ref.at[pl.ds(0, txs - 1)], o1_send)

        @pl.when(jnp.logical_not(worker))
        def _():
            wait_all(x_hbm.at[pl.ds(0, each)], xin_send)
        for k in range(3):
            for phase, (a, b) in enumerate(SENT):
                wait_all(gathered[k].at[:, pl.ds(0, a), pl.ds(0, b)], send_sem.at[k, phase])


def solution(mesh):
    txs, tys = mesh.shape["tx"], mesh.shape["ty"]
    act_spec = P("dp", None, "tx")
    vec_tx = P(None, "tx")
    proj_spec = P(None, "tx", "ty", None)
    head_vec = P(None, "ty", None)
    in_specs = (act_spec, vec_tx, vec_tx, proj_spec, head_vec, proj_spec, proj_spec, head_vec,
                P(None, "ty", None, "tx"), vec_tx, vec_tx, vec_tx,
                P(None, "tx", "ty"), P(None, "ty"), P(None, "ty", "tx"), vec_tx)

    def local_fn(x_in, ln1_gain, ln1_bias, w_q, b_q, w_k, w_v, b_v, w_o, b_o, ln2_gain, ln2_bias, w_up, b_up, w_down, b_down):
        layers, depth, heads, head = w_q.shape
        imgs, tokens, part = x_in.shape
        hidden = w_up.shape[2]
        each, pair = imgs // tys, heads * head
        assert tys == 4 * CORES and txs == 4 and 4 * pair == hidden and depth == part and hidden % part == 0 and each < txs

        tall, wide = (4, 2, hidden // 8, part), (4, 2, depth // 8, hidden)
        wq, wk, wv = (w.transpose(0, 2, 3, 1).reshape((layers,) + tall[1:]) for w in (w_q, w_k, w_v))
        wo = w_o.reshape((layers,) + tall[1:])

        vmem = pl.BlockSpec(memory_space=pltpu.VMEM)
        hbm = pl.BlockSpec(memory_space=pl.ANY)
        dma = pltpu.SemaphoreType.DMA

        def buf(lead, shape):
            return pltpu.VMEM(lead + shape, BF16)

        out, *_ = pl.pallas_call(
            functools.partial(kernel, head, each),
            out_shape=(pltpu.VMEM(x_in.shape, BF16),
                       jax.ShapeDtypeStruct((layers, tys, txs) + tall, BF16),
                       jax.ShapeDtypeStruct((layers, tys, txs) + wide, BF16),
                       jax.ShapeDtypeStruct((layers, tys, txs) + tall, BF16)),
            in_specs=[hbm] * 7 + [vmem] * 9,
            out_specs=(vmem,) + (hbm,) * 3,
            scratch_shapes=[
                buf((txs,), (tokens, part)), buf((txs,), (tokens, part)), pltpu.VMEM((txs, tokens, part), F32),
                buf((), (tokens, 3 * pair)), buf((), (tokens, pair)), buf((), (tokens, hidden)),
                buf((layers,), tall), buf((layers,), wide), buf((layers,), tall),
                buf((tys, txs), tall), buf((tys, txs), wide), buf((tys, txs), tall),
                pltpu.VMEM((6, layers, part), F32), pltpu.VMEM((layers, 3 * pair + hidden), F32),
                pltpu.VMEM((txs, 6, layers, part), F32), pltpu.VMEM((tys, layers, 3 * pair + hidden), F32),
                dma((3, 5)), dma((3 * layers, 4)), dma((3 * layers, 3)), dma((6,)), dma((3,)), dma((3, tys)), dma, dma, dma, dma,
                dma, dma((txs,)), dma, dma((PARTS, txs)), dma((8,)), dma((3, PARTS * each)), dma,
            ],
            compiler_params=pltpu.CompilerParams(collective_id=0, has_side_effects=True, vmem_limit_bytes=52 << 20),
            cost_estimate=pl.CostEstimate(flops=80_000_000_000, bytes_accessed=150_000_000, transcendentals=20_000_000),
            name="encoder",
        )(x_in, wq, wk, wv, wo, w_up.reshape((layers,) + wide), w_down.reshape((layers,) + tall),
          b_q, b_v, b_up, ln1_gain, ln1_bias, b_o, ln2_gain, ln2_bias, b_down)
        return out

    return jax.shard_map(local_fn, mesh=mesh, in_specs=in_specs, out_specs=act_spec, check_vma=False)
```

```python
import functools
import math

import jax
import jax.numpy as jnp
from jax import lax
from jax.experimental import pallas as pl
from jax.experimental.pallas import tpu as pltpu
from jax.sharding import PartitionSpec as P

EPS = 1e-6
F32, BF16 = jnp.float32, jnp.bfloat16
MESH = pl.DeviceIdType.MESH
CORES = 2
STEPS = {"xp": (1, 0), "xm": (-1, 0), "yp": (0, 1), "ym": (0, -1)}


def phases():
    out = [[] for _ in range(5)]
    for to, (sx, sy) in STEPS.items():
        s, turned = sx + sy, "B" if sx else "A"
        sign = "plus" if s > 0 else "minus"

        def along(d, e, sx=sx):
            return (d, e) if sx else (e, d)

        out[0] += [(to, (0, 0), "all", "all")]
        out[1] += [(to, along(-s, 0), "all", sign)] + [(to, along(0, e), turned, "all") for e in (-1, 1)]
        out[2] += [(to, along(0, 2), turned, "all")] + [(to, along(-s, e), turned, sign) for e in (-1, 1)]
        out[3] += [(to, along(-s, 2), turned, sign)]
    for part in out:
        n = len(part) // 4
        part[:] = [part[link * n + i] for i in range(n) for link in range(4)]
    for dx in range(-1, 3):
        for dy in range(-1, 3):
            out[abs(dx) + abs(dy)].append(("sib", (dx, dy), "all", "all"))
    return out


PHASES = phases()
SENT = ((5, 1), (5, 2), (5, 2), (5, 1), (1, 1))
BROUGHT = ((4, 1), (6, 1), (4, 1), (1, 1))
PASSED = ((4, 1), (8, 1), (4, 1))
BEFORE = "s10 s01 s20"
SLOTS = (
    ("l00 c00", "s11", "s30 l01", "s02 c01", "s21 l10", "s12", "s40 l02 c10 c02", "s31 s03 l11"),
    ("s22 l20 c20 c11", "s41 s13 l12", "s32 l21 c12", "c21", "s04", "s23 l30", "s42 l22 c30", "c22"),
    ("s05 s14", "s33 l31", "s15 c31", "", "s24 s43 l40 l32", "c32 c40", "s25 l50", "s34 l41 c50"),
    ("s35 l51 s44 l42", "c41 c51", "s45 l52", "", "", "", "c42 c52", ""),
)
RINGS = (((0,), (1,)), ((2, 3), (4, 5)), ((6,), (7,)))
PARTS = 3


def dot(a, b):
    return jnp.dot(a, b, preferred_element_type=F32)


def kernel(head, each, x_hbm, *refs):
    (wq_ref, wk_ref, wv_ref, wo_ref, wup_ref, wdown_ref, bq_ref, bv_ref, bup_ref,
     gain1_ref, shift1_ref, bo_ref, gain2_ref, shift2_ref, bdown_ref,
     out_ref, ga_ref, gu_ref, gd_ref,
     x_ref, h_ref, acc_ref, qkv_ref, o_ref, u_ref, own_a, own_u, own_d, wbuf_a, wbuf_u, wbuf_d, own_vec, own_bias, vecs, biases,
     send_sem, recv_sem, core_sem, in_sem, own_sem, load_sem, vec_send, vec_recv, bias_send, bias_recv,
     xin_send, xin_recv, o1_send, o1_recv, ring_send, ring_recv, ring_core) = refs
    layers, tys, txs = ga_ref.shape[:3]
    groups = 3 * layers
    owns, gathered = (own_a, own_u, own_d), (ga_ref, gu_ref, gd_ref)
    nx, ny = tys // CORES, txs
    tokens, part = x_ref.shape[1:]
    me_t, me_s = lax.axis_index("tx"), lax.axis_index("ty")
    my_x, my_c = me_s // CORES, lax.rem(me_s, CORES)
    sibling = my_x * CORES + (CORES - 1 - my_c)
    worker = me_t < each

    def ty_at(dx):
        return lax.rem(my_x + dx + nx, nx) * CORES + my_c

    def tx_at(dy):
        return lax.rem(me_t + dy + ny, ny)

    def target(to):
        if to == "sib":
            return {"ty": sibling}
        dx, dy = STEPS[to]
        return {"ty": ty_at(dx)} if dx else {"tx": tx_at(dy)}

    fills = [pltpu.make_async_copy(w, own_a.at[:, i], in_sem.at[i]) for i, w in enumerate((wq_ref, wk_ref, wv_ref, wo_ref))]
    fills += [pltpu.make_async_copy(wup_ref, own_u, in_sem.at[4]), pltpu.make_async_copy(wdown_ref, own_d, in_sem.at[5])]
    for c in fills:
        c.start()
    for i, ref in enumerate((gain1_ref, shift1_ref, bo_ref, gain2_ref, shift2_ref, bdown_ref)):
        own_vec[i] = ref[...]
    pair = o_ref.shape[1]
    own_bias[:, pl.ds(0, pair)] = jnp.concatenate([bq_ref[:, i, :] for i in range(pair // head)], axis=-1)
    own_bias[:, pl.ds(pair, pair)] = jnp.zeros((layers, pair), F32)
    own_bias[:, pl.ds(2 * pair, pair)] = jnp.concatenate([bv_ref[:, i, :] for i in range(pair // head)], axis=-1)
    own_bias[:, pl.ds(3 * pair, bup_ref.shape[1])] = bup_ref[...]

    barrier = pltpu.get_barrier_semaphore()
    for k in range(1, txs):
        pl.semaphore_signal(barrier, inc=1, device_id={"tx": tx_at(k)}, device_id_type=MESH)
    for k in range(1, tys):
        pl.semaphore_signal(barrier, inc=1, device_id={"ty": lax.rem(me_s + k, tys)}, device_id_type=MESH)
    pl.semaphore_wait(barrier, txs - 1 + tys - 1)

    def halves(g):
        cut = 1 if g == 0 else 2
        return {"all": pl.ds(0, 4), "A": pl.ds(0, cut), "B": pl.ds(cut, 4 - cut)}

    signs = {"all": pl.ds(0, 2), "plus": pl.ds(0, 1), "minus": pl.ds(1, 1)}

    def piece(g, ty, tx, half, sign):
        return gathered[g % 3].at[g // 3, ty, tx, halves(g)[half], signs[sign]]

    def copy(phase, i, g):
        to, (dx, dy), half, sign = PHASES[phase][i]
        place = piece(g, ty_at(dx), tx_at(dy), half, sign)
        return pltpu.make_async_remote_copy(
            src_ref=owns[g % 3].at[g // 3] if phase == 0 else place, dst_ref=place, send_sem=send_sem.at[g % 3, phase],
            recv_sem=core_sem.at[g, abs(dx)] if to == "sib" else recv_sem.at[g, phase],
            device_id=target(to), device_id_type=MESH)

    def wait_all(place, sem):
        pltpu.make_async_copy(place, place, sem).wait()

    def blocks(g, shape):
        return gathered[g % 3].at[g // 3, pl.ds(0, shape[0]), pl.ds(0, shape[1])]

    def column(step):
        rem = lax.rem if isinstance(step, jax.Array) else lambda p, q: p % q
        region = (step // 2 + 1) // 2
        near = rem(region, 2)
        ring = near * (1 + rem(step, 2)) + 3 * (region // 2)
        core = (1 - near) * rem(step, 2) + near * (step // 2 - 1)
        return lax.rem(my_x + ring + ring // 2 - 2 * (ring // 3), nx) * CORES + lax.rem(my_c + core, CORES)

    def load(k, layer, step):
        return pltpu.make_async_copy(gathered[k].at[layer, column(step)], (wbuf_a, wbuf_u, wbuf_d)[k].at[step], load_sem.at[k, step])

    def event(kind, first, second):
        with jax.named_scope(f"{kind}_{first}_{second}"):
            first, second = int(first), int(second)
            if kind == "c":
                wait_all(blocks(first, PASSED[second]), core_sem.at[first, second])
            if kind in "cl":
                @pl.when(worker)
                def _():
                    for step in RINGS[second][kind == "c"]:
                        load(first % 3, first // 3, step).start()
                return
            phase, g = first, second
            if phase:
                wait_all(blocks(g, BROUGHT[phase - 1]), recv_sem.at[g, phase - 1])
            for i in range(len(PHASES[phase])):
                copy(phase, i, g).start()

    for c in fills[:4]:
        c.wait()
    event("s", 0, 0)
    for c in fills[4:]:
        c.wait()
    keep = [pltpu.make_async_copy(owns[i], gathered[i].at[:, me_s, me_t], own_sem.at[i]) for i in range(3)]
    for c in keep:
        c.start()

    def x_copy(j):
        return pltpu.make_async_remote_copy(
            src_ref=x_hbm.at[me_s * each + j], dst_ref=x_ref.at[me_t], send_sem=xin_send,
            recv_sem=xin_recv.at[me_t], device_id={"tx": j}, device_id_type=MESH)

    def x_local():
        return pltpu.make_async_copy(x_hbm.at[me_s * each + me_t], x_ref.at[me_t], xin_recv.at[me_t])

    for j in range(each):
        @pl.when(me_t != j)
        def _():
            x_copy(j).start()

        @pl.when(me_t == j)
        def _():
            x_local().start()

    def vec_copy(k):
        return pltpu.make_async_remote_copy(
            src_ref=own_vec, dst_ref=vecs.at[me_t], send_sem=vec_send, recv_sem=vec_recv,
            device_id={"tx": tx_at(k)}, device_id_type=MESH)

    def bias_copy(k):
        return pltpu.make_async_remote_copy(
            src_ref=own_bias, dst_ref=biases.at[me_s], send_sem=bias_send, recv_sem=bias_recv,
            device_id={"ty": lax.rem(me_s + k, tys)}, device_id_type=MESH)

    for k in range(1, txs):
        vec_copy(k).start()
    for k in range(1, tys):
        bias_copy(k).start()
    vecs[me_t] = own_vec[...]
    biases[me_s] = own_bias[...]

    for e in BEFORE.split():
        event(*e)

    with jax.named_scope("wait_vectors"):
        for sem in (vec_send, vec_recv):
            wait_all(vecs.at[pl.ds(0, txs - 1)], sem)
        for sem in (bias_send, bias_recv):
            wait_all(biases.at[pl.ds(0, tys - 1)], sem)
        for c in keep:
            c.wait()

    @pl.when(worker)
    def _():
        with jax.named_scope("wait_x"):
            for m in range(txs):
                pltpu.make_async_copy(x_hbm.at[0], x_ref.at[m], xin_recv.at[m]).wait()

    def vec(row, layer):
        return jnp.concatenate([vecs[t, row, pl.ds(layer, 1), :] for t in range(txs)], axis=-1)

    def norm(gain_row, shift_row, layer):
        rows = 96

        def body(r, _):
            at = pl.ds(pl.multiple_of(r * rows, rows), rows)
            x_f = jnp.concatenate([x_ref[t, at, :] for t in range(txs)], axis=-1).astype(F32)
            mean = jnp.mean(x_f, axis=-1, keepdims=True)
            centred = x_f - mean
            variance = jnp.mean(centred * centred, axis=-1, keepdims=True)
            h = (centred * lax.rsqrt(variance + EPS) * vec(gain_row, layer) + vec(shift_row, layer)).astype(BF16)
            for t in range(txs):
                h_ref[t, at, :] = h[:, t * part:(t + 1) * part]
                acc_ref[t, at, :] = jnp.zeros((rows, part), F32)
            return 0

        lax.fori_loop(0, tokens // rows, body, 0)

    def finish(bias_row, layer, start, count):
        rows = 96

        def body(r, _):
            at = pl.ds(pl.multiple_of(start + r * rows, rows), rows)
            for t in range(txs):
                bias = vecs[t, bias_row, pl.ds(layer, 1), :]
                x_ref[t, at, :] = (x_ref[t, at, :].astype(F32) + acc_ref[t, at, :] + bias).astype(BF16)
            return 0

        lax.fori_loop(0, count // rows, body, 0)

    def run(parts, kinds, layer, body, middle=None):
        def step_body(step, _):
            for s, names in enumerate(parts):
                @pl.when(step == s)
                def _(names=names):
                    for e in names.split():
                        event(*e)

            if middle is not None:
                @pl.when(step == tys // 2)
                def _():
                    middle()

            @pl.when(worker)
            def _():
                if parts:
                    with jax.named_scope("wait_load"):
                        for k in kinds:
                            load(k, layer, step).wait()
                with jax.named_scope(f"compute_{kinds[0]}_{layer}"):
                    body(column(step), step)
            return 0

        lax.fori_loop(0, tys, step_body, 0)

    def attention(layer, ty, slot):
        def project(first, columns):
            total = jnp.zeros((tokens, columns), F32)
            for t in range(txs):
                w = wbuf_a[slot, t, pl.ds(first, columns // pair)].reshape(columns, part)
                total += lax.dot_general(h_ref[t], w, (((1,), (1,)), ((), ())), preferred_element_type=F32)
            return total

        at = pl.ds(0, 2 * pair)
        qkv_ref[:, at] = (project(0, 2 * pair) + biases[ty, pl.ds(layer, 1), at]).astype(BF16)
        at = pl.ds(2 * pair, pair)
        qkv_ref[:, at] = (project(2, pair) + biases[ty, pl.ds(layer, 1), at]).astype(BF16)

        scale = head ** -0.5 * math.log2(math.e)
        chunk = 192
        for c in range(tokens // chunk):
            rows = pl.ds(c * chunk, chunk)
            outs = []
            for hd in range(pair // head):
                q = qkv_ref[rows, pl.ds(hd * head, head)]
                k = qkv_ref[:, pl.ds(pair + hd * head, head)]
                v = qkv_ref[:, pl.ds(2 * pair + hd * head, head)]
                s = lax.dot_general(q, k, (((1,), (1,)), ((), ())), preferred_element_type=F32)
                e = jnp.exp2((s - jnp.max(s, axis=-1, keepdims=True)) * scale)
                p = (e * (1.0 / jnp.sum(e, axis=-1, keepdims=True))).astype(BF16)
                outs.append(dot(p, v))
            o_ref[rows, :] = jnp.concatenate(outs, axis=-1).astype(BF16)

        for t in range(txs):
            acc_ref[t] += dot(o_ref[...], wbuf_a[slot, t, 3].reshape(pair, part))

    def mlp(layer, start, count, ty, slot):
        rows = pl.ds(start, count)
        hidden = u_ref.shape[1]
        for n in range(hidden // part):
            at = pl.ds(n * part, part)
            total = jnp.zeros((count, part), F32)
            for t in range(txs):
                total += dot(h_ref[t, rows, :], wbuf_u[slot, t, :, :, :, at].reshape(part, part))
            bias = biases[ty, pl.ds(layer, 1), pl.ds(3 * pair + n * part, part)]
            u_ref[rows, at] = jax.nn.gelu(total + bias, approximate=True).astype(BF16)
        for t in range(txs):
            acc_ref[t, rows, :] += dot(u_ref[rows, :], wbuf_d[slot, t].reshape(hidden, part))

    def at_work(scope, *calls):
        @pl.when(worker)
        def _():
            with jax.named_scope(scope):
                for f, *args in calls:
                    f(*args)

    each_part = tokens // PARTS
    for layer in range(layers):
        last = layer == layers - 1
        at_work("norm", (norm, 0, 1, layer))
        run(SLOTS[2 * layer], (0,), layer, functools.partial(attention, layer))
        at_work("finish_norm", (finish, 2, layer, 0, tokens), (norm, 3, 4, layer))
        if not last:
            run(SLOTS[2 * layer + 1], (1, 2), layer, functools.partial(mlp, layer, 0, tokens))
            at_work("finish", (finish, 5, layer, 0, tokens))

    def o1_copy(j, r):
        rows = pl.ds(r * each_part, each_part)
        return pltpu.make_async_remote_copy(
            src_ref=x_ref.at[j, rows], dst_ref=out_ref.at[me_s * each + me_t, rows], send_sem=o1_send,
            recv_sem=o1_recv.at[r, me_t], device_id={"tx": j}, device_id_type=MESH)

    def slices(r):
        @pl.when(worker)
        def _():
            for far in (False, True):
                for j in reversed(range(txs)):
                    is_far = lax.rem(me_t - j + txs, txs) == txs // 2

                    @pl.when((me_t != j) & (is_far if far else jnp.logical_not(is_far)))
                    def _(j=j):
                        o1_copy(j, r).start()

    def keep_own(r):
        rows = pl.ds(r * each_part, each_part)
        out_ref[me_s * each + me_t, rows, :] = x_ref[me_t, rows, :]

    def part_of(image, r):
        return out_ref.at[image, pl.ds(r * each_part, each_part)]

    def wait_slice(m, r):
        wait_all(part_of(0, r), o1_recv.at[r, m])

    ring = (("xp", 0, 0, 2), ("xm", 0, 0, 2), ("sib", 0, 0, 2),
            ("xp", -1, 0, 1), ("xm", 1, 1, 1), ("sib", -1, 0, 2), ("sib", 1, 0, 2), ("sib", 2, 0, 2))

    def ring_place(kind, ty, m, r):
        first, count = ring[kind][2:]
        return out_ref.at[ty * each + m, pl.ds(r * each_part + first * each_part // 2, count * each_part // 2)]

    def ring_copy(kind, m, r):
        to, dx, _, count = ring[kind]
        place = ring_place(kind, ty_at(dx), m, r)
        if to == "sib":
            sem = ring_core
        else:
            sem = ring_recv.at[2 if count == 1 else kind, r * each + m]
        return pltpu.make_async_remote_copy(
            src_ref=place, dst_ref=place, send_sem=ring_send.at[kind], recv_sem=sem, device_id=target(to), device_id_type=MESH)

    def ring_wait(stage, m, r):
        wait_all(part_of(0, r), ring_recv.at[stage, r * each + m])

    def start_ring(m, r):
        for kind in (0, 1, 2):
            ring_copy(kind, m, r).start()

    def mlp_part(r, middle):
        run(SLOTS[2 * layers - 1] if r == 0 else (), (1, 2), layers - 1,
            functools.partial(mlp, layers - 1, r * each_part, each_part), middle)
        at_work("finish", (finish, 5, layers - 1, r * each_part, each_part))

        @pl.when(worker)
        def _():
            keep_own(r)
        slices(r)

        @pl.when(worker)
        def _():
            start_ring(me_t, r)

    def spread(m, r):
        @pl.when(me_t != m)
        def _():
            wait_slice(m, r)
            start_ring(m, r)

    def pass_on(m, r):
        ring_wait(0, m, r)
        ring_copy(3, m, r).start()
        ring_copy(5, m, r).start()
        ring_wait(1, m, r)
        ring_copy(4, m, r).start()
        ring_copy(6, m, r).start()

    def hand_over(m, r):
        ring_wait(2, m, r)
        ring_copy(7, m, r).start()

    def stages(r):
        def each_image(*todo):
            todo = [(stage, r - delay) for stage, delay in todo if 0 <= r - delay < PARTS]

            def body(i, _):
                for stage, of in todo:
                    stage(lax.rem(me_t + (each - 1) * i, each), of)
                return 0

            if todo:
                lax.fori_loop(0, each, body, 0)

        with jax.named_scope(f"output_{r}"):
            each_image((pass_on, 2), (spread, 1))
            each_image((hand_over, 3))

    for r in range(PARTS):
        mlp_part(r, functools.partial(stages, r) if r else None)
    for r in range(PARTS, PARTS + 3):
        stages(r)

    with jax.named_scope("wait_core"):
        wait_all(out_ref.at[pl.ds(0, 4 * each)], ring_core)

    with jax.named_scope("wait_sent"):
        for kind in range(len(ring)):
            wait_all(out_ref.at[pl.ds(0, each), pl.ds(0, tokens * ring[kind][3] // 2)], ring_send.at[kind])

        @pl.when(worker)
        def _():
            wait_all(x_hbm.at[pl.ds(0, each - 1)], xin_send)
            wait_all(x_ref.at[pl.ds(0, txs - 1)], o1_send)

        @pl.when(jnp.logical_not(worker))
        def _():
            wait_all(x_hbm.at[pl.ds(0, each)], xin_send)
        for k in range(3):
            for phase, (a, b) in enumerate(SENT):
                wait_all(gathered[k].at[:, pl.ds(0, a), pl.ds(0, b)], send_sem.at[k, phase])


def solution(mesh):
    txs, tys = mesh.shape["tx"], mesh.shape["ty"]
    act_spec = P("dp", None, "tx")
    vec_tx = P(None, "tx")
    proj_spec = P(None, "tx", "ty", None)
    head_vec = P(None, "ty", None)
    in_specs = (act_spec, vec_tx, vec_tx, proj_spec, head_vec, proj_spec, proj_spec, head_vec,
                P(None, "ty", None, "tx"), vec_tx, vec_tx, vec_tx,
                P(None, "tx", "ty"), P(None, "ty"), P(None, "ty", "tx"), vec_tx)

    def local_fn(x_in, ln1_gain, ln1_bias, w_q, b_q, w_k, w_v, b_v, w_o, b_o, ln2_gain, ln2_bias, w_up, b_up, w_down, b_down):
        layers, depth, heads, head = w_q.shape
        imgs, tokens, part = x_in.shape
        hidden = w_up.shape[2]
        each, pair = imgs // tys, heads * head
        assert tys == 4 * CORES and txs == 4 and 4 * pair == hidden and depth == part and hidden % part == 0 and each < txs

        tall, wide = (4, 2, hidden // 8, part), (4, 2, depth // 8, hidden)
        wq, wk, wv = (w.transpose(0, 2, 3, 1).reshape((layers,) + tall[1:]) for w in (w_q, w_k, w_v))
        wo = w_o.reshape((layers,) + tall[1:])

        vmem = pl.BlockSpec(memory_space=pltpu.VMEM)
        hbm = pl.BlockSpec(memory_space=pl.ANY)
        dma = pltpu.SemaphoreType.DMA

        def buf(lead, shape):
            return pltpu.VMEM(lead + shape, BF16)

        out, *_ = pl.pallas_call(
            functools.partial(kernel, head, each),
            out_shape=(pltpu.VMEM(x_in.shape, BF16),
                       jax.ShapeDtypeStruct((layers, tys, txs) + tall, BF16),
                       jax.ShapeDtypeStruct((layers, tys, txs) + wide, BF16),
                       jax.ShapeDtypeStruct((layers, tys, txs) + tall, BF16)),
            in_specs=[hbm] * 7 + [vmem] * 9,
            out_specs=(vmem,) + (hbm,) * 3,
            scratch_shapes=[
                buf((txs,), (tokens, part)), buf((txs,), (tokens, part)), pltpu.VMEM((txs, tokens, part), F32),
                buf((), (tokens, 3 * pair)), buf((), (tokens, pair)), buf((), (tokens, hidden)),
                buf((layers,), tall), buf((layers,), wide), buf((layers,), tall),
                buf((tys, txs), tall), buf((tys, txs), wide), buf((tys, txs), tall),
                pltpu.VMEM((6, layers, part), F32), pltpu.VMEM((layers, 3 * pair + hidden), F32),
                pltpu.VMEM((txs, 6, layers, part), F32), pltpu.VMEM((tys, layers, 3 * pair + hidden), F32),
                dma((3, 5)), dma((3 * layers, 4)), dma((3 * layers, 3)), dma((6,)), dma((3,)), dma((3, tys)), dma, dma, dma, dma,
                dma, dma((txs,)), dma, dma((PARTS, txs)), dma((8,)), dma((3, PARTS * each)), dma,
            ],
            compiler_params=pltpu.CompilerParams(collective_id=0, has_side_effects=True, vmem_limit_bytes=52 << 20),
            cost_estimate=pl.CostEstimate(flops=80_000_000_000, bytes_accessed=150_000_000, transcendentals=20_000_000),
            name="encoder",
        )(x_in, wq, wk, wv, wo, w_up.reshape((layers,) + wide), w_down.reshape((layers,) + tall),
          b_q, b_v, b_up, ln1_gain, ln1_bias, b_o, ln2_gain, ln2_bias, b_down)
        return out

    return jax.shard_map(local_fn, mesh=mesh, in_specs=in_specs, out_specs=act_spec, check_vma=False)
```
